32 devices in a mesh: dp: 4 (over z), ctx: 2 (over x), tp: 4 (over y, core).
Axes of the slice: x: 2, y: 2, z: 4, core: 2. Of those that a mesh axis runs over, the one named last changes fastest.
Arguments:
- tokens: bfloat16 [4096, 2048], P(('dp', 'ctx')), may hold values from -6 to 6
- segments: int32 [4, 1024], P('dp'), may hold values from 0 to 3, never falling along the last dimension, each value on 1 to 512 neighbouring positions
- attn_gain: float32 [2048], replicated, may hold values from 0.5 to 1.5
- query_weight: bfloat16 [2048, 2048], P(None, 'tp'), may hold values from -0.125 to 0.125
- key_weight: bfloat16 [2048, 256], P(None, 'tp'), may hold values from -0.125 to 0.125
- value_weight: bfloat16 [2048, 256], P(None, 'tp'), may hold values from -0.125 to 0.125
- output_weight: bfloat16 [2048, 2048], P('tp'), may hold values from -2 to 2
- mlp_gain: float32 [2048], replicated, may hold values from 0.5 to 1.5
- gate_weight: bfloat16 [2048, 5632], P(None, 'tp'), may hold values from -0.125 to 0.125
- up_weight: bfloat16 [2048, 5632], P(None, 'tp'), may hold values from -0.125 to 0.125
- down_weight: bfloat16 [5632, 2048], P('tp'), may hold values from -0.078125 to 0.078125
- cotangent: bfloat16 [4096, 2048], P(('dp', 'ctx')), may hold values from -6 to 6
Outputs:
- layer_out: float32 [4096, 2048], P(('dp', 'ctx'))
- tokens_grad: float32 [4096, 2048], P(('dp', 'ctx'))
- attn_gain_grad: float32 [2048], P(('dp', 'ctx'))
- query_grad: float32 [2048, 2048], P(('dp', 'ctx'), 'tp')
- key_grad: float32 [2048, 256], P(('dp', 'ctx'), 'tp')
- value_grad: float32 [2048, 256], P(('dp', 'ctx'), 'tp')
- output_grad: float32 [2048, 2048], P('tp', ('dp', 'ctx'))
- mlp_gain_grad: float32 [2048], P(('dp', 'ctx'))
- gate_grad: float32 [2048, 5632], P(('dp', 'ctx'), 'tp')
- up_grad: float32 [2048, 5632], P(('dp', 'ctx'), 'tp')
- down_grad: float32 [5632, 2048], P('tp', ('dp', 'ctx'))
The draws below stay inside these ranges and needn't reach their ends.
Inputs may be any that keep to these rules, and one draw needn't show every extreme that they name: `segments`: along each packed sequence the document numbers never fall; a document has 1 to 512 tokens, and one document of each sequence has exactly 512.
All inputs are finite; a program needn't handle non-finite values.
Results may differ from the reference program's by a relative error of at most 0.013.
Values may be sent and summed in bfloat16 or wider, within the bound.
A program may use at most 192 MiB of HBM per device.

```python
import math
import jax
import jax.numpy as jnp
import numpy as np
from jax import lax

D = 2048
HEADS = 32
KV_HEADS = 4
HEAD = 64
FF = 5632
SPAN = 512
SEQ = 1024
TOKENS = 4096
N_DP = 4


def level_of(key, extent, cuts, low, top_value):
    def one(dim, parts):
        steps = jax.random.uniform(jax.random.fold_in(jax.random.fold_in(key, 6), dim), (parts,), jnp.float32, low / len(cuts), top_value / len(cuts))
        return jnp.repeat(jnp.exp(steps), extent[dim] // parts).reshape((-1,) + (1,) * (len(extent) - dim - 1))

    factor_of = one(*cuts[0])
    for cut in cuts[1:]:
        factor_of = factor_of * one(*cut)
    return factor_of


def profile(number_of, total, bound, slope):
    weights = [(1 << 20) // math.isqrt(rank ** slope) + 1 for rank in range(2, number_of + 1)]
    spare, given = total - bound - (number_of - 1), [1] * (number_of - 1)
    while spare > 0:
        movable = [i for i in range(number_of - 1) if given[i] < bound]
        mass, remaining = sum([weights[i] for i in movable]), spare
        for i in movable:
            more = min(bound - given[i], max(1, remaining * weights[i] // mass), spare)
            given[i] = given[i] + more
            spare = spare - more
    return np.array([bound] + given)


def uneven_parts(own_key, number_of, total, bound, skew):
    if number_of == 2:
        one = jax.random.randint(own_key, (), max(1, total - bound), min(bound, total - 1) + 1)
        return jnp.stack([one, total - one])
    tallies = jnp.asarray(profile(number_of, total, bound, skew), jnp.int32)
    twos = (number_of - 1) // 2
    giver, receiver = tallies[1:1 + 2 * twos:2], tallies[2:2 + 2 * twos:2]
    margin = jnp.minimum(giver - 1, bound - receiver)
    moved = jax.random.randint(jax.random.fold_in(own_key, 1), (twos,), 0, 1 << 20) % (margin + 1)
    tallies = tallies.at[1:1 + 2 * twos:2].set(giver - moved).at[2:2 + 2 * twos:2].set(receiver + moved)
    return tallies[jax.random.permutation(jax.random.fold_in(own_key, 2), number_of)]


def normal_values(own_key, shape, deviation, most, split=(), kind=jnp.bfloat16):
    result = jax.random.normal(own_key, shape, jnp.float32) * deviation
    if len(split) > 0:
        result = level_of(own_key, shape, split, -0.22, 0.18) * result
    return jnp.clip(result, min=-most, max=most).astype(kind)


def setup_inputs(seed: int = 0) -> dict:
    streams_of = jax.random.split(jax.random.key(seed), 13)
    tokens = normal_values(streams_of[0], (TOKENS, D), 1.0, 6.0, ((0, 8),))
    segments = jax.vmap(lambda own: jnp.searchsorted(jnp.cumsum(uneven_parts(own, max(4, SEQ // 256), SEQ, SEQ // 2, 2)), jnp.arange(SEQ), side="right"))(jax.random.split(streams_of[1], N_DP)).reshape((N_DP, SEQ)).astype(jnp.int32)
    attn_gain = jnp.clip(1.0 + 0.1 * jax.random.normal(streams_of[2], (D,), jnp.float32), 0.5, 1.5)
    query_weight = normal_values(streams_of[3], (D, HEADS * HEAD), D ** -0.5, 0.125, ((1, 4),))
    key_weight = normal_values(streams_of[4], (D, KV_HEADS * HEAD), D ** -0.5, 0.125, ((1, 4),))
    value_weight = normal_values(streams_of[5], (D, KV_HEADS * HEAD), D ** -0.5, 0.125, ((1, 4),))
    output_weight = normal_values(streams_of[6], (HEADS * HEAD, D), (max(1, HEADS * HEAD // 256)) ** -0.5, 2.0, ((0, 4),))
    mlp_gain = jnp.clip(1.0 + 0.1 * jax.random.normal(streams_of[7], (D,), jnp.float32), 0.5, 1.5)
    gate_weight = normal_values(streams_of[8], (D, FF), D ** -0.5, 0.125, ((1, 4),))
    up_weight = normal_values(streams_of[9], (D, FF), D ** -0.5, 0.125, ((1, 4),))
    down_weight = normal_values(streams_of[10], (FF, D), FF ** -0.5, 0.078125, ((0, 4),))
    cotangent = normal_values(streams_of[11], (TOKENS, D), 1.0, 6.0, ((0, 8),))
    return dict(tokens=tokens, segments=segments, attn_gain=attn_gain, query_weight=query_weight, key_weight=key_weight, value_weight=value_weight, output_weight=output_weight, mlp_gain=mlp_gain, gate_weight=gate_weight, up_weight=up_weight, down_weight=down_weight, cotangent=cotangent)


@jax.custom_vjp
def low(v):
    return lax.optimization_barrier(v.astype(jnp.bfloat16)).astype(jnp.float32)

@jax.custom_vjp
def low_back(v):
    return v

def low_keep(v):
    return (low(v), None)

def low_pass(kept, grad):
    return (grad,)

def back_keep(v):
    return (v, None)

def back_low(kept, grad):
    return (low(grad),)
low.defvjp(low_keep, low_pass)
low_back.defvjp(back_keep, back_low)
EPSILON = 1e-05
MASKED = -1000000000.0

def matmul(left_side, right_side):
    return jnp.dot(left_side, right_side, precision=lax.Precision.HIGHEST, preferred_element_type=jnp.float32)

def normalize(values, gain_vec):
    inverse = lax.rsqrt(lax.optimization_barrier(jnp.mean(values * values, axis=-1, keepdims=True)) + EPSILON)
    return values * inverse * gain_vec

def rope_tables(positions, head_width):
    frequency = 10000.0 ** (-jnp.arange(0, head_width, 2, dtype=jnp.float32) / head_width)
    angles = positions.astype(jnp.float32)[:, None] * frequency[None, :]
    cos_table = jnp.concatenate([jnp.cos(angles), jnp.cos(angles)], -1)
    sin_table = jnp.concatenate([jnp.sin(angles), jnp.sin(angles)], -1)
    return (cos_table, sin_table)

def rotate(values, cos_table, sin_table):
    half_width = values.shape[-1] // 2
    turned = jnp.concatenate([-values[..., half_width:], values[..., :half_width]], -1)
    return values * cos_table[:, None, :] + turned * sin_table[:, None, :]

def layer(tokens, attn_gain, query_weight, key_weight, value_weight, output_weight, mlp_gain, gate_weight, up_weight, down_weight, segments):
    length = tokens.shape[0]
    groups = HEADS // KV_HEADS
    positions = jnp.arange(length, dtype=jnp.int32)
    cos_table, sin_table = rope_tables(positions, HEAD)
    attn_in = low(normalize(tokens, attn_gain))
    queries = low_back(matmul(attn_in, query_weight)).reshape(length, HEADS, HEAD)
    keys_pre = low_back(matmul(attn_in, key_weight)).reshape(length, KV_HEADS, HEAD)
    values = low(low_back(matmul(attn_in, value_weight))).reshape(length, KV_HEADS, HEAD)
    queries_rot = low(rotate(queries, cos_table, sin_table)).reshape(length // SPAN, SPAN, KV_HEADS, groups, HEAD)
    keys_rot = low(rotate(keys_pre, cos_table, sin_table))
    score_scale = HEAD ** (-0.5)

    def attend(query_block):
        query_rows, query_segs, query_pos = query_block
        raw_scores = jnp.einsum('bgnd,kgd->gnbk', query_rows, keys_rot, precision=lax.Precision.HIGHEST)
        scores = low_back(raw_scores * score_scale)
        allowed = (query_segs[:, None] == segments[None, :]) & (positions[None, :] <= query_pos[:, None])
        scores = jnp.where(allowed[None, None], scores, MASKED)
        soft_weights = low(jax.nn.softmax(scores, axis=-1))
        return jnp.einsum('gnbk,kgd->bgnd', soft_weights, values, precision=lax.Precision.HIGHEST)
    mixed_heads = lax.map(jax.checkpoint(attend), (queries_rot, segments.reshape(length // SPAN, SPAN), positions.reshape(length // SPAN, SPAN)))
    heads_out = low(low_back(mixed_heads.reshape(length, HEADS * HEAD)))
    branch = low_back(matmul(heads_out, output_weight))
    middle = tokens + branch
    mlp_in = low(normalize(middle, mlp_gain))
    gate_pre = low_back(matmul(mlp_in, gate_weight))
    up_pre = low_back(matmul(mlp_in, up_weight))
    hidden = low(jax.nn.silu(gate_pre) * up_pre)
    return middle + low_back(matmul(hidden, down_weight))

def reference(tokens, segments, attn_gain, query_weight, key_weight, value_weight, output_weight, mlp_gain, gate_weight, up_weight, down_weight, cotangent):
    params = tuple((weight.astype(jnp.float32) for weight in (attn_gain, query_weight, key_weight, value_weight, output_weight, mlp_gain, gate_weight, up_weight, down_weight)))
    stacked = tokens.astype(jnp.float32).reshape(N_DP, SEQ, D)
    cot_stack = cotangent.astype(jnp.float32).reshape(N_DP, SEQ, D)

    def per_sequence(totals, member):
        seq_tokens, seq_cot, seq_segs = member

        def apply_layer(inputs, *weights):
            return layer(inputs, *weights, seq_segs)
        output, pullback = jax.vjp(apply_layer, seq_tokens, *params)
        gradients = pullback(seq_cot)
        summed = tuple((running + gradient for running, gradient in zip(totals, gradients[1:])))
        return (summed, (output, gradients[0]))
    zero_grads = tuple((jnp.zeros_like(weight) for weight in params))
    totals, (outputs, input_grads) = lax.scan(per_sequence, zero_grads, (stacked, cot_stack, segments))
    return (outputs.reshape(TOKENS, D), input_grads.reshape(TOKENS, D), totals[0], totals[1], totals[2], totals[3], totals[4], totals[5], totals[6], totals[7], totals[8])
```

```python
import functools

import jax
import jax.numpy as jnp
from jax import lax
from jax.experimental import pallas as pl
from jax.experimental.pallas import tpu as pltpu
from jax.sharding import PartitionSpec as P

HEAD = 64
EPSILON = 1e-05
MASKED = -1000000000.0
BF = jnp.bfloat16
F32 = jnp.float32
QB = 128


def contract(left_side, right_side, left_dim, right_dim):
    return lax.dot_general(
        left_side,
        right_side,
        (((left_dim,), (right_dim,)), ((), ())),
        preferred_element_type=F32,
    )


def swap(value, axis, mask):
    size = lax.axis_size(axis)
    return lax.ppermute(value, axis, [(i, i ^ mask) for i in range(size)])


def bits_of(axis):
    return [(axis, 1 << k) for k in range((lax.axis_size(axis) - 1).bit_length())]


def rope_tables(positions, head_width):
    frequency = 10000.0 ** (-jnp.arange(0, head_width, 2, dtype=F32) / head_width)
    angles = positions.astype(F32)[:, None] * frequency[None, :]
    cos_half, sin_half = jnp.cos(angles), jnp.sin(angles)
    return (
        jnp.concatenate([cos_half] * 4, -1),
        jnp.concatenate([sin_half] * 4, -1),
    )


def lane_index(shape):
    return lax.broadcasted_iota(jnp.int32, shape, len(shape) - 1)


def turn(values):
    low = lane_index(values.shape) % HEAD < HEAD // 2
    width = values.shape[-1]
    return jnp.where(
        low, -pltpu.roll(values, width - HEAD // 2, 1), pltpu.roll(values, HEAD // 2, 1)
    )


def enter_kernel(x_ref, gain_ref, wq_ref, wkv_ref, cos_ref, sin_ref, a_ref, q_ref, kv_ref):
    x = x_ref[...].astype(F32)
    inverse = lax.rsqrt(jnp.mean(x * x, axis=-1, keepdims=True) + EPSILON)
    a = (x * inverse * gain_ref[...]).astype(BF)
    a_ref[...] = a
    cos, sin = cos_ref[...], sin_ref[...]
    pairs = q_ref.shape[1] // 128
    q = jnp.dot(a, wq_ref[...], preferred_element_type=F32)
    cos_all = jnp.concatenate([cos] * pairs, -1)
    sin_all = jnp.concatenate([sin] * pairs, -1)
    q_rot = (q * cos_all + turn(q) * sin_all).astype(BF)
    q_ref[...] = q_rot * (HEAD**-0.5)
    kv = jnp.dot(a, wkv_ref[...], preferred_element_type=F32)
    is_key = lane_index(kv.shape) < HEAD
    kv_ref[...] = jnp.where(is_key, kv * cos + turn(kv) * sin, kv).astype(BF)


def enter(tokens, gain, wq, wkv, cos, sin):
    rows, d = tokens.shape
    tile = 128
    row = lambda i: (i, 0)
    fixed = lambda i: (0, 0)
    return pl.pallas_call(
        enter_kernel,
        grid=(rows // tile,),
        in_specs=[
            pl.BlockSpec((tile, d), row),
            pl.BlockSpec((1, d), fixed),
            pl.BlockSpec(wq.shape, fixed),
            pl.BlockSpec(wkv.shape, fixed),
            pl.BlockSpec((tile, 128), row),
            pl.BlockSpec((tile, 128), row),
        ],
        out_specs=[
            pl.BlockSpec((tile, d), row),
            pl.BlockSpec((tile, wq.shape[1]), row),
            pl.BlockSpec((tile, 128), row),
        ],
        out_shape=[
            jax.ShapeDtypeStruct((rows, d), BF),
            jax.ShapeDtypeStruct((rows, wq.shape[1]), BF),
            jax.ShapeDtypeStruct((rows, 128), BF),
        ],
        name="enter",
    )(tokens, gain, wq, wkv, cos, sin)


def lay_keys(ctx, kv_ref, k_refs, v_refs):
    count, rows, _ = kv_ref.shape
    for j in range(count):
        kv = kv_ref[j].astype(F32)
        other = pltpu.roll(kv, HEAD, 1)
        low = lane_index(kv.shape) < HEAD
        at = pl.ds(pl.multiple_of((ctx ^ j) * rows, rows), rows)
        k_refs[0][at, :] = jnp.where(low, kv, 0.0).astype(BF)
        k_refs[1][at, :] = jnp.where(low, 0.0, other).astype(BF)
        v_refs[0][at, :] = jnp.where(low, other, 0.0).astype(BF)
        v_refs[1][at, :] = jnp.where(low, 0.0, kv).astype(BF)


def mask_of(ctx, block, rows, window, segc_ref, segr_ref, pairs):
    first_q = ctx * rows + block * QB
    start = pl.multiple_of(jnp.maximum(first_q + QB - window, 0), QB)
    key_seg = segc_ref[pl.ds(start, window), :]
    query_seg = segr_ref[:, pl.ds(pl.multiple_of(first_q, QB), QB)]
    key_pos = start + lax.broadcasted_iota(jnp.int32, (window, QB), 0)
    query_pos = first_q + lax.broadcasted_iota(jnp.int32, (window, QB), 1)
    bias = jnp.where((key_seg == query_seg) & (key_pos <= query_pos), 0.0, MASKED)
    return start, jnp.concatenate([bias] * pairs, -1)


def stack_pairs(ref, at, pairs):
    return jnp.concatenate([ref[at, 128 * g : 128 * (g + 1)] for g in range(pairs)], 0)


def forward_kernel(q_ref, kv_ref, segc_ref, segr_ref, o_ref, lse_ref, k0, k1, v0, v1, *, window):
    rows = q_ref.shape[0]
    pairs = q_ref.shape[1] // 128
    ctx = lax.axis_index("ctx")
    k_refs, v_refs = (k0, k1), (v0, v1)
    lay_keys(ctx, kv_ref, k_refs, v_refs)

    def body(block, carry):
        start, bias = mask_of(ctx, block, rows, window, segc_ref, segr_ref, pairs)
        at = pl.ds(pl.multiple_of(block * QB, QB), QB)
        keys_at = pl.ds(start, window)
        queries = stack_pairs(q_ref, at, pairs)
        mixed = None
        for parity in range(2):
            scores = contract(k_refs[parity][keys_at, :], queries, 1, 1) + bias
            top = jnp.max(scores, axis=0, keepdims=True)
            weights = jnp.exp(scores - top)
            total = jnp.sum(weights, axis=0, keepdims=True)
            lse_ref[pl.ds(block * 2 + parity, 1), :] = top + jnp.log(total)
            part = contract(v_refs[parity][keys_at, :], weights.astype(BF), 0, 0) / total
            mixed = part if mixed is None else mixed + part
        mixed = mixed.T.astype(BF)
        for g in range(pairs):
            o_ref[at, 128 * g : 128 * (g + 1)] = mixed[QB * g : QB * (g + 1), :]
        return carry

    lax.fori_loop(0, rows // QB, body, 0)


def attend(q, kv, seg_col, seg_row, window):
    rows, width = q.shape
    count = kv.shape[0]
    pairs = width // 128
    return pl.pallas_call(
        functools.partial(forward_kernel, window=window),
        out_shape=[
            jax.ShapeDtypeStruct((rows, width), BF),
            jax.ShapeDtypeStruct((rows // QB * 2, QB * pairs), F32),
        ],
        in_specs=[pl.BlockSpec(memory_space=pltpu.VMEM)] * 4,
        out_specs=[pl.BlockSpec(memory_space=pltpu.VMEM)] * 2,
        scratch_shapes=[pltpu.VMEM((count * rows, 128), BF)] * 4,
        name="attend",
    )(q, kv, seg_col, seg_row)


def backward_kernel(
    q_ref,
    hb_ref,
    kv_ref,
    lse_ref,
    segc_ref,
    segr_ref,
    cos_ref,
    sin_ref,
    qb_ref,
    own_ref,
    far_ref,
    k0,
    k1,
    v0,
    v1,
    dk,
    dv,
    *,
    window,
):
    rows = q_ref.shape[0]
    pairs = q_ref.shape[1] // 128
    count = kv_ref.shape[0]
    ctx = lax.axis_index("ctx")
    core = lax.rem(lax.axis_index("tp"), 2)
    k_refs, v_refs = (k0, k1), (v0, v1)
    lay_keys(ctx, kv_ref, k_refs, v_refs)
    dk[...] = jnp.zeros_like(dk)
    dv[...] = jnp.zeros_like(dv)
    half_blocks = rows // QB // 2

    def body(block, carry):
        start, bias = mask_of(ctx, block, rows, window, segc_ref, segr_ref, pairs)
        at = pl.ds(pl.multiple_of(block * QB, QB), QB)
        keys_at = pl.ds(start, window)
        queries = stack_pairs(q_ref, at, pairs)
        swapped = lax.rem(block + core * half_blocks, 2 * half_blocks)
        backs = stack_pairs(hb_ref, pl.ds(pl.multiple_of(swapped * QB, QB), QB), pairs)
        low = lane_index(queries.shape) < HEAD
        zero = jnp.zeros_like(queries)
        dq = None
        for parity in range(2):
            keep = low if parity == 0 else jnp.logical_not(low)
            keys = k_refs[parity][keys_at, :]
            scores = contract(keys, queries, 1, 1) + bias
            weights = jnp.exp(scores - lse_ref[pl.ds(block * 2 + parity, 1), :])
            back = contract(v_refs[parity][keys_at, :], backs, 1, 1)
            delta = jnp.sum(weights * back, axis=0, keepdims=True)
            score_back = (weights * (back - delta)).astype(BF)
            part = contract(keys, score_back, 0, 0)
            dq = part if dq is None else dq + part
            dk[keys_at, :] += contract(score_back, jnp.where(keep, queries, zero), 1, 0)
            dv[keys_at, :] += contract(weights.astype(BF), jnp.where(keep, backs, zero), 1, 0)
        dq = dq.T * (HEAD**-0.5)
        cos, sin = cos_ref[at, :], sin_ref[at, :]
        for g in range(pairs):
            piece = dq[QB * g : QB * (g + 1), :]
            qb_ref[at, 128 * g : 128 * (g + 1)] = (piece * cos - turn(piece * sin)).astype(BF)
        return carry

    lax.fori_loop(0, rows // QB, body, 0)
    for j in range(count):
        at = pl.ds(pl.multiple_of((ctx ^ j) * rows, rows), rows)
        a, b = dk[at, :], dv[at, :]
        low = lane_index(a.shape) < HEAD
        both = jnp.where(low, a + pltpu.roll(a, HEAD, 1), b + pltpu.roll(b, HEAD, 1))
        if j == 0:
            own_ref[...] = both
        else:
            far_ref[j - 1] = both.astype(BF)


def attend_back(q, hb, kv, lse, seg_col, seg_row, cos, sin, window):
    rows, width = q.shape
    count = kv.shape[0]
    return pl.pallas_call(
        functools.partial(backward_kernel, window=window),
        out_shape=[
            jax.ShapeDtypeStruct((rows, width), BF),
            jax.ShapeDtypeStruct((rows, 128), F32),
            jax.ShapeDtypeStruct((count - 1, rows, 128), BF),
        ],
        in_specs=[pl.BlockSpec(memory_space=pltpu.VMEM)] * 8,
        out_specs=[pl.BlockSpec(memory_space=pltpu.VMEM)] * 3,
        scratch_shapes=[pltpu.VMEM((count * rows, 128), BF)] * 4
        + [pltpu.VMEM((count * rows, 128), F32)] * 2,
        name="attend_back",
    )(q, hb, kv, lse, seg_col, seg_row, cos, sin)


def join_kernel(*refs):
    own_ref, cos_ref, sin_ref = refs[0], refs[-3], refs[-2]
    out_ref = refs[-1]
    total = own_ref[...]
    for ref in refs[1:-3]:
        total = total + ref[...].astype(F32)
    is_key = lane_index(total.shape) < HEAD
    turned = total * cos_ref[...] - turn(total * sin_ref[...])
    out_ref[...] = jnp.where(is_key, turned, total).astype(BF)


def join_keys(own, far, cos, sin):
    return pl.pallas_call(
        join_kernel,
        out_shape=jax.ShapeDtypeStruct(own.shape, BF),
        name="join_keys",
    )(own, *far, cos, sin)


def hidden_kernel(m_ref, hb_ref, wg_ref, wu_ref, h_ref, gb_ref, ub_ref):
    m = m_ref[...]
    width = wg_ref.shape[1]
    step = 256

    def chunk(at):
        gate = jnp.dot(m, wg_ref[:, at], preferred_element_type=F32)
        up = jnp.dot(m, wu_ref[:, at], preferred_element_type=F32)
        back = hb_ref[:, at]
        sig = jax.nn.sigmoid(gate)
        silu = gate * sig
        h_ref[:, at] = (silu * up).astype(BF)
        gb_ref[:, at] = (back * up * sig * (1.0 + gate * (1.0 - sig))).astype(BF)
        ub_ref[:, at] = (back * silu).astype(BF)

    def body(i, carry):
        chunk(pl.ds(pl.multiple_of(i * step, step), step))
        return carry

    lax.fori_loop(0, width // step, body, 0)
    if width % step:
        chunk(pl.ds(width // step * step, width % step))


def hidden_parts(m, hb, wg, wu):
    rows, d = m.shape
    width = wg.shape[1]
    tile = 256
    row = lambda i: (i, 0)
    fixed = lambda i: (0, 0)
    out = jax.ShapeDtypeStruct((rows, width), BF)
    return pl.pallas_call(
        hidden_kernel,
        grid=(rows // tile,),
        in_specs=[
            pl.BlockSpec((tile, d), row),
            pl.BlockSpec((tile, width), row),
            pl.BlockSpec(wg.shape, fixed, pipeline_mode=pl.Buffered(1)),
            pl.BlockSpec(wu.shape, fixed, pipeline_mode=pl.Buffered(1)),
        ],
        out_specs=[pl.BlockSpec((tile, width), row)] * 3,
        out_shape=[out] * 3,
        compiler_params=pltpu.CompilerParams(vmem_limit_bytes=48 << 20),
        cost_estimate=pl.CostEstimate(
            flops=4 * rows * d * width,
            bytes_accessed=4 * d * width + 2 * rows * d + 10 * rows * width,
            transcendentals=rows * width,
        ),
        name="hidden_parts",
    )(m, hb, wg, wu)


def shards(
    tokens,
    segments,
    attn_gain,
    query_weight,
    key_weight,
    value_weight,
    output_weight,
    mlp_gain,
    gate_weight,
    up_weight,
    down_weight,
    cotangent,
):
    rows, d = tokens.shape
    half = rows // 2
    seq = segments.shape[1]
    window = min(seq, seq // 2 + QB)
    ctx, dp = lax.axis_index("ctx"), lax.axis_index("dp")
    n_ctx, n_dp = lax.axis_size("ctx"), lax.axis_size("dp")
    core = lax.rem(lax.axis_index("tp"), 2)
    tp_rest = bits_of("tp")[1:]
    block_width = d // (n_ctx * n_dp)
    every_bit = bits_of("ctx") + bits_of("dp")
    mlp_share = [("ctx", 1), ("dp", 1)]
    attn_share = [("ctx", 1)]
    mlp_reduce = [b for b in every_bit if b not in mlp_share]
    attn_reduce = [b for b in every_bit if b not in attn_share]

    def owner_offsets(reduce_bits):
        found = [[]]
        for bit in reduce_bits:
            found = [f for f in found] + []
        result = []
        for code in range(1 << len(reduce_bits)):
            chosen = [
                reduce_bits[i]
                for i in range(len(reduce_bits))
                if code >> (len(reduce_bits) - 1 - i) & 1
            ]
            result.append(chosen)
        return result

    def owner_start(chosen, flip=()):
        other_dp, other_ctx = dp, ctx
        for axis, mask in list(chosen) + list(flip):
            if axis == "dp":
                other_dp = other_dp ^ mask
            else:
                other_ctx = other_ctx ^ mask
        return (other_dp * n_ctx + other_ctx) * block_width

    def columns(value, chosen, flip=()):
        return lax.dynamic_slice_in_dim(value, owner_start(chosen, flip), block_width, 1)

    def all_columns(value, reduce_bits, flip=()):
        return jnp.concatenate(
            [columns(value, chosen, flip) for chosen in owner_offsets(reduce_bits)], 1
        )

    def own_half(value):
        return lax.dynamic_slice_in_dim(value, core * half, half, 0)

    def other_half(value):
        return lax.dynamic_slice_in_dim(value, (1 - core) * half, half, 0)

    def both_halves(value):
        return jnp.concatenate([own_half(value), other_half(value)], 0)

    def join_cores(value):
        return jnp.concatenate([value, swap(value, "tp", 1)], 0)

    def share(value, bits):
        pieces = [value]
        for axis, mask in bits:
            pieces = pieces + [swap(piece, axis, mask) for piece in pieces]
        return join_cores(jnp.concatenate(pieces[1:], 0))

    def tp_sum(send, keep):
        total = keep + swap(send.astype(BF), "tp", 1).astype(F32)
        for axis, mask in tp_rest:
            low = total.astype(BF)
            total = low.astype(F32) + swap(low, axis, mask).astype(F32)
        return total

    def reduce_blocks(value, reduce_bits, dim):
        for axis, mask in reduce_bits:
            middle = value.shape[dim] // 2
            keep = lax.slice_in_dim(value, 0, middle, axis=dim)
            send = lax.slice_in_dim(value, middle, 2 * middle, axis=dim).astype(BF)
            value = keep + swap(send, axis, mask).astype(F32)
        return value

    def sum_gain(value):
        value = value + swap(value, "tp", 1)
        for axis, mask in every_bit:
            value = value + swap(value, axis, mask)
        return lax.dynamic_slice_in_dim(value, owner_start(()), block_width, 0)

    seg_row = segments
    seg_col = jnp.swapaxes(segments, 0, 1)
    query_pos = ctx * rows + jnp.arange(rows, dtype=jnp.int32)
    cos_table, sin_table = rope_tables(query_pos, HEAD)
    kv_weight = jnp.concatenate([key_weight, value_weight], 1)
    cot_half = own_half(cotangent)
    cot_own = jnp.concatenate([cot_half, other_half(cotangent)], 0)
    cot_far = share(cot_half, mlp_share)
    x_half = own_half(tokens).astype(F32)

    attn_in, q_rot, kv_own = enter(
        tokens, attn_gain[None], query_weight, kv_weight, cos_table, sin_table
    )
    kv_parts = [kv_own]
    for axis, mask in bits_of("ctx"):
        kv_parts = kv_parts + [swap(piece, axis, mask) for piece in kv_parts]
    kv_all = jnp.stack(kv_parts, 0)
    heads_out, lse = attend(q_rot, kv_all, seg_col, seg_row, window)
    heads_mine, heads_other = own_half(heads_out), other_half(heads_out)
    middle = x_half + tp_sum(
        contract(heads_other, output_weight, 1, 0), contract(heads_mine, output_weight, 1, 0)
    )
    inverse_two = lax.rsqrt(jnp.mean(middle * middle, axis=-1, keepdims=True) + EPSILON)
    normed_two = middle * inverse_two
    mlp_half = (normed_two * mlp_gain).astype(BF)
    mlp_own = join_cores(mlp_half)
    mlp_far = share(mlp_half, mlp_share)

    back_own = contract(cot_own, down_weight, 1, 1)
    back_far = contract(cot_far, down_weight, 1, 1)
    hidden_own, gate_own, up_own = hidden_parts(mlp_own, back_own, gate_weight, up_weight)

    def mlp_back(at):
        return contract(gate_own[at], gate_weight, 1, 1) + contract(up_own[at], up_weight, 1, 1)

    mlp_in_back = tp_sum(mlp_back(slice(half, rows)), mlp_back(slice(0, half)))
    scaled = mlp_in_back * mlp_gain
    middle_back = cot_half.astype(F32) + inverse_two * (
        scaled - normed_two * jnp.mean(scaled * normed_two, axis=-1, keepdims=True)
    )
    mlp_gain_grad = sum_gain(jnp.sum(mlp_in_back * normed_two, axis=0))
    branch_half = middle_back.astype(BF)
    branch_own = join_cores(branch_half)
    heads_back = contract(branch_own, output_weight, 1, 1).astype(BF)

    out_half = middle + tp_sum(
        contract(hidden_own[half:], down_weight, 1, 0),
        contract(hidden_own[:half], down_weight, 1, 0),
    )

    def whole_rows(value):
        far = swap(value, "tp", 1)
        first = jnp.where(core == 0, value, far)
        second = jnp.where(core == 0, far, value)
        return jnp.concatenate([first, second], 0)

    layer_out = whole_rows(out_half)

    hidden_far, gate_far, up_far = hidden_parts(mlp_far, back_far, gate_weight, up_weight)
    mlp_cols = all_columns(mlp_own, mlp_reduce), all_columns(mlp_far, mlp_reduce)
    cot_cols = all_columns(cot_own, mlp_reduce), all_columns(cot_far, mlp_reduce)

    down_grad = reduce_blocks(
        contract(hidden_own, cot_cols[0], 0, 0) + contract(hidden_far, cot_cols[1], 0, 0),
        mlp_reduce,
        1,
    )
    gate_grad = reduce_blocks(
        contract(mlp_cols[0], gate_own, 0, 0) + contract(mlp_cols[1], gate_far, 0, 0),
        mlp_reduce,
        0,
    )
    up_grad = reduce_blocks(
        contract(mlp_cols[0], up_own, 0, 0) + contract(mlp_cols[1], up_far, 0, 0),
        mlp_reduce,
        0,
    )

    query_back, kv_part, kv_far = attend_back(
        q_rot, heads_back, kv_all, lse, seg_col, seg_row, cos_table, sin_table, window
    )
    kv_back = join_keys(
        kv_part,
        [swap_to(kv_far[j - 1], j) for j in range(1, n_ctx)],
        cos_table,
        sin_table,
    )
    qkv_back = jnp.concatenate([query_back, kv_back], 1)
    back_mine, back_other = own_half(qkv_back), other_half(qkv_back)
    q_width = query_back.shape[1]

    def attn_back(part):
        return contract(part[:, :q_width], query_weight, 1, 1) + contract(
            part[:, q_width:], kv_weight, 1, 1
        )

    attn_in_back = tp_sum(attn_back(back_other), attn_back(back_mine))
    inverse_one = lax.rsqrt(jnp.mean(x_half * x_half, axis=-1, keepdims=True) + EPSILON)
    normed_one = x_half * inverse_one
    scaled_one = attn_in_back * attn_gain
    tokens_half = middle_back + inverse_one * (
        scaled_one - normed_one * jnp.mean(scaled_one * normed_one, axis=-1, keepdims=True)
    )
    tokens_grad = whole_rows(tokens_half)
    attn_gain_grad = sum_gain(jnp.sum(attn_in_back * normed_one, axis=0))

    flip = attn_share
    attn_cols = both_halves(all_columns(attn_in, attn_reduce))
    attn_cols_far = share(own_half(all_columns(attn_in, attn_reduce, flip)), attn_share)
    heads_rel = jnp.concatenate([heads_mine, heads_other], 0)
    heads_far = swap(heads_rel, *attn_share[0])
    branch_cols = all_columns(branch_own, attn_reduce)
    branch_cols_far = share(all_columns(branch_half, attn_reduce, flip), attn_share)
    back_rel = jnp.concatenate([back_mine, back_other], 0)
    back_far_rel = swap(back_rel, *attn_share[0])
    output_grad = reduce_blocks(
        contract(heads_rel, branch_cols, 0, 0) + contract(heads_far, branch_cols_far, 0, 0),
        attn_reduce,
        1,
    )
    qkv_grad = reduce_blocks(
        contract(attn_cols, back_rel, 0, 0) + contract(attn_cols_far, back_far_rel, 0, 0),
        attn_reduce,
        0,
    )
    return (
        layer_out,
        tokens_grad,
        attn_gain_grad,
        qkv_grad[:, :q_width],
        qkv_grad[:, q_width : q_width + HEAD],
        qkv_grad[:, q_width + HEAD :],
        output_grad,
        mlp_gain_grad,
        gate_grad,
        up_grad,
        down_grad,
    )


def swap_to(value, mask):
    return swap(value, "ctx", mask)


def solution(mesh):
    return jax.shard_map(
        shards,
        mesh=mesh,
        in_specs=(
            P(("dp", "ctx"), None),
            P("dp", None),
            P(),
            P(None, "tp"),
            P(None, "tp"),
            P(None, "tp"),
            P("tp", None),
            P(),
            P(None, "tp"),
            P(None, "tp"),
            P("tp", None),
            P(("dp", "ctx"), None),
        ),
        out_specs=(
            P(("dp", "ctx"), None),
            P(("dp", "ctx"), None),
            P(("dp", "ctx")),
            P(("dp", "ctx"), "tp"),
            P(("dp", "ctx"), "tp"),
            P(("dp", "ctx"), "tp"),
            P("tp", ("dp", "ctx")),
            P(("dp", "ctx")),
            P(("dp", "ctx"), "tp"),
            P(("dp", "ctx"), "tp"),
            P("tp", ("dp", "ctx")),
        ),
        check_vma=False,
    )
```

```python
import functools

import jax
import jax.numpy as jnp
from jax import lax
from jax.experimental import pallas as pl
from jax.experimental.pallas import tpu as pltpu
from jax.sharding import PartitionSpec as P

HEAD = 64
EPSILON = 1e-05
MASKED = -1000000000.0
BF = jnp.bfloat16
F32 = jnp.float32
QB = 128


def contract(left_side, right_side, left_dim, right_dim):
    return lax.dot_general(
        left_side,
        right_side,
        (((left_dim,), (right_dim,)), ((), ())),
        preferred_element_type=F32,
    )


def swap(value, axis, mask):
    size = lax.axis_size(axis)
    return lax.ppermute(value, axis, [(i, i ^ mask) for i in range(size)])


def bits_of(axis):
    return [(axis, 1 << k) for k in range((lax.axis_size(axis) - 1).bit_length())]


def rope_tables(positions, head_width):
    frequency = 10000.0 ** (-jnp.arange(0, head_width, 2, dtype=F32) / head_width)
    angles = positions.astype(F32)[:, None] * frequency[None, :]
    cos_half, sin_half = jnp.cos(angles), jnp.sin(angles)
    return (
        jnp.concatenate([cos_half] * 4, -1),
        jnp.concatenate([sin_half] * 4, -1),
    )


def lane_index(shape):
    return lax.broadcasted_iota(jnp.int32, shape, len(shape) - 1)


def turn(values):
    low = lane_index(values.shape) % HEAD < HEAD // 2
    width = values.shape[-1]
    return jnp.where(
        low, -pltpu.roll(values, width - HEAD // 2, 1), pltpu.roll(values, HEAD // 2, 1)
    )


def enter_kernel(x_ref, gain_ref, wq_ref, wkv_ref, cos_ref, sin_ref, a_ref, q_ref, kv_ref):
    x = x_ref[...].astype(F32)
    inverse = lax.rsqrt(jnp.mean(x * x, axis=-1, keepdims=True) + EPSILON)
    a = (x * inverse * gain_ref[...]).astype(BF)
    a_ref[...] = a
    cos, sin = cos_ref[...], sin_ref[...]
    pairs = q_ref.shape[1] // 128
    q = jnp.dot(a, wq_ref[...], preferred_element_type=F32)
    cos_all = jnp.concatenate([cos] * pairs, -1)
    sin_all = jnp.concatenate([sin] * pairs, -1)
    q_rot = (q * cos_all + turn(q) * sin_all).astype(BF)
    q_ref[...] = q_rot * (HEAD**-0.5)
    kv = jnp.dot(a, wkv_ref[...], preferred_element_type=F32)
    is_key = lane_index(kv.shape) < HEAD
    kv_ref[...] = jnp.where(is_key, kv * cos + turn(kv) * sin, kv).astype(BF)


def enter(tokens, gain, wq, wkv, cos, sin):
    rows, d = tokens.shape
    tile = 128
    row = lambda i: (i, 0)
    fixed = lambda i: (0, 0)
    return pl.pallas_call(
        enter_kernel,
        grid=(rows // tile,),
        in_specs=[
            pl.BlockSpec((tile, d), row),
            pl.BlockSpec((1, d), fixed),
            pl.BlockSpec(wq.shape, fixed),
            pl.BlockSpec(wkv.shape, fixed),
            pl.BlockSpec((tile, 128), row),
            pl.BlockSpec((tile, 128), row),
        ],
        out_specs=[
            pl.BlockSpec((tile, d), row),
            pl.BlockSpec((tile, wq.shape[1]), row),
            pl.BlockSpec((tile, 128), row),
        ],
        out_shape=[
            jax.ShapeDtypeStruct((rows, d), BF),
            jax.ShapeDtypeStruct((rows, wq.shape[1]), BF),
            jax.ShapeDtypeStruct((rows, 128), BF),
        ],
        name="enter",
    )(tokens, gain, wq, wkv, cos, sin)


def lay_keys(ctx, kv_ref, k_refs, v_refs):
    count, rows, _ = kv_ref.shape
    for j in range(count):
        kv = kv_ref[j].astype(F32)
        other = pltpu.roll(kv, HEAD, 1)
        low = lane_index(kv.shape) < HEAD
        at = pl.ds(pl.multiple_of((ctx ^ j) * rows, rows), rows)
        k_refs[0][at, :] = jnp.where(low, kv, 0.0).astype(BF)
        k_refs[1][at, :] = jnp.where(low, 0.0, other).astype(BF)
        v_refs[0][at, :] = jnp.where(low, other, 0.0).astype(BF)
        v_refs[1][at, :] = jnp.where(low, 0.0, kv).astype(BF)


def mask_of(ctx, block, rows, window, segc_ref, segr_ref, pairs):
    first_q = ctx * rows + block * QB
    start = pl.multiple_of(jnp.maximum(first_q + QB - window, 0), QB)
    key_seg = segc_ref[pl.ds(start, window), :]
    query_seg = segr_ref[:, pl.ds(pl.multiple_of(first_q, QB), QB)]
    key_pos = start + lax.broadcasted_iota(jnp.int32, (window, QB), 0)
    query_pos = first_q + lax.broadcasted_iota(jnp.int32, (window, QB), 1)
    bias = jnp.where((key_seg == query_seg) & (key_pos <= query_pos), 0.0, MASKED)
    return start, jnp.concatenate([bias] * pairs, -1)


def stack_pairs(ref, at, pairs):
    return jnp.concatenate([ref[at, 128 * g : 128 * (g + 1)] for g in range(pairs)], 0)


def forward_kernel(q_ref, kv_ref, segc_ref, segr_ref, o_ref, lse_ref, k0, k1, v0, v1, *, window):
    rows = q_ref.shape[0]
    pairs = q_ref.shape[1] // 128
    ctx = lax.axis_index("ctx")
    k_refs, v_refs = (k0, k1), (v0, v1)
    lay_keys(ctx, kv_ref, k_refs, v_refs)

    def body(block, carry):
        start, bias = mask_of(ctx, block, rows, window, segc_ref, segr_ref, pairs)
        at = pl.ds(pl.multiple_of(block * QB, QB), QB)
        keys_at = pl.ds(start, window)
        queries = stack_pairs(q_ref, at, pairs)
        mixed = None
        for parity in range(2):
            scores = contract(k_refs[parity][keys_at, :], queries, 1, 1) + bias
            top = jnp.max(scores, axis=0, keepdims=True)
            weights = jnp.exp(scores - top)
            total = jnp.sum(weights, axis=0, keepdims=True)
            lse_ref[pl.ds(block * 2 + parity, 1), :] = top + jnp.log(total)
            part = contract(v_refs[parity][keys_at, :], weights.astype(BF), 0, 0) / total
            mixed = part if mixed is None else mixed + part
        mixed = mixed.T.astype(BF)
        for g in range(pairs):
            o_ref[at, 128 * g : 128 * (g + 1)] = mixed[QB * g : QB * (g + 1), :]
        return carry

    lax.fori_loop(0, rows // QB, body, 0)


def attend(q, kv, seg_col, seg_row, window):
    rows, width = q.shape
    count = kv.shape[0]
    pairs = width // 128
    return pl.pallas_call(
        functools.partial(forward_kernel, window=window),
        out_shape=[
            jax.ShapeDtypeStruct((rows, width), BF),
            jax.ShapeDtypeStruct((rows // QB * 2, QB * pairs), F32),
        ],
        in_specs=[pl.BlockSpec(memory_space=pltpu.VMEM)] * 4,
        out_specs=[pl.BlockSpec(memory_space=pltpu.VMEM)] * 2,
        scratch_shapes=[pltpu.VMEM((count * rows, 128), BF)] * 4,
        name="attend",
    )(q, kv, seg_col, seg_row)


def backward_kernel(
    q_ref,
    hb_ref,
    kv_ref,
    lse_ref,
    segc_ref,
    segr_ref,
    cos_ref,
    sin_ref,
    qb_ref,
    own_ref,
    far_ref,
    k0,
    k1,
    v0,
    v1,
    dk,
    dv,
    *,
    window,
):
    rows = q_ref.shape[0]
    pairs = q_ref.shape[1] // 128
    count = kv_ref.shape[0]
    ctx = lax.axis_index("ctx")
    core = lax.rem(lax.axis_index("tp"), 2)
    k_refs, v_refs = (k0, k1), (v0, v1)
    lay_keys(ctx, kv_ref, k_refs, v_refs)
    dk[...] = jnp.zeros_like(dk)
    dv[...] = jnp.zeros_like(dv)
    half_blocks = rows // QB // 2

    def body(block, carry):
        start, bias = mask_of(ctx, block, rows, window, segc_ref, segr_ref, pairs)
        at = pl.ds(pl.multiple_of(block * QB, QB), QB)
        keys_at = pl.ds(start, window)
        queries = stack_pairs(q_ref, at, pairs)
        swapped = lax.rem(block + core * half_blocks, 2 * half_blocks)
        backs = stack_pairs(hb_ref, pl.ds(pl.multiple_of(swapped * QB, QB), QB), pairs)
        low = lane_index(queries.shape) < HEAD
        zero = jnp.zeros_like(queries)
        dq = None
        for parity in range(2):
            keep = low if parity == 0 else jnp.logical_not(low)
            keys = k_refs[parity][keys_at, :]
            scores = contract(keys, queries, 1, 1) + bias
            weights = jnp.exp(scores - lse_ref[pl.ds(block * 2 + parity, 1), :])
            back = contract(v_refs[parity][keys_at, :], backs, 1, 1)
            delta = jnp.sum(weights * back, axis=0, keepdims=True)
            score_back = (weights * (back - delta)).astype(BF)
            part = contract(keys, score_back, 0, 0)
            dq = part if dq is None else dq + part
            dk[keys_at, :] += contract(score_back, jnp.where(keep, queries, zero), 1, 0)
            dv[keys_at, :] += contract(weights.astype(BF), jnp.where(keep, backs, zero), 1, 0)
        dq = dq.T * (HEAD**-0.5)
        cos, sin = cos_ref[at, :], sin_ref[at, :]
        for g in range(pairs):
            piece = dq[QB * g : QB * (g + 1), :]
            qb_ref[at, 128 * g : 128 * (g + 1)] = (piece * cos - turn(piece * sin)).astype(BF)
        return carry

    lax.fori_loop(0, rows // QB, body, 0)
    for j in range(count):
        at = pl.ds(pl.multiple_of((ctx ^ j) * rows, rows), rows)
        a, b = dk[at, :], dv[at, :]
        low = lane_index(a.shape) < HEAD
        both = jnp.where(low, a + pltpu.roll(a, HEAD, 1), b + pltpu.roll(b, HEAD, 1))
        if j == 0:
            own_ref[...] = both
        else:
            far_ref[j - 1] = both.astype(BF)


def attend_back(q, hb, kv, lse, seg_col, seg_row, cos, sin, window):
    rows, width = q.shape
    count = kv.shape[0]
    return pl.pallas_call(
        functools.partial(backward_kernel, window=window),
        out_shape=[
            jax.ShapeDtypeStruct((rows, width), BF),
            jax.ShapeDtypeStruct((rows, 128), F32),
            jax.ShapeDtypeStruct((count - 1, rows, 128), BF),
        ],
        in_specs=[pl.BlockSpec(memory_space=pltpu.VMEM)] * 8,
        out_specs=[pl.BlockSpec(memory_space=pltpu.VMEM)] * 3,
        scratch_shapes=[pltpu.VMEM((count * rows, 128), BF)] * 4
        + [pltpu.VMEM((count * rows, 128), F32)] * 2,
        name="attend_back",
    )(q, hb, kv, lse, seg_col, seg_row, cos, sin)


def join_kernel(*refs):
    own_ref, cos_ref, sin_ref = refs[0], refs[-3], refs[-2]
    out_ref = refs[-1]
    total = own_ref[...]
    for ref in refs[1:-3]:
        total = total + ref[...].astype(F32)
    is_key = lane_index(total.shape) < HEAD
    turned = total * cos_ref[...] - turn(total * sin_ref[...])
    out_ref[...] = jnp.where(is_key, turned, total).astype(BF)


def join_keys(own, far, cos, sin):
    return pl.pallas_call(
        join_kernel,
        out_shape=jax.ShapeDtypeStruct(own.shape, BF),
        name="join_keys",
    )(own, *far, cos, sin)


STEP = 256


def gated(m, cot, wg, wu, wd):
    gate = contract(m, wg, 1, 0)
    up = contract(m, wu, 1, 0)
    back = contract(cot, wd, 1, 1)
    sig = 0.5 * jnp.tanh(0.5 * gate) + 0.5
    silu = gate * sig
    return (
        (silu * up).astype(BF),
        (back * up * (sig + silu * (1.0 - sig))).astype(BF),
        (back * silu).astype(BF),
    )


def own_kernel(
    m_ref,
    c_ref,
    wg_hbm,
    wu_hbm,
    wd_hbm,
    h_ref,
    gb_ref,
    ub_ref,
    send_ref,
    keep_ref,
    wg_ref,
    wu_ref,
    wd_ref,
    sems,
    *,
    tile,
):
    rows, d = m_ref.shape
    half = rows // 2
    width = wg_ref.shape[1]
    full, tail = divmod(width, STEP)

    def span(c, w):
        return pl.ds(c * STEP if isinstance(c, int) else pl.multiple_of(c * STEP, STEP), w)

    def copies(c, w):
        at = span(c, w)
        return [
            pltpu.make_async_copy(wg_hbm.at[:, at], wg_ref.at[:, at], sems.at[0, c]),
            pltpu.make_async_copy(wu_hbm.at[:, at], wu_ref.at[:, at], sems.at[1, c]),
            pltpu.make_async_copy(wd_hbm.at[at, :], wd_ref.at[at, :], sems.at[2, c]),
        ]

    for c in range(full + (1 if tail else 0)):
        for copy in copies(c, STEP if c < full else tail):
            copy.start()

    def chunk(c, w):
        for copy in copies(c, w):
            copy.wait()
        at = span(c, w)
        wg, wu, wd = wg_ref[:, at], wu_ref[:, at], wd_ref[at, :]
        for t in range(rows // tile):
            r = slice(t * tile, (t + 1) * tile)
            h, gb, ub = gated(m_ref[r, :], c_ref[r, :], wg, wu, wd)
            h_ref[r, at] = h
            gb_ref[r, at] = gb
            ub_ref[r, at] = ub

    def chunk_step(c, carry):
        chunk(c, STEP)
        return carry

    lax.fori_loop(0, full, chunk_step, 0)
    if tail:
        chunk(full, tail)

    def back_step(i, carry):
        at = span(i, STEP)
        wg, wu = wg_ref[at, :], wu_ref[at, :]
        for t in range(rows // tile):
            r = slice(t * tile, (t + 1) * tile)
            part = contract(gb_ref[r, :], wg, 1, 1) + contract(ub_ref[r, :], wu, 1, 1)
            if t * tile < half:
                keep_ref[r, at] = part
            else:
                send_ref[t * tile - half : (t + 1) * tile - half, at] = part.astype(BF)
        return carry

    lax.fori_loop(0, d // STEP, back_step, 0)


def own_rows(m, cot, wg, wu, wd):
    rows, d = m.shape
    width = wg.shape[1]
    out = jax.ShapeDtypeStruct((rows, width), BF)
    vmem = pl.BlockSpec(memory_space=pltpu.VMEM)
    hbm = pl.BlockSpec(memory_space=pl.ANY)
    return pl.pallas_call(
        functools.partial(own_kernel, tile=256),
        in_specs=[vmem, vmem, hbm, hbm, hbm],
        out_specs=[vmem] * 5,
        out_shape=[out] * 3
        + [jax.ShapeDtypeStruct((rows // 2, d), BF), jax.ShapeDtypeStruct((rows // 2, d), F32)],
        scratch_shapes=[pltpu.VMEM((d, width), BF)] * 2
        + [pltpu.VMEM((width, d), BF), pltpu.SemaphoreType.DMA((3, pl.cdiv(width, STEP)))],
        compiler_params=pltpu.CompilerParams(vmem_limit_bytes=58 << 20),
        cost_estimate=pl.CostEstimate(
            flops=10 * rows * d * width,
            bytes_accessed=6 * d * width + 10 * rows * d + 6 * rows * width,
            transcendentals=rows * width,
        ),
        name="own_rows",
    )(m, cot, wg, wu, wd)


def far_kernel(*refs, count, width, tile, block, offsets, sliced):
    m, cot = refs[:count], refs[count : 2 * count]
    refs = refs[2 * count :]
    m_src, c_src = m, cot
    if sliced:
        m_src, c_src = refs[:count], refs[count : 2 * count]
        refs = refs[2 * count :]
    wg_ref, wu_ref, wd_ref, h_own, gb_own, ub_own = refs[:6]
    gk, uk, dk, sends = refs[6:10]
    m_turned, c_turned, h_all, gb_all, ub_all = refs[10:]
    step = pl.program_id(0)
    rows = m[0].shape[0]
    first = gk.shape[0]

    @pl.when(step == 0)
    def _():
        if not sliced:
            dp, ctx = lax.axis_index("dp"), lax.axis_index("ctx")
            n_ctx = lax.axis_size("ctx")
            starts = [
                pl.multiple_of(((dp ^ a) * n_ctx + (ctx ^ b)) * block, 128) for a, b in offsets
            ]
        for src, dst in ((m_src, m_turned), (c_src, c_turned)):
            at = 0
            for ref in src:
                long = ref.shape[0]
                if sliced:
                    dst[:, at : at + long] = ref[...].T
                else:
                    for j, start in enumerate(starts):
                        piece = ref[:, pl.ds(start, block)]
                        dst[j * block : (j + 1) * block, at : at + long] = piece.T
                at += long

    def body(w):
        wg, wu, wd = wg_ref[:, :w], wu_ref[:, :w], wd_ref[:w, :]
        h_all[:rows, :w] = h_own[:, :w]
        gb_all[:rows, :w] = gb_own[:, :w]
        ub_all[:rows, :w] = ub_own[:, :w]
        at = rows
        for i in range(1, count):
            long = m[i].shape[0]
            size = min(tile, long)
            for t in range(long // size):
                src = slice(t * size, (t + 1) * size)
                dst = slice(at + t * size, at + (t + 1) * size)
                h, gb, ub = gated(m[i][src, :], cot[i][src, :], wg, wu, wd)
                h_all[dst, :w] = h
                gb_all[dst, :w] = gb
                ub_all[dst, :w] = ub
            at += long
        for i, (src, keep) in enumerate(((gb_all, gk), (ub_all, uk))):
            grad = contract(m_turned[...], src[:, :w], 1, 0)
            keep[:, :w] = grad[:first]
            sends[i, :, :w] = grad[first:].astype(BF)
        grad = contract(c_turned[...], h_all[:, :w], 1, 0)
        dk[:w, :] = grad[:first].T
        sends[2, :, :w] = grad[first:].astype(BF)

    full, tail = divmod(width, STEP)
    if tail:
        pl.when(step < full)(lambda: body(STEP))
        pl.when(step == full)(lambda: body(tail))
    else:
        body(STEP)


def far_rows(ms, cots, m_cols, cot_cols, wg, wu, wd, own, block, offsets):
    count = len(ms)
    rows, d = ms[0].shape
    width = wg.shape[1]
    total = sum(m.shape[0] for m in ms)
    wide = block * len(offsets)
    first = wide // 2
    fixed = lambda i: (0, 0)
    col = lambda i: (0, i)
    row = lambda i: (i, 0)
    whole = lambda a: pl.BlockSpec(a.shape, fixed, pipeline_mode=pl.Buffered(1))
    shape = jax.ShapeDtypeStruct
    extra = [] if m_cols is None else list(m_cols) + list(cot_cols)
    return pl.pallas_call(
        functools.partial(
            far_kernel,
            count=count,
            width=width,
            tile=512,
            block=block,
            offsets=offsets,
            sliced=m_cols is not None,
        ),
        grid=(pl.cdiv(width, STEP),),
        in_specs=[whole(a) for a in list(ms) + list(cots) + extra]
        + [pl.BlockSpec((d, STEP), col)] * 2
        + [pl.BlockSpec((STEP, d), row)]
        + [pl.BlockSpec((rows, STEP), col)] * 3,
        out_specs=[pl.BlockSpec((first, STEP), col)] * 2
        + [
            pl.BlockSpec((STEP, first), row),
            pl.BlockSpec((3, first, STEP), lambda i: (0, 0, i)),
        ],
        out_shape=[shape((first, width), F32)] * 2
        + [shape((width, first), F32), shape((3, first, width), BF)],
        scratch_shapes=[pltpu.VMEM((wide, total), BF)] * 2
        + [pltpu.VMEM((total, STEP), BF)] * 3,
        compiler_params=pltpu.CompilerParams(vmem_limit_bytes=60 << 20),
        cost_estimate=pl.CostEstimate(
            flops=6 * (total - rows) * d * width + 6 * total * wide * width,
            bytes_accessed=6 * d * width + 4 * total * d + 6 * rows * width,
            transcendentals=(total - rows) * width,
        ),
        name="far_rows",
    )(*ms, *cots, *extra, wg, wu, wd, *own)


def shards(
    tokens,
    segments,
    attn_gain,
    query_weight,
    key_weight,
    value_weight,
    output_weight,
    mlp_gain,
    gate_weight,
    up_weight,
    down_weight,
    cotangent,
):
    rows, d = tokens.shape
    half = rows // 2
    seq = segments.shape[1]
    window = min(seq, seq // 2 + QB)
    ctx, dp = lax.axis_index("ctx"), lax.axis_index("dp")
    n_ctx, n_dp = lax.axis_size("ctx"), lax.axis_size("dp")
    core = lax.rem(lax.axis_index("tp"), 2)
    tp_rest = bits_of("tp")[1:]
    block_width = d // (n_ctx * n_dp)
    every_bit = bits_of("ctx") + bits_of("dp")
    attn_share = [("ctx", 1)]
    mlp_reduce = bits_of("ctx")[1:] + bits_of("dp")[:-1]
    attn_reduce = [b for b in every_bit if b not in attn_share]

    def owner_offsets(reduce_bits):
        return [
            [bit for i, bit in enumerate(reduce_bits) if code >> (len(reduce_bits) - 1 - i) & 1]
            for code in range(1 << len(reduce_bits))
        ]

    def owner_start(chosen, flip=()):
        other_dp, other_ctx = dp, ctx
        for axis, mask in list(chosen) + list(flip):
            if axis == "dp":
                other_dp = other_dp ^ mask
            else:
                other_ctx = other_ctx ^ mask
        return (other_dp * n_ctx + other_ctx) * block_width

    def columns(value, chosen, flip=()):
        return lax.dynamic_slice_in_dim(value, owner_start(chosen, flip), block_width, 1)

    def all_columns(value, reduce_bits, flip=()):
        return jnp.concatenate(
            [columns(value, chosen, flip) for chosen in owner_offsets(reduce_bits)], 1
        )

    def own_half(value):
        return lax.dynamic_slice_in_dim(value, core * half, half, 0)

    def other_half(value):
        return lax.dynamic_slice_in_dim(value, (1 - core) * half, half, 0)

    def both_halves(value):
        return jnp.concatenate([own_half(value), other_half(value)], 0)

    def join_cores(value):
        return jnp.concatenate([value, swap(value, "tp", 1)], 0)

    def share(value, bits):
        pieces = [value]
        for axis, mask in bits:
            pieces = pieces + [swap(piece, axis, mask) for piece in pieces]
        return join_cores(jnp.concatenate(pieces[1:], 0))

    def share_group(by_ctx, by_dp, gate, gate_dp):
        both = swap(after(by_dp, gate_dp), "ctx", 1)
        return [
            by_ctx,
            swap(after(by_ctx, gate), "tp", 1),
            by_dp,
            swap(after(by_dp, gate_dp), "tp", 1),
            both,
            swap(both, "tp", 1),
        ]

    def mirror(value):
        return swap(value, "dp", n_dp - 1)

    def tp_start(send, keep):
        total = keep + swap(send.astype(BF), "tp", 1).astype(F32)
        for axis, mask in tp_rest[:-1]:
            low = total.astype(BF)
            total = low.astype(F32) + swap(low, axis, mask).astype(F32)
        low = total.astype(BF)
        return low, swap(low, *tp_rest[-1])

    def tp_end(low, other):
        return low.astype(F32) + other.astype(F32)

    def after(value, *others):
        return lax.optimization_barrier((value,) + others)[0]

    def reduce_blocks(value, reduce_bits, dim):
        for axis, mask in reduce_bits:
            middle = value.shape[dim] // 2
            keep = lax.slice_in_dim(value, 0, middle, axis=dim)
            send = lax.slice_in_dim(value, middle, 2 * middle, axis=dim).astype(BF)
            value = keep + swap(send, axis, mask).astype(F32)
        return value

    def sum_gains(value):
        value = value + swap(value, "tp", 1)
        for axis, mask in every_bit:
            value = value + swap(value, axis, mask)
        return lax.dynamic_slice_in_dim(value, owner_start(()), block_width, 1)

    def whole_rows(value):
        out = jnp.zeros((rows, value.shape[1]), F32)
        out = lax.dynamic_update_slice_in_dim(out, value, core * half, 0)
        return lax.dynamic_update_slice_in_dim(out, swap(value, "tp", 1), (1 - core) * half, 0)

    seg_row = segments
    seg_col = jnp.swapaxes(segments, 0, 1)
    query_pos = ctx * rows + jnp.arange(rows, dtype=jnp.int32)
    cos_table, sin_table = rope_tables(query_pos, HEAD)
    kv_weight = jnp.concatenate([key_weight, value_weight], 1)
    cot_half = own_half(cotangent)
    cot_own = jnp.concatenate([cot_half, other_half(cotangent)], 0)
    x_half = own_half(tokens).astype(F32)

    attn_in, q_rot, kv_own = enter(
        tokens, attn_gain[None], query_weight, kv_weight, cos_table, sin_table
    )
    kv_parts = [kv_own]
    for axis, mask in bits_of("ctx"):
        kv_parts = kv_parts + [swap(piece, axis, mask) for piece in kv_parts]
    kv_all = jnp.stack(kv_parts, 0)
    cot_start = after(cot_half, kv_all)
    cot_ctx, cot_dp = swap(cot_start, "ctx", 1), mirror(cot_start)
    heads_out, lse = attend(q_rot, kv_all, seg_col, seg_row, window)
    heads_mine, heads_other = own_half(heads_out), other_half(heads_out)
    low_one, far_one = tp_start(
        contract(heads_other, output_weight, 1, 0), contract(heads_mine, output_weight, 1, 0)
    )
    middle = x_half + tp_end(low_one, far_one)
    inverse_two = lax.rsqrt(jnp.mean(middle * middle, axis=-1, keepdims=True) + EPSILON)
    normed_two = middle * inverse_two
    mlp_half = (normed_two * mlp_gain).astype(BF)
    mlp_ctx, mlp_dp = swap(mlp_half, "ctx", 1), mirror(mlp_half)
    mlp_own = join_cores(mlp_half)
    cot_group = [cot_own] + share_group(cot_ctx, cot_dp, low_one, mlp_own)

    hidden_own, gate_own, up_own, back_send, back_keep = own_rows(
        mlp_own, cot_own, gate_weight, up_weight, down_weight
    )
    low_three, far_three = tp_start(back_send, back_keep)
    mlp_group = [mlp_own] + share_group(mlp_ctx, mlp_dp, back_send, low_three)
    hidden_own = after(hidden_own, low_three)

    offsets = tuple(
        (
            sum(mask for axis, mask in chosen if axis == "dp"),
            sum(mask for axis, mask in chosen if axis == "ctx"),
        )
        for chosen in owner_offsets(mlp_reduce)
    )
    aligned = block_width % 128 == 0
    m_cols = None if aligned else [all_columns(m, mlp_reduce) for m in mlp_group]
    c_cols = None if aligned else [all_columns(c, mlp_reduce) for c in cot_group]
    far = far_rows(
        mlp_group,
        cot_group,
        m_cols,
        c_cols,
        gate_weight,
        up_weight,
        down_weight,
        (hidden_own, gate_own, up_own),
        block_width,
        offsets,
    )

    crossed = swap(far[3], *mlp_reduce[0])
    mlp_in_back = tp_end(low_three, after(far_three, far[3]))
    scaled = mlp_in_back * mlp_gain
    middle_back = cot_half.astype(F32) + inverse_two * (
        scaled - normed_two * jnp.mean(scaled * normed_two, axis=-1, keepdims=True)
    )
    mlp_gain_part = jnp.sum(mlp_in_back * normed_two, axis=0)
    branch_half = middle_back.astype(BF)
    branch_own = join_cores(branch_half)
    heads_back = contract(branch_own, output_weight, 1, 1).astype(BF)

    hidden_two = after(hidden_own, branch_half)
    low_two, far_two = tp_start(
        contract(hidden_two[half:], down_weight, 1, 0),
        contract(hidden_two[:half], down_weight, 1, 0),
    )

    query_back, kv_part, kv_far = attend_back(
        q_rot, heads_back, kv_all, lse, seg_col, seg_row, cos_table, sin_table, window
    )
    kv_back = join_keys(
        kv_part,
        [swap(kv_far[j - 1], "ctx", j) for j in range(1, n_ctx)],
        cos_table,
        sin_table,
    )
    qkv_back = jnp.concatenate([query_back, kv_back], 1)
    back_mine, back_other = own_half(qkv_back), other_half(qkv_back)
    q_width = query_back.shape[1]

    def attn_back(part):
        return contract(part[:, :q_width], query_weight, 1, 1) + contract(
            part[:, q_width:], kv_weight, 1, 1
        )

    low_four, far_four = tp_start(attn_back(back_other), attn_back(back_mine))
    layer_out = whole_rows(middle + tp_end(low_two, after(far_two, low_four)))
    attn_in_back = tp_end(low_four, far_four)
    inverse_one = lax.rsqrt(jnp.mean(x_half * x_half, axis=-1, keepdims=True) + EPSILON)
    normed_one = x_half * inverse_one
    scaled_one = attn_in_back * attn_gain
    tokens_half = middle_back + inverse_one * (
        scaled_one - normed_one * jnp.mean(scaled_one * normed_one, axis=-1, keepdims=True)
    )
    tokens_grad = whole_rows(tokens_half)
    crossed = after(crossed, low_four).astype(F32)
    gate_grad = reduce_blocks(far[0] + crossed[0], mlp_reduce[1:], 0)
    up_grad = reduce_blocks(far[1] + crossed[1], mlp_reduce[1:], 0)
    down_grad = reduce_blocks(far[2] + crossed[2].T, mlp_reduce[1:], 1)
    gains = sum_gains(jnp.stack([jnp.sum(attn_in_back * normed_one, axis=0), mlp_gain_part]))

    flip = attn_share
    attn_cols = both_halves(all_columns(attn_in, attn_reduce))
    attn_cols_far = share(
        after(own_half(all_columns(attn_in, attn_reduce, flip)), mlp_group[1]), attn_share
    )
    heads_rel = jnp.concatenate([heads_mine, heads_other], 0)
    heads_far = swap(after(heads_rel, mlp_group[1]), *attn_share[0])
    branch_cols = all_columns(branch_own, attn_reduce)
    branch_cols_far = share(all_columns(branch_half, attn_reduce, flip), attn_share)
    back_rel = jnp.concatenate([back_mine, back_other], 0)
    back_far_rel = swap(back_rel, *attn_share[0])
    output_grad = reduce_blocks(
        contract(heads_rel, branch_cols, 0, 0) + contract(heads_far, branch_cols_far, 0, 0),
        attn_reduce,
        1,
    )
    qkv_grad = reduce_blocks(
        contract(attn_cols, back_rel, 0, 0) + contract(attn_cols_far, back_far_rel, 0, 0),
        attn_reduce,
        0,
    )
    return (
        layer_out,
        tokens_grad,
        gains[0],
        qkv_grad[:, :q_width],
        qkv_grad[:, q_width : q_width + HEAD],
        qkv_grad[:, q_width + HEAD :],
        output_grad,
        gains[1],
        gate_grad,
        up_grad,
        down_grad,
    )


def solution(mesh):
    return jax.shard_map(
        shards,
        mesh=mesh,
        in_specs=(
            P(("dp", "ctx"), None),
            P("dp", None),
            P(),
            P(None, "tp"),
            P(None, "tp"),
            P(None, "tp"),
            P("tp", None),
            P(),
            P(None, "tp"),
            P(None, "tp"),
            P("tp", None),
            P(("dp", "ctx"), None),
        ),
        out_specs=(
            P(("dp", "ctx"), None),
            P(("dp", "ctx"), None),
            P(("dp", "ctx")),
            P(("dp", "ctx"), "tp"),
            P(("dp", "ctx"), "tp"),
            P(("dp", "ctx"), "tp"),
            P("tp", ("dp", "ctx")),
            P(("dp", "ctx")),
            P(("dp", "ctx"), "tp"),
            P(("dp", "ctx"), "tp"),
            P("tp", ("dp", "ctx")),
        ),
        check_vma=False,
    )
```

```python
import functools

import jax
import jax.numpy as jnp
from jax import lax
from jax.experimental import pallas as pl
from jax.experimental.pallas import tpu as pltpu
from jax.sharding import PartitionSpec as P

HEAD = 64
EPSILON = 1e-05
MASKED = -1000000000.0
BF = jnp.bfloat16
F32 = jnp.float32
QB = 128
BRIEF = pl.CostEstimate(flops=1, bytes_accessed=1, transcendentals=0)


def contract(left_side, right_side, left_dim, right_dim):
    return lax.dot_general(
        left_side,
        right_side,
        (((left_dim,), (right_dim,)), ((), ())),
        preferred_element_type=F32,
    )


def swap(value, axis, mask):
    size = lax.axis_size(axis)
    return lax.ppermute(value, axis, [(i, i ^ mask) for i in range(size)])


def bits_of(axis):
    return [(axis, 1 << k) for k in range((lax.axis_size(axis) - 1).bit_length())]


def rope_tables(positions, head_width):
    frequency = 10000.0 ** (-jnp.arange(0, head_width, 2, dtype=F32) / head_width)
    angles = positions.astype(F32)[:, None] * frequency[None, :]
    cos_half, sin_half = jnp.cos(angles), jnp.sin(angles)
    return (
        jnp.concatenate([cos_half] * 4, -1),
        jnp.concatenate([sin_half] * 4, -1),
    )


def lane_index(shape):
    return lax.broadcasted_iota(jnp.int32, shape, len(shape) - 1)


def turn(values):
    low = lane_index(values.shape) % HEAD < HEAD // 2
    width = values.shape[-1]
    return jnp.where(
        low, -pltpu.roll(values, width - HEAD // 2, 1), pltpu.roll(values, HEAD // 2, 1)
    )


def mate(axis, mask):
    return {axis: lax.axis_index(axis) ^ mask}


def greet(routes):
    barrier = pltpu.get_barrier_semaphore()
    distinct = sorted(set(routes))
    for axis, mask in distinct:
        pl.semaphore_signal(
            barrier, inc=1, device_id=mate(axis, mask), device_id_type=pl.DeviceIdType.MESH
        )
    pl.semaphore_wait(barrier, len(distinct))


def link(src, dst, sent, got, slot, route):
    return pltpu.make_async_remote_copy(
        src_ref=src,
        dst_ref=dst,
        send_sem=sent.at[slot],
        recv_sem=got.at[slot],
        device_id=mate(*route),
        device_id_type=pl.DeviceIdType.MESH,
    )


def links(sources, landings, sent, got, routes, base=0):
    return [
        link(src, dst, sent, got, base + k, route)
        for k, (src, dst, route) in enumerate(zip(sources, landings, routes))
    ]


def exchange_kernel(*refs, routes):
    n = len(routes)
    greet(routes)
    copies = links(refs[:n], refs[n : 2 * n], *refs[2 * n :], routes)
    for copy in copies:
        copy.start()
    for copy in copies:
        copy.wait()


def exchange(carried, collective_id, name):
    arrays = [value for value, _ in carried]
    anywhere = pl.BlockSpec(memory_space=pl.ANY)
    return pl.pallas_call(
        functools.partial(exchange_kernel, routes=tuple(route for _, route in carried)),
        in_specs=[anywhere] * len(arrays),
        out_specs=[anywhere] * len(arrays),
        out_shape=[jax.ShapeDtypeStruct(a.shape, a.dtype) for a in arrays],
        scratch_shapes=[pltpu.SemaphoreType.DMA((len(arrays),))] * 2,
        compiler_params=pltpu.CompilerParams(collective_id=collective_id, has_side_effects=True),
        cost_estimate=BRIEF,
        name=name,
    )(*arrays)


def enter_kernel(x_ref, gain_ref, wq_ref, wkv_ref, cos_ref, sin_ref, a_ref, q_ref, kv_ref):
    x = x_ref[...].astype(F32)
    inverse = lax.rsqrt(jnp.mean(x * x, axis=-1, keepdims=True) + EPSILON)
    a = (x * inverse * gain_ref[...]).astype(BF)
    a_ref[...] = a
    cos, sin = cos_ref[...], sin_ref[...]
    pairs = q_ref.shape[1] // 128
    q = jnp.dot(a, wq_ref[...], preferred_element_type=F32)
    cos_all = jnp.concatenate([cos] * pairs, -1)
    sin_all = jnp.concatenate([sin] * pairs, -1)
    q_rot = (q * cos_all + turn(q) * sin_all).astype(BF)
    q_ref[...] = q_rot * (HEAD**-0.5)
    kv = jnp.dot(a, wkv_ref[...], preferred_element_type=F32)
    is_key = lane_index(kv.shape) < HEAD
    kv_ref[...] = jnp.where(is_key, kv * cos + turn(kv) * sin, kv).astype(BF)


def enter(tokens, gain, wq, wkv, cos, sin):
    rows, d = tokens.shape
    tile = 128
    row = lambda i: (i, 0)
    fixed = lambda i: (0, 0)
    return pl.pallas_call(
        enter_kernel,
        grid=(rows // tile,),
        in_specs=[
            pl.BlockSpec((tile, d), row),
            pl.BlockSpec((1, d), fixed),
            pl.BlockSpec(wq.shape, fixed),
            pl.BlockSpec(wkv.shape, fixed),
            pl.BlockSpec((tile, 128), row),
            pl.BlockSpec((tile, 128), row),
        ],
        out_specs=[
            pl.BlockSpec((tile, d), row),
            pl.BlockSpec((tile, wq.shape[1]), row),
            pl.BlockSpec((tile, 128), row),
        ],
        out_shape=[
            jax.ShapeDtypeStruct((rows, d), BF),
            jax.ShapeDtypeStruct((rows, wq.shape[1]), BF),
            jax.ShapeDtypeStruct((rows, 128), BF),
        ],
        cost_estimate=BRIEF,
        name="enter",
    )(tokens, gain, wq, wkv, cos, sin)


def lay_keys(ctx, kv_ref, k_refs, v_refs):
    count, rows, _ = kv_ref.shape
    for j in range(count):
        kv = kv_ref[j].astype(F32)
        other = pltpu.roll(kv, HEAD, 1)
        low = lane_index(kv.shape) < HEAD
        at = pl.ds(pl.multiple_of((ctx ^ j) * rows, rows), rows)
        k_refs[0][at, :] = jnp.where(low, kv, 0.0).astype(BF)
        k_refs[1][at, :] = jnp.where(low, 0.0, other).astype(BF)
        v_refs[0][at, :] = jnp.where(low, other, 0.0).astype(BF)
        v_refs[1][at, :] = jnp.where(low, 0.0, kv).astype(BF)


def mask_of(ctx, block, rows, window, segc_ref, segr_ref, pairs):
    first_q = ctx * rows + block * QB
    start = pl.multiple_of(jnp.maximum(first_q + QB - window, 0), QB)
    key_seg = segc_ref[pl.ds(start, window), :]
    query_seg = segr_ref[:, pl.ds(pl.multiple_of(first_q, QB), QB)]
    key_pos = start + lax.broadcasted_iota(jnp.int32, (window, QB), 0)
    query_pos = first_q + lax.broadcasted_iota(jnp.int32, (window, QB), 1)
    bias = jnp.where((key_seg == query_seg) & (key_pos <= query_pos), 0.0, MASKED)
    return start, jnp.concatenate([bias] * pairs, -1)


def stack_pairs(ref, at, pairs):
    return jnp.concatenate([ref[at, 128 * g : 128 * (g + 1)] for g in range(pairs)], 0)


def forward_kernel(q_ref, kv_ref, segc_ref, segr_ref, o_ref, lse_ref, k0, k1, v0, v1, *, window):
    rows = q_ref.shape[0]
    pairs = q_ref.shape[1] // 128
    ctx = lax.axis_index("ctx")
    k_refs, v_refs = (k0, k1), (v0, v1)
    lay_keys(ctx, kv_ref, k_refs, v_refs)

    def body(block, carry):
        start, bias = mask_of(ctx, block, rows, window, segc_ref, segr_ref, pairs)
        at = pl.ds(pl.multiple_of(block * QB, QB), QB)
        keys_at = pl.ds(start, window)
        queries = stack_pairs(q_ref, at, pairs)
        mixed = None
        for parity in range(2):
            scores = contract(k_refs[parity][keys_at, :], queries, 1, 1) + bias
            top = jnp.max(scores, axis=0, keepdims=True)
            weights = jnp.exp(scores - top)
            total = jnp.sum(weights, axis=0, keepdims=True)
            lse_ref[pl.ds(block * 2 + parity, 1), :] = top + jnp.log(total)
            part = contract(v_refs[parity][keys_at, :], weights.astype(BF), 0, 0) / total
            mixed = part if mixed is None else mixed + part
        mixed = mixed.T.astype(BF)
        for g in range(pairs):
            o_ref[at, 128 * g : 128 * (g + 1)] = mixed[QB * g : QB * (g + 1), :]
        return carry

    lax.fori_loop(0, rows // QB, body, 0)


def attend(q, kv, seg_col, seg_row, window):
    rows, width = q.shape
    count = kv.shape[0]
    pairs = width // 128
    return pl.pallas_call(
        functools.partial(forward_kernel, window=window),
        out_shape=[
            jax.ShapeDtypeStruct((rows, width), BF),
            jax.ShapeDtypeStruct((rows // QB * 2, QB * pairs), F32),
        ],
        in_specs=[pl.BlockSpec(memory_space=pltpu.VMEM)] * 4,
        out_specs=[pl.BlockSpec(memory_space=pltpu.VMEM)] * 2,
        scratch_shapes=[pltpu.VMEM((count * rows, 128), BF)] * 4,
        cost_estimate=BRIEF,
        name="attend",
    )(q, kv, seg_col, seg_row)


def backward_kernel(
    q_ref,
    hb_ref,
    kv_ref,
    lse_ref,
    segc_ref,
    segr_ref,
    cos_ref,
    sin_ref,
    qb_ref,
    own_ref,
    far_ref,
    k0,
    k1,
    v0,
    v1,
    dk,
    dv,
    *,
    window,
):
    rows = q_ref.shape[0]
    pairs = q_ref.shape[1] // 128
    count = kv_ref.shape[0]
    ctx = lax.axis_index("ctx")
    core = lax.rem(lax.axis_index("tp"), 2)
    k_refs, v_refs = (k0, k1), (v0, v1)
    lay_keys(ctx, kv_ref, k_refs, v_refs)
    dk[...] = jnp.zeros_like(dk)
    dv[...] = jnp.zeros_like(dv)
    half_blocks = rows // QB // 2

    def body(block, carry):
        start, bias = mask_of(ctx, block, rows, window, segc_ref, segr_ref, pairs)
        at = pl.ds(pl.multiple_of(block * QB, QB), QB)
        keys_at = pl.ds(start, window)
        queries = stack_pairs(q_ref, at, pairs)
        swapped = lax.rem(block + core * half_blocks, 2 * half_blocks)
        backs = stack_pairs(hb_ref, pl.ds(pl.multiple_of(swapped * QB, QB), QB), pairs)
        low = lane_index(queries.shape) < HEAD
        zero = jnp.zeros_like(queries)
        dq = None
        for parity in range(2):
            keep = low if parity == 0 else jnp.logical_not(low)
            keys = k_refs[parity][keys_at, :]
            scores = contract(keys, queries, 1, 1) + bias
            weights = jnp.exp(scores - lse_ref[pl.ds(block * 2 + parity, 1), :])
            back = contract(v_refs[parity][keys_at, :], backs, 1, 1)
            delta = jnp.sum(weights * back, axis=0, keepdims=True)
            score_back = (weights * (back - delta)).astype(BF)
            part = contract(keys, score_back, 0, 0)
            dq = part if dq is None else dq + part
            dk[keys_at, :] += contract(score_back, jnp.where(keep, queries, zero), 1, 0)
            dv[keys_at, :] += contract(weights.astype(BF), jnp.where(keep, backs, zero), 1, 0)
        dq = dq.T * (HEAD**-0.5)
        cos, sin = cos_ref[at, :], sin_ref[at, :]
        for g in range(pairs):
            piece = dq[QB * g : QB * (g + 1), :]
            qb_ref[at, 128 * g : 128 * (g + 1)] = (piece * cos - turn(piece * sin)).astype(BF)
        return carry

    lax.fori_loop(0, rows // QB, body, 0)
    for j in range(count):
        at = pl.ds(pl.multiple_of((ctx ^ j) * rows, rows), rows)
        a, b = dk[at, :], dv[at, :]
        low = lane_index(a.shape) < HEAD
        both = jnp.where(low, a + pltpu.roll(a, HEAD, 1), b + pltpu.roll(b, HEAD, 1))
        if j == 0:
            own_ref[...] = both
        else:
            far_ref[j - 1] = both.astype(BF)


def attend_back(q, hb, kv, lse, seg_col, seg_row, cos, sin, window):
    rows, width = q.shape
    count = kv.shape[0]
    return pl.pallas_call(
        functools.partial(backward_kernel, window=window),
        out_shape=[
            jax.ShapeDtypeStruct((rows, width), BF),
            jax.ShapeDtypeStruct((rows, 128), F32),
            jax.ShapeDtypeStruct((count - 1, rows, 128), BF),
        ],
        in_specs=[pl.BlockSpec(memory_space=pltpu.VMEM)] * 8,
        out_specs=[pl.BlockSpec(memory_space=pltpu.VMEM)] * 3,
        scratch_shapes=[pltpu.VMEM((count * rows, 128), BF)] * 4
        + [pltpu.VMEM((count * rows, 128), F32)] * 2,
        cost_estimate=BRIEF,
        name="attend_back",
    )(q, hb, kv, lse, seg_col, seg_row, cos, sin)


def join_kernel(*refs):
    own_ref, cos_ref, sin_ref = refs[0], refs[-3], refs[-2]
    out_ref = refs[-1]
    total = own_ref[...]
    for ref in refs[1:-3]:
        total = total + ref[...].astype(F32)
    is_key = lane_index(total.shape) < HEAD
    turned = total * cos_ref[...] - turn(total * sin_ref[...])
    out_ref[...] = jnp.where(is_key, turned, total).astype(BF)


def join_keys(own, far, cos, sin):
    return pl.pallas_call(
        join_kernel,
        out_shape=jax.ShapeDtypeStruct(own.shape, BF),
        name="join_keys",
    )(own, *far, cos, sin)


STEP = 256


def gated(m, cot, wg, wu, wd):
    gate = contract(m, wg, 1, 0)
    up = contract(m, wu, 1, 0)
    back = contract(cot, wd, 1, 1)
    sig = 0.5 * jnp.tanh(0.5 * gate) + 0.5
    silu = gate * sig
    return (
        (silu * up).astype(BF),
        (back * up * (sig + silu * (1.0 - sig))).astype(BF),
        (back * silu).astype(BF),
    )


def own_kernel(
    m_ref,
    c_ref,
    wg_hbm,
    wu_hbm,
    wd_hbm,
    sources,
    h_ref,
    gb_ref,
    ub_ref,
    send_ref,
    keep_ref,
    landings,
    wg_ref,
    wu_ref,
    wd_ref,
    sems,
    sent,
    got,
    *,
    tile,
    routes,
):
    rows, d = m_ref.shape
    half = rows // 2
    width = wg_ref.shape[1]
    full, tail = divmod(width, STEP)

    def span(c, w):
        return pl.ds(c * STEP if isinstance(c, int) else pl.multiple_of(c * STEP, STEP), w)

    def copies(c, w):
        at = span(c, w)
        return [
            pltpu.make_async_copy(wg_hbm.at[:, at], wg_ref.at[:, at], sems.at[0, c]),
            pltpu.make_async_copy(wu_hbm.at[:, at], wu_ref.at[:, at], sems.at[1, c]),
            pltpu.make_async_copy(wd_hbm.at[at, :], wd_ref.at[at, :], sems.at[2, c]),
        ]

    for c in range(full + (1 if tail else 0)):
        for copy in copies(c, STEP if c < full else tail):
            copy.start()
    greet(routes)
    carried = links(sources, landings, sent, got, routes)
    for copy in carried:
        copy.start()

    def chunk(c, w):
        for copy in copies(c, w):
            copy.wait()
        at = span(c, w)
        wg, wu, wd = wg_ref[:, at], wu_ref[:, at], wd_ref[at, :]
        for t in range(rows // tile):
            r = slice(t * tile, (t + 1) * tile)
            h, gb, ub = gated(m_ref[r, :], c_ref[r, :], wg, wu, wd)
            h_ref[r, at] = h
            gb_ref[r, at] = gb
            ub_ref[r, at] = ub

    def chunk_step(c, carry):
        chunk(c, STEP)
        return carry

    lax.fori_loop(0, full, chunk_step, 0)
    if tail:
        chunk(full, tail)

    def back_step(i, carry):
        at = span(i, STEP)
        wg, wu = wg_ref[at, :], wu_ref[at, :]
        for t in range(rows // tile):
            r = slice(t * tile, (t + 1) * tile)
            part = contract(gb_ref[r, :], wg, 1, 1) + contract(ub_ref[r, :], wu, 1, 1)
            if t * tile < half:
                keep_ref[r, at] = part
            else:
                send_ref[t * tile - half : (t + 1) * tile - half, at] = part.astype(BF)
        return carry

    lax.fori_loop(0, d // STEP, back_step, 0)
    for copy in carried:
        copy.wait()


def own_rows(m, cot, wg, wu, wd, carried):
    arrays = [value for value, _ in carried]
    routes = tuple(route for _, route in carried)
    rows, d = m.shape
    width = wg.shape[1]
    out = jax.ShapeDtypeStruct((rows, width), BF)
    vmem = pl.BlockSpec(memory_space=pltpu.VMEM)
    hbm = pl.BlockSpec(memory_space=pl.ANY)
    return pl.pallas_call(
        functools.partial(own_kernel, tile=256, routes=routes),
        in_specs=[vmem, vmem, hbm, hbm, hbm, [hbm] * len(arrays)],
        out_specs=[vmem] * 5 + [[hbm] * len(arrays)],
        out_shape=[out] * 3
        + [jax.ShapeDtypeStruct((rows // 2, d), BF), jax.ShapeDtypeStruct((rows // 2, d), F32)]
        + [[jax.ShapeDtypeStruct(a.shape, a.dtype) for a in arrays]],
        scratch_shapes=[pltpu.VMEM((d, width), BF)] * 2
        + [pltpu.VMEM((width, d), BF), pltpu.SemaphoreType.DMA((3, pl.cdiv(width, STEP)))]
        + [pltpu.SemaphoreType.DMA((len(arrays),))] * 2,
        compiler_params=pltpu.CompilerParams(
            vmem_limit_bytes=58 << 20, collective_id=1, has_side_effects=True
        ),
        cost_estimate=BRIEF,
        name="own_rows",
    )(m, cot, wg, wu, wd, arrays)


def more_kernel(*refs, count, width, routes):
    m, cot, refs = refs[:count], refs[count : 2 * count], refs[2 * count :]
    wg_ref, wu_ref, wd_ref, hidden_ref = refs[:4]
    n = len(routes)
    sources, refs = refs[4 : 4 + n], refs[4 + n :]
    h_ref, gb_ref, ub_ref, send_ref, keep_ref = refs[:5]
    landings, (total, sent, got) = refs[5 : 5 + n], refs[5 + n :]
    step = pl.program_id(0)
    full, tail = divmod(width, STEP)
    steps = full + (1 if tail else 0)
    half = total.shape[0] // 2
    lanes = 512

    @pl.when(step == 0)
    def _():
        greet(routes)
        for copy in links(sources, landings, sent, got, routes):
            copy.start()
        total[...] = jnp.zeros_like(total)

    def body(w):
        wg, wu, wd = wg_ref[:, :w], wu_ref[:, :w], wd_ref[:w, :]
        at = 0
        for i in range(count):
            long = m[i].shape[0]
            dst = slice(at, at + long)
            h, gb, ub = gated(m[i][...], cot[i][...], wg, wu, wd)
            h_ref[dst, :w] = h
            gb_ref[dst, :w] = gb
            ub_ref[dst, :w] = ub
            at += long
        for c in range(total.shape[1] // lanes):
            cols = slice(c * lanes, (c + 1) * lanes)
            total[:, cols] += contract(hidden_ref[:, :w], wd[:, cols], 1, 0)

    if tail:
        pl.when(step < full)(lambda: body(STEP))
        pl.when(step == full)(lambda: body(tail))
    else:
        body(STEP)

    @pl.when(step == steps - 1)
    def _():
        keep_ref[...] = total[:half]
        send_ref[...] = total[half:].astype(BF)
        for copy in links(sources, landings, sent, got, routes):
            copy.wait()


def more_rows(ms, cots, wg, wu, wd, hidden, carried):
    count = len(ms)
    d = ms[0].shape[1]
    width = wg.shape[1]
    rows = sum(m.shape[0] for m in ms)
    own = hidden.shape[0]
    fixed = lambda i: (0, 0)
    col = lambda i: (0, i)
    row = lambda i: (i, 0)
    whole = lambda a: pl.BlockSpec(a.shape, fixed, pipeline_mode=pl.Buffered(1))
    anywhere = pl.BlockSpec(memory_space=pl.ANY)
    shape = jax.ShapeDtypeStruct
    arrays = [value for value, _ in carried]
    return pl.pallas_call(
        functools.partial(
            more_kernel, count=count, width=width, routes=tuple(route for _, route in carried)
        ),
        grid=(pl.cdiv(width, STEP),),
        in_specs=[whole(a) for a in list(ms) + list(cots)]
        + [pl.BlockSpec((d, STEP), col)] * 2
        + [pl.BlockSpec((STEP, d), row), pl.BlockSpec((own, STEP), col)]
        + [anywhere] * len(arrays),
        out_specs=[pl.BlockSpec((rows, STEP), col)] * 3
        + [pl.BlockSpec((own // 2, d), fixed)] * 2
        + [anywhere] * len(arrays),
        out_shape=[shape((rows, width), BF)] * 3
        + [shape((own // 2, d), BF), shape((own // 2, d), F32)]
        + [shape(a.shape, a.dtype) for a in arrays],
        scratch_shapes=[pltpu.VMEM((own, d), F32)]
        + [pltpu.SemaphoreType.DMA((len(arrays),))] * 2,
        compiler_params=pltpu.CompilerParams(
            vmem_limit_bytes=58 << 20, collective_id=3, has_side_effects=True
        ),
        cost_estimate=BRIEF,
        name="more_rows",
    )(*ms, *cots, wg, wu, wd, hidden, *arrays)


def far_kernel(*refs, count, ready, width, tile, block, offsets, sliced, routes, cross):
    m, cot = refs[:count], refs[count : 2 * count]
    refs = refs[2 * count :]
    m_src, c_src = m, cot
    if sliced:
        m_src, c_src = refs[:count], refs[count : 2 * count]
        refs = refs[2 * count :]
    wg_ref, wu_ref, wd_ref = refs[:3]
    known = [refs[3:6], refs[6:9]]
    refs = refs[9:]
    n = len(routes)
    sources, refs = refs[:n], refs[n:]
    gk, uk, dk = refs[:3]
    landings, refs = refs[3 : 3 + n], refs[3 + n :]
    m_turned, c_turned, h_all, gb_all, ub_all, sends, gets, sent, got = refs
    step = pl.program_id(0)
    first = gk.shape[0]
    full, tail = divmod(width, STEP)
    steps = full + (1 if tail else 0)

    def carried():
        return links(sources, landings, sent, got, routes, steps)

    @pl.when(step == 0)
    def _():
        greet(list(routes) + [cross])
        for copy in carried():
            copy.start()
        if not sliced:
            dp, ctx = lax.axis_index("dp"), lax.axis_index("ctx")
            n_ctx = lax.axis_size("ctx")
            starts = [
                pl.multiple_of(((dp ^ a) * n_ctx + (ctx ^ b)) * block, 128) for a, b in offsets
            ]
        for src, dst in ((m_src, m_turned), (c_src, c_turned)):
            at = 0
            for ref in src:
                long = ref.shape[0]
                if sliced:
                    dst[:, at : at + long] = ref[...].T
                else:
                    for j, start in enumerate(starts):
                        piece = ref[:, pl.ds(start, block)]
                        dst[j * block : (j + 1) * block, at : at + long] = piece.T
                at += long

    def crossing(c, w):
        return link(sends.at[c, :, :, :w], gets.at[c, :, :, :w], sent, got, c, cross)

    def body(w):
        wg, wu, wd = wg_ref[:, :w], wu_ref[:, :w], wd_ref[:w, :]
        at = 0
        for some in known:
            long = some[0].shape[0]
            for src, dst in zip(some, (h_all, gb_all, ub_all)):
                dst[at : at + long, :w] = src[:, :w]
            at += long
        for i in range(ready, count):
            long = m[i].shape[0]
            size = min(tile, long)
            for t in range(long // size):
                src = slice(t * size, (t + 1) * size)
                dst = slice(at + t * size, at + (t + 1) * size)
                h, gb, ub = gated(m[i][src, :], cot[i][src, :], wg, wu, wd)
                h_all[dst, :w] = h
                gb_all[dst, :w] = gb
                ub_all[dst, :w] = ub
            at += long
        lanes = pl.ds(pl.multiple_of(step * STEP, STEP), w)
        for i, (src, keep) in enumerate(((gb_all, gk), (ub_all, uk))):
            grad = contract(m_turned[...], src[:, :w], 1, 0)
            keep[:, lanes] = grad[:first]
            sends[step, i, :, :w] = grad[first:].astype(BF)
        grad = contract(c_turned[...], h_all[:, :w], 1, 0)
        dk[lanes, :] = grad[:first].T
        sends[step, 2, :, :w] = grad[first:].astype(BF)
        crossing(step, w).start()

    if tail:
        pl.when(step < full)(lambda: body(STEP))
        pl.when(step == full)(lambda: body(tail))
    else:
        body(STEP)

    @pl.when(step == steps - 1)
    def _():
        for c in range(steps):
            w = STEP if c < full else tail
            crossing(c, w).wait()
            at = slice(c * STEP, c * STEP + w)
            gk[:, at] += gets[c, 0, :, :w].astype(F32)
            uk[:, at] += gets[c, 1, :, :w].astype(F32)
            dk[at, :] += gets[c, 2, :, :w].astype(F32).T
        for copy in carried():
            copy.wait()


def far_rows(ms, cots, m_cols, cot_cols, wg, wu, wd, known, ready, block, offsets, cross, carried):
    count = len(ms)
    d = ms[0].shape[1]
    width = wg.shape[1]
    total = sum(m.shape[0] for m in ms)
    wide = block * len(offsets)
    first = wide // 2
    steps = pl.cdiv(width, STEP)
    fixed = lambda i: (0, 0)
    col = lambda i: (0, i)
    row = lambda i: (i, 0)
    whole = lambda a: pl.BlockSpec(a.shape, fixed, pipeline_mode=pl.Buffered(1))
    anywhere = pl.BlockSpec(memory_space=pl.ANY)
    shape = jax.ShapeDtypeStruct
    extra = [] if m_cols is None else list(m_cols) + list(cot_cols)
    arrays = [value for value, _ in carried]
    routes = tuple(route for _, route in carried)
    sems = pltpu.SemaphoreType.DMA((steps + len(carried),))
    return pl.pallas_call(
        functools.partial(
            far_kernel,
            count=count,
            ready=ready,
            width=width,
            tile=512,
            block=block,
            offsets=offsets,
            sliced=m_cols is not None,
            routes=routes,
            cross=cross,
        ),
        grid=(steps,),
        in_specs=[whole(a) for a in list(ms) + list(cots) + extra]
        + [pl.BlockSpec((d, STEP), col)] * 2
        + [pl.BlockSpec((STEP, d), row)]
        + [pl.BlockSpec((a.shape[0], STEP), col) for a in known]
        + [anywhere] * len(carried),
        out_specs=[pl.BlockSpec((first, width), fixed)] * 2
        + [pl.BlockSpec((width, first), fixed)]
        + [anywhere] * len(carried),
        out_shape=[shape((first, width), F32)] * 2
        + [shape((width, first), F32)]
        + [shape(a.shape, a.dtype) for a in arrays],
        scratch_shapes=[pltpu.VMEM((wide, total), BF)] * 2
        + [pltpu.VMEM((total, STEP), BF)] * 3
        + [pltpu.VMEM((steps, 3, first, STEP), BF)] * 2
        + [sems] * 2,
        compiler_params=pltpu.CompilerParams(
            vmem_limit_bytes=60 << 20, collective_id=0, has_side_effects=True
        ),
        cost_estimate=BRIEF,
        name="far_rows",
    )(*ms, *cots, *extra, wg, wu, wd, *known, *arrays)


def shards(
    tokens,
    segments,
    attn_gain,
    query_weight,
    key_weight,
    value_weight,
    output_weight,
    mlp_gain,
    gate_weight,
    up_weight,
    down_weight,
    cotangent,
):
    rows, d = tokens.shape
    half = rows // 2
    seq = segments.shape[1]
    window = min(seq, seq // 2 + QB)
    ctx, dp = lax.axis_index("ctx"), lax.axis_index("dp")
    n_ctx, n_dp = lax.axis_size("ctx"), lax.axis_size("dp")
    core = lax.rem(lax.axis_index("tp"), 2)
    tp_rest = bits_of("tp")[1:]
    block_width = d // (n_ctx * n_dp)
    every_bit = bits_of("ctx") + bits_of("dp")
    attn_share = [("ctx", 1)]
    mlp_reduce = bits_of("ctx")[1:] + bits_of("dp")[:-1]
    attn_reduce = [b for b in every_bit if b not in attn_share]

    def owner_offsets(reduce_bits):
        return [
            [bit for i, bit in enumerate(reduce_bits) if code >> (len(reduce_bits) - 1 - i) & 1]
            for code in range(1 << len(reduce_bits))
        ]

    def owner_start(chosen, flip=()):
        other_dp, other_ctx = dp, ctx
        for axis, mask in list(chosen) + list(flip):
            if axis == "dp":
                other_dp = other_dp ^ mask
            else:
                other_ctx = other_ctx ^ mask
        return (other_dp * n_ctx + other_ctx) * block_width

    def columns(value, chosen, flip=()):
        return lax.dynamic_slice_in_dim(value, owner_start(chosen, flip), block_width, 1)

    def all_columns(value, reduce_bits, flip=()):
        return jnp.concatenate(
            [columns(value, chosen, flip) for chosen in owner_offsets(reduce_bits)], 1
        )

    def own_half(value):
        return lax.dynamic_slice_in_dim(value, core * half, half, 0)

    def other_half(value):
        return lax.dynamic_slice_in_dim(value, (1 - core) * half, half, 0)

    def both_halves(value):
        return jnp.concatenate([own_half(value), other_half(value)], 0)

    def join_cores(value):
        return jnp.concatenate([value, swap(value, "tp", 1)], 0)

    def with_core(pieces):
        return [piece for value in pieces for piece in (value, swap(value, "tp", 1))]

    def mirror(value):
        return swap(value, "dp", n_dp - 1)

    def tp_low(send, keep):
        total = keep + swap(send.astype(BF), "tp", 1).astype(F32)
        for axis, mask in tp_rest[:-1]:
            low = total.astype(BF)
            total = low.astype(F32) + swap(low, axis, mask).astype(F32)
        return total.astype(BF)

    def tp_end(low, other):
        return low.astype(F32) + other.astype(F32)

    def after(value, *others):
        return lax.optimization_barrier((value,) + others)[0]

    def reduce_blocks(value, reduce_bits, dim):
        for axis, mask in reduce_bits:
            middle = value.shape[dim] // 2
            keep = lax.slice_in_dim(value, 0, middle, axis=dim)
            send = lax.slice_in_dim(value, middle, 2 * middle, axis=dim).astype(BF)
            value = keep + swap(send, axis, mask).astype(F32)
        return value

    def sum_gains(value):
        value = value + swap(value, "tp", 1)
        for axis, mask in every_bit:
            value = value + swap(value, axis, mask)
        return lax.dynamic_slice_in_dim(value, owner_start(()), block_width, 1)

    def whole_rows(value):
        out = jnp.zeros((rows, value.shape[1]), F32)
        out = lax.dynamic_update_slice_in_dim(out, value, core * half, 0)
        return lax.dynamic_update_slice_in_dim(out, swap(value, "tp", 1), (1 - core) * half, 0)

    seg_row = segments
    seg_col = jnp.swapaxes(segments, 0, 1)
    query_pos = ctx * rows + jnp.arange(rows, dtype=jnp.int32)
    cos_table, sin_table = rope_tables(query_pos, HEAD)
    kv_weight = jnp.concatenate([key_weight, value_weight], 1)
    cot_half = own_half(cotangent)
    cot_own = jnp.concatenate([cot_half, other_half(cotangent)], 0)
    x_half = own_half(tokens).astype(F32)

    attn_in, q_rot, kv_own = enter(
        tokens, attn_gain[None], query_weight, kv_weight, cos_table, sin_table
    )
    kv_parts = [kv_own]
    for axis, mask in bits_of("ctx"):
        kv_parts = kv_parts + [swap(piece, axis, mask) for piece in kv_parts]
    kv_all = jnp.stack(kv_parts, 0)
    quarter = half // 2
    cot_dp_a = mirror(cot_half[:quarter])
    kv_all = after(kv_all, cot_dp_a)
    heads_out, lse = attend(q_rot, kv_all, seg_col, seg_row, window)
    heads_mine, heads_other = own_half(heads_out), other_half(heads_out)
    low_one = tp_low(
        contract(heads_other, output_weight, 1, 0), contract(heads_mine, output_weight, 1, 0)
    )
    last, side, across = tp_rest[-1], ("ctx", 1), ("dp", n_dp - 1)
    far_one, cot_ctx, cot_dp_b = exchange(
        [(low_one, last), (cot_half, side), (cot_half[quarter:], across)], 2, "exchange_one"
    )
    middle = x_half + tp_end(low_one, far_one)
    inverse_two = lax.rsqrt(jnp.mean(middle * middle, axis=-1, keepdims=True) + EPSILON)
    normed_two = middle * inverse_two
    mlp_half = (normed_two * mlp_gain).astype(BF)
    mlp_own = join_cores(mlp_half)
    hidden_own, gate_own, up_own, back_send, back_keep, (mlp_ctx, mlp_dp_a) = own_rows(
        mlp_own,
        cot_own,
        gate_weight,
        up_weight,
        down_weight,
        [(mlp_half, side), (mlp_half[:quarter], across)],
    )
    low_three = tp_low(back_send, back_keep)
    mlp_near, cot_near = with_core([mlp_ctx]), with_core([cot_ctx])
    more = more_rows(
        mlp_near,
        cot_near,
        gate_weight,
        up_weight,
        down_weight,
        hidden_own,
        [
            (low_three, last),
            (cot_dp_a, side),
            (cot_dp_b, side),
            (mlp_half[quarter:], across),
        ],
    )
    down_send, down_keep, far_three, cot_both_a, cot_both_b, mlp_dp_b = more[3:]
    mlp_both = [swap(after(piece, far_three), "ctx", 1) for piece in (mlp_dp_a, mlp_dp_b)]
    low_two = tp_low(down_send, down_keep)
    mlp_in_back = tp_end(low_three, far_three)
    scaled = mlp_in_back * mlp_gain
    middle_back = cot_half.astype(F32) + inverse_two * (
        scaled - normed_two * jnp.mean(scaled * normed_two, axis=-1, keepdims=True)
    )
    mlp_gain_part = jnp.sum(mlp_in_back * normed_two, axis=0)
    branch_half = middle_back.astype(BF)
    branch_own = join_cores(branch_half)
    heads_back = contract(branch_own, output_weight, 1, 1).astype(BF)

    query_back, kv_part, kv_far = attend_back(
        q_rot, heads_back, kv_all, lse, seg_col, seg_row, cos_table, sin_table, window
    )
    kv_back = join_keys(
        kv_part,
        [swap(kv_far[j - 1], "ctx", j) for j in range(1, n_ctx)],
        cos_table,
        sin_table,
    )
    qkv_back = jnp.concatenate([query_back, kv_back], 1)
    back_mine, back_other = own_half(qkv_back), other_half(qkv_back)
    q_width = query_back.shape[1]

    def attn_back(part):
        return contract(part[:, :q_width], query_weight, 1, 1) + contract(
            part[:, q_width:], kv_weight, 1, 1
        )

    low_four = tp_low(
        attn_back(after(back_other, *mlp_both)), attn_back(after(back_mine, *mlp_both))
    )

    flip = attn_share
    attn_cols = both_halves(all_columns(attn_in, attn_reduce))
    attn_cols_half = own_half(all_columns(attn_in, attn_reduce, flip))
    heads_rel = jnp.concatenate([heads_mine, heads_other], 0)
    branch_cols = all_columns(branch_own, attn_reduce)
    branch_cols_half = all_columns(branch_half, attn_reduce, flip)
    back_rel = jnp.concatenate([back_mine, back_other], 0)

    mlp_group = [mlp_own] + mlp_near + with_core([mlp_dp_a, mlp_dp_b] + mlp_both)
    cot_group = [cot_own] + cot_near + with_core([cot_dp_a, cot_dp_b, cot_both_a, cot_both_b])
    offsets = tuple(
        (
            sum(mask for axis, mask in chosen if axis == "dp"),
            sum(mask for axis, mask in chosen if axis == "ctx"),
        )
        for chosen in owner_offsets(mlp_reduce)
    )
    aligned = block_width % 128 == 0
    m_cols = None if aligned else [all_columns(m, mlp_reduce) for m in mlp_group]
    c_cols = None if aligned else [all_columns(c, mlp_reduce) for c in cot_group]
    far = far_rows(
        mlp_group,
        cot_group,
        m_cols,
        c_cols,
        gate_weight,
        up_weight,
        down_weight,
        [hidden_own, gate_own, up_own, *more[:3]],
        3,
        block_width,
        offsets,
        mlp_reduce[0],
        [
            (low_four, last),
            (low_two, last),
            (branch_cols_half, side),
            (heads_rel, side),
            (attn_cols_half, side),
            (back_rel, side),
        ],
    )
    gate_part, up_part, down_part, far_four, far_two = far[:5]
    branch_cols_far, heads_far, attn_cols_far, back_far_rel = far[5:]
    branch_cols_far, attn_cols_far = join_cores(branch_cols_far), join_cores(attn_cols_far)


    layer_out = whole_rows(middle + tp_end(low_two, far_two))
    attn_in_back = tp_end(low_four, far_four)
    inverse_one = lax.rsqrt(jnp.mean(x_half * x_half, axis=-1, keepdims=True) + EPSILON)
    normed_one = x_half * inverse_one
    scaled_one = attn_in_back * attn_gain
    tokens_half = middle_back + inverse_one * (
        scaled_one - normed_one * jnp.mean(scaled_one * normed_one, axis=-1, keepdims=True)
    )
    tokens_grad = whole_rows(tokens_half)
    gate_grad = reduce_blocks(gate_part, mlp_reduce[1:], 0)
    up_grad = reduce_blocks(up_part, mlp_reduce[1:], 0)
    down_grad = reduce_blocks(down_part, mlp_reduce[1:], 1)
    gains = sum_gains(jnp.stack([jnp.sum(attn_in_back * normed_one, axis=0), mlp_gain_part]))

    output_grad = reduce_blocks(
        contract(heads_rel, branch_cols, 0, 0) + contract(heads_far, branch_cols_far, 0, 0),
        attn_reduce,
        1,
    )
    qkv_grad = reduce_blocks(
        contract(attn_cols, back_rel, 0, 0) + contract(attn_cols_far, back_far_rel, 0, 0),
        attn_reduce,
        0,
    )
    return (
        layer_out,
        tokens_grad,
        gains[0],
        qkv_grad[:, :q_width],
        qkv_grad[:, q_width : q_width + HEAD],
        qkv_grad[:, q_width + HEAD :],
        output_grad,
        gains[1],
        gate_grad,
        up_grad,
        down_grad,
    )


def solution(mesh):
    return jax.shard_map(
        shards,
        mesh=mesh,
        in_specs=(
            P(("dp", "ctx"), None),
            P("dp", None),
            P(),
            P(None, "tp"),
            P(None, "tp"),
            P(None, "tp"),
            P("tp", None),
            P(),
            P(None, "tp"),
            P(None, "tp"),
            P("tp", None),
            P(("dp", "ctx"), None),
        ),
        out_specs=(
            P(("dp", "ctx"), None),
            P(("dp", "ctx"), None),
            P(("dp", "ctx")),
            P(("dp", "ctx"), "tp"),
            P(("dp", "ctx"), "tp"),
            P(("dp", "ctx"), "tp"),
            P("tp", ("dp", "ctx")),
            P(("dp", "ctx")),
            P(("dp", "ctx"), "tp"),
            P(("dp", "ctx"), "tp"),
            P("tp", ("dp", "ctx")),
        ),
        check_vma=False,
    )
```

```python
import functools

import jax
import jax.numpy as jnp
from jax import lax
from jax.experimental import pallas as pl
from jax.experimental.pallas import tpu as pltpu
from jax.sharding import PartitionSpec as P

HEAD = 64
EPSILON = 1e-05
MASKED = -1000000000.0
BF = jnp.bfloat16
F32 = jnp.float32
QB = 128
BRIEF = pl.CostEstimate(flops=1, bytes_accessed=1, transcendentals=0)


def contract(left_side, right_side, left_dim, right_dim):
    return lax.dot_general(
        left_side,
        right_side,
        (((left_dim,), (right_dim,)), ((), ())),
        preferred_element_type=F32,
    )


def swap(value, axis, mask):
    size = lax.axis_size(axis)
    return lax.ppermute(value, axis, [(i, i ^ mask) for i in range(size)])


def bits_of(axis):
    return [(axis, 1 << k) for k in range((lax.axis_size(axis) - 1).bit_length())]


def rope_tables(positions, head_width):
    frequency = 10000.0 ** (-jnp.arange(0, head_width, 2, dtype=F32) / head_width)
    angles = positions.astype(F32)[:, None] * frequency[None, :]
    cos_half, sin_half = jnp.cos(angles), jnp.sin(angles)
    return (
        jnp.concatenate([cos_half] * 4, -1),
        jnp.concatenate([sin_half] * 4, -1),
    )


def lane_index(shape):
    return lax.broadcasted_iota(jnp.int32, shape, len(shape) - 1)


def turn(values):
    low = lane_index(values.shape) % HEAD < HEAD // 2
    width = values.shape[-1]
    return jnp.where(
        low, -pltpu.roll(values, width - HEAD // 2, 1), pltpu.roll(values, HEAD // 2, 1)
    )


def mate(axis, mask):
    return {axis: lax.axis_index(axis) ^ mask}


def greet(routes):
    barrier = pltpu.get_barrier_semaphore()
    distinct = sorted(set(routes))
    for axis, mask in distinct:
        pl.semaphore_signal(
            barrier, inc=1, device_id=mate(axis, mask), device_id_type=pl.DeviceIdType.MESH
        )
    pl.semaphore_wait(barrier, len(distinct))


def link(src, dst, sent, got, slot, route):
    return pltpu.make_async_remote_copy(
        src_ref=src,
        dst_ref=dst,
        send_sem=sent.at[slot],
        recv_sem=got.at[slot],
        device_id=mate(*route),
        device_id_type=pl.DeviceIdType.MESH,
    )


def links(sources, landings, sent, got, routes, base=0):
    return [
        link(src, dst, sent, got, base + k, route)
        for k, (src, dst, route) in enumerate(zip(sources, landings, routes))
    ]


def exchange_kernel(*refs, routes):
    n = len(routes)
    greet(routes)
    copies = links(refs[:n], refs[n : 2 * n], *refs[2 * n :], routes)
    for copy in copies:
        copy.start()
    for copy in copies:
        copy.wait()


def exchange(carried, collective_id, name):
    arrays = [value for value, _ in carried]
    anywhere = pl.BlockSpec(memory_space=pl.ANY)
    return pl.pallas_call(
        functools.partial(exchange_kernel, routes=tuple(route for _, route in carried)),
        in_specs=[anywhere] * len(arrays),
        out_specs=[anywhere] * len(arrays),
        out_shape=[jax.ShapeDtypeStruct(a.shape, a.dtype) for a in arrays],
        scratch_shapes=[pltpu.SemaphoreType.DMA((len(arrays),))] * 2,
        compiler_params=pltpu.CompilerParams(collective_id=collective_id, has_side_effects=True),
        cost_estimate=BRIEF,
        name=name,
    )(*arrays)


def enter_kernel(x_ref, gain_ref, wq_ref, wkv_ref, cos_ref, sin_ref, a_ref, q_ref, kv_ref):
    x = x_ref[...].astype(F32)
    inverse = lax.rsqrt(jnp.mean(x * x, axis=-1, keepdims=True) + EPSILON)
    a = (x * inverse * gain_ref[...]).astype(BF)
    a_ref[...] = a
    cos, sin = cos_ref[...], sin_ref[...]
    pairs = q_ref.shape[1] // 128
    q = jnp.dot(a, wq_ref[...], preferred_element_type=F32)
    cos_all = jnp.concatenate([cos] * pairs, -1)
    sin_all = jnp.concatenate([sin] * pairs, -1)
    q_rot = (q * cos_all + turn(q) * sin_all).astype(BF)
    q_ref[...] = q_rot * (HEAD**-0.5)
    kv = jnp.dot(a, wkv_ref[...], preferred_element_type=F32)
    is_key = lane_index(kv.shape) < HEAD
    kv_ref[...] = jnp.where(is_key, kv * cos + turn(kv) * sin, kv).astype(BF)


def enter(tokens, gain, wq, wkv, cos, sin):
    rows, d = tokens.shape
    tile = 128
    row = lambda i: (i, 0)
    fixed = lambda i: (0, 0)
    return pl.pallas_call(
        enter_kernel,
        grid=(rows // tile,),
        in_specs=[
            pl.BlockSpec((tile, d), row),
            pl.BlockSpec((1, d), fixed),
            pl.BlockSpec(wq.shape, fixed),
            pl.BlockSpec(wkv.shape, fixed),
            pl.BlockSpec((tile, 128), row),
            pl.BlockSpec((tile, 128), row),
        ],
        out_specs=[
            pl.BlockSpec((tile, d), row),
            pl.BlockSpec((tile, wq.shape[1]), row),
            pl.BlockSpec((tile, 128), row),
        ],
        out_shape=[
            jax.ShapeDtypeStruct((rows, d), BF),
            jax.ShapeDtypeStruct((rows, wq.shape[1]), BF),
            jax.ShapeDtypeStruct((rows, 128), BF),
        ],
        cost_estimate=BRIEF,
        name="enter",
    )(tokens, gain, wq, wkv, cos, sin)


def lay_keys(ctx, kv_ref, k_refs, v_refs):
    count, rows, _ = kv_ref.shape
    for j in range(count):
        kv = kv_ref[j].astype(F32)
        other = pltpu.roll(kv, HEAD, 1)
        low = lane_index(kv.shape) < HEAD
        at = pl.ds(pl.multiple_of((ctx ^ j) * rows, rows), rows)
        k_refs[0][at, :] = jnp.where(low, kv, 0.0).astype(BF)
        k_refs[1][at, :] = jnp.where(low, 0.0, other).astype(BF)
        v_refs[0][at, :] = jnp.where(low, other, 0.0).astype(BF)
        v_refs[1][at, :] = jnp.where(low, 0.0, kv).astype(BF)


def mask_of(ctx, block, rows, window, segc_ref, segr_ref, pairs):
    first_q = ctx * rows + block * QB
    start = pl.multiple_of(jnp.maximum(first_q + QB - window, 0), QB)
    key_seg = segc_ref[pl.ds(start, window), :]
    query_seg = segr_ref[:, pl.ds(pl.multiple_of(first_q, QB), QB)]
    key_pos = start + lax.broadcasted_iota(jnp.int32, (window, QB), 0)
    query_pos = first_q + lax.broadcasted_iota(jnp.int32, (window, QB), 1)
    bias = jnp.where((key_seg == query_seg) & (key_pos <= query_pos), 0.0, MASKED)
    return start, jnp.concatenate([bias] * pairs, -1)


def stack_pairs(ref, at, pairs):
    return jnp.concatenate([ref[at, 128 * g : 128 * (g + 1)] for g in range(pairs)], 0)


def forward_kernel(q_ref, kv_ref, segc_ref, segr_ref, o_ref, lse_ref, k0, k1, v0, v1, *, window):
    rows = q_ref.shape[0]
    pairs = q_ref.shape[1] // 128
    ctx = lax.axis_index("ctx")
    k_refs, v_refs = (k0, k1), (v0, v1)
    lay_keys(ctx, kv_ref, k_refs, v_refs)

    def body(block, carry):
        start, bias = mask_of(ctx, block, rows, window, segc_ref, segr_ref, pairs)
        at = pl.ds(pl.multiple_of(block * QB, QB), QB)
        keys_at = pl.ds(start, window)
        queries = stack_pairs(q_ref, at, pairs)
        mixed = None
        for parity in range(2):
            scores = contract(k_refs[parity][keys_at, :], queries, 1, 1) + bias
            top = jnp.max(scores, axis=0, keepdims=True)
            weights = jnp.exp(scores - top)
            total = jnp.sum(weights, axis=0, keepdims=True)
            lse_ref[pl.ds(block * 2 + parity, 1), :] = top + jnp.log(total)
            part = contract(v_refs[parity][keys_at, :], weights.astype(BF), 0, 0) / total
            mixed = part if mixed is None else mixed + part
        mixed = mixed.T.astype(BF)
        for g in range(pairs):
            o_ref[at, 128 * g : 128 * (g + 1)] = mixed[QB * g : QB * (g + 1), :]
        return carry

    lax.fori_loop(0, rows // QB, body, 0)


def attend(q, kv, seg_col, seg_row, window):
    rows, width = q.shape
    count = kv.shape[0]
    pairs = width // 128
    return pl.pallas_call(
        functools.partial(forward_kernel, window=window),
        out_shape=[
            jax.ShapeDtypeStruct((rows, width), BF),
            jax.ShapeDtypeStruct((rows // QB * 2, QB * pairs), F32),
        ],
        in_specs=[pl.BlockSpec(memory_space=pltpu.VMEM)] * 4,
        out_specs=[pl.BlockSpec(memory_space=pltpu.VMEM)] * 2,
        scratch_shapes=[pltpu.VMEM((count * rows, 128), BF)] * 4,
        cost_estimate=BRIEF,
        name="attend",
    )(q, kv, seg_col, seg_row)


def backward_kernel(
    q_ref,
    hb_ref,
    kv_ref,
    lse_ref,
    segc_ref,
    segr_ref,
    cos_ref,
    sin_ref,
    sources,
    qb_ref,
    own_ref,
    far_ref,
    landings,
    k0,
    k1,
    v0,
    v1,
    dk,
    dv,
    sent,
    got,
    *,
    window,
    routes,
):
    rows = q_ref.shape[0]
    pairs = q_ref.shape[1] // 128
    count = kv_ref.shape[0]
    ctx = lax.axis_index("ctx")
    core = lax.rem(lax.axis_index("tp"), 2)
    k_refs, v_refs = (k0, k1), (v0, v1)
    greet(routes)
    carried = links(sources, landings, sent, got, routes)
    for copy in carried:
        copy.start()
    lay_keys(ctx, kv_ref, k_refs, v_refs)
    dk[...] = jnp.zeros_like(dk)
    dv[...] = jnp.zeros_like(dv)
    half_blocks = rows // QB // 2

    def body(block, carry):
        start, bias = mask_of(ctx, block, rows, window, segc_ref, segr_ref, pairs)
        at = pl.ds(pl.multiple_of(block * QB, QB), QB)
        keys_at = pl.ds(start, window)
        queries = stack_pairs(q_ref, at, pairs)
        swapped = lax.rem(block + core * half_blocks, 2 * half_blocks)
        backs = stack_pairs(hb_ref, pl.ds(pl.multiple_of(swapped * QB, QB), QB), pairs)
        low = lane_index(queries.shape) < HEAD
        zero = jnp.zeros_like(queries)
        dq = None
        for parity in range(2):
            keep = low if parity == 0 else jnp.logical_not(low)
            keys = k_refs[parity][keys_at, :]
            scores = contract(keys, queries, 1, 1) + bias
            weights = jnp.exp(scores - lse_ref[pl.ds(block * 2 + parity, 1), :])
            back = contract(v_refs[parity][keys_at, :], backs, 1, 1)
            delta = jnp.sum(weights * back, axis=0, keepdims=True)
            score_back = (weights * (back - delta)).astype(BF)
            part = contract(keys, score_back, 0, 0)
            dq = part if dq is None else dq + part
            dk[keys_at, :] += contract(score_back, jnp.where(keep, queries, zero), 1, 0)
            dv[keys_at, :] += contract(weights.astype(BF), jnp.where(keep, backs, zero), 1, 0)
        dq = dq.T * (HEAD**-0.5)
        cos, sin = cos_ref[at, :], sin_ref[at, :]
        for g in range(pairs):
            piece = dq[QB * g : QB * (g + 1), :]
            qb_ref[at, 128 * g : 128 * (g + 1)] = (piece * cos - turn(piece * sin)).astype(BF)
        return carry

    lax.fori_loop(0, rows // QB, body, 0)
    for j in range(count):
        at = pl.ds(pl.multiple_of((ctx ^ j) * rows, rows), rows)
        a, b = dk[at, :], dv[at, :]
        low = lane_index(a.shape) < HEAD
        both = jnp.where(low, a + pltpu.roll(a, HEAD, 1), b + pltpu.roll(b, HEAD, 1))
        if j == 0:
            own_ref[...] = both
        else:
            far_ref[j - 1] = both.astype(BF)
    for copy in carried:
        copy.wait()


def attend_back(q, hb, kv, lse, seg_col, seg_row, cos, sin, window, carried):
    rows, width = q.shape
    count = kv.shape[0]
    arrays = [value for value, _ in carried]
    anywhere = pl.BlockSpec(memory_space=pl.ANY)
    return pl.pallas_call(
        functools.partial(
            backward_kernel, window=window, routes=tuple(route for _, route in carried)
        ),
        out_shape=[
            jax.ShapeDtypeStruct((rows, width), BF),
            jax.ShapeDtypeStruct((rows, 128), F32),
            jax.ShapeDtypeStruct((count - 1, rows, 128), BF),
            [jax.ShapeDtypeStruct(a.shape, a.dtype) for a in arrays],
        ],
        in_specs=[pl.BlockSpec(memory_space=pltpu.VMEM)] * 8 + [[anywhere] * len(arrays)],
        out_specs=[pl.BlockSpec(memory_space=pltpu.VMEM)] * 3 + [[anywhere] * len(arrays)],
        scratch_shapes=[pltpu.VMEM((count * rows, 128), BF)] * 4
        + [pltpu.VMEM((count * rows, 128), F32)] * 2
        + [pltpu.SemaphoreType.DMA((len(arrays),))] * 2,
        compiler_params=pltpu.CompilerParams(collective_id=4, has_side_effects=True),
        cost_estimate=BRIEF,
        name="attend_back",
    )(q, hb, kv, lse, seg_col, seg_row, cos, sin, arrays)


def join_kernel(*refs):
    own_ref, cos_ref, sin_ref = refs[0], refs[-3], refs[-2]
    out_ref = refs[-1]
    total = own_ref[...]
    for ref in refs[1:-3]:
        total = total + ref[...].astype(F32)
    is_key = lane_index(total.shape) < HEAD
    turned = total * cos_ref[...] - turn(total * sin_ref[...])
    out_ref[...] = jnp.where(is_key, turned, total).astype(BF)


def join_keys(own, far, cos, sin):
    return pl.pallas_call(
        join_kernel,
        out_shape=jax.ShapeDtypeStruct(own.shape, BF),
        name="join_keys",
    )(own, *far, cos, sin)


STEP = 256


def gated(m, cot, wg, wu, wd):
    gate = contract(m, wg, 1, 0)
    up = contract(m, wu, 1, 0)
    back = contract(cot, wd, 1, 1)
    sig = 0.5 * jnp.tanh(0.5 * gate) + 0.5
    silu = gate * sig
    return (
        (silu * up).astype(BF),
        (back * up * (sig + silu * (1.0 - sig))).astype(BF),
        (back * silu).astype(BF),
    )


def own_kernel(
    m_refs,
    c_refs,
    wg_hbm,
    wu_hbm,
    wd_hbm,
    sources,
    h_ref,
    gb_ref,
    ub_ref,
    send_ref,
    keep_ref,
    landings,
    wg_ref,
    wu_ref,
    wd_ref,
    sems,
    sent,
    got,
    *,
    tile,
    routes,
):
    half, d = m_refs[0].shape
    rows = 2 * half
    width = wg_ref.shape[1]
    full, tail = divmod(width, STEP)

    def span(c, w):
        return pl.ds(c * STEP if isinstance(c, int) else pl.multiple_of(c * STEP, STEP), w)

    def copies(c, w):
        at = span(c, w)
        return [
            pltpu.make_async_copy(wg_hbm.at[:, at], wg_ref.at[:, at], sems.at[0, c]),
            pltpu.make_async_copy(wu_hbm.at[:, at], wu_ref.at[:, at], sems.at[1, c]),
            pltpu.make_async_copy(wd_hbm.at[at, :], wd_ref.at[at, :], sems.at[2, c]),
        ]

    carried = links(sources, landings, sent, got, routes)
    greet(routes)
    for copy in carried:
        copy.start()
    for c in range(full + (1 if tail else 0)):
        for copy in copies(c, STEP if c < full else tail):
            copy.start()

    def chunk(c, w):
        for copy in copies(c, w):
            copy.wait()
        at = span(c, w)
        wg, wu, wd = wg_ref[:, at], wu_ref[:, at], wd_ref[at, :]
        for t in range(rows // tile):
            r = slice(t * tile, (t + 1) * tile)
            piece, at_row = divmod(t * tile, half)
            local = slice(at_row, at_row + tile)
            h, gb, ub = gated(m_refs[piece][local, :], c_refs[piece][local, :], wg, wu, wd)
            h_ref[r, at] = h
            gb_ref[r, at] = gb
            ub_ref[r, at] = ub

    def chunk_step(c, carry):
        chunk(c, STEP)
        return carry

    lax.fori_loop(0, full, chunk_step, 0)
    if tail:
        chunk(full, tail)

    def back_step(i, carry):
        at = span(i, STEP)
        wg, wu = wg_ref[at, :], wu_ref[at, :]
        for t in range(rows // tile):
            r = slice(t * tile, (t + 1) * tile)
            part = contract(gb_ref[r, :], wg, 1, 1) + contract(ub_ref[r, :], wu, 1, 1)
            if t * tile < half:
                keep_ref[r, at] = part
            else:
                send_ref[t * tile - half : (t + 1) * tile - half, at] = part.astype(BF)
        return carry

    lax.fori_loop(0, d // STEP, back_step, 0)
    for copy in carried:
        copy.wait()


def own_rows(ms, cots, wg, wu, wd, carried):
    arrays = [value for value, _ in carried]
    routes = tuple(route for _, route in carried)
    rows, d = 2 * ms[0].shape[0], ms[0].shape[1]
    width = wg.shape[1]
    out = jax.ShapeDtypeStruct((rows, width), BF)
    vmem = pl.BlockSpec(memory_space=pltpu.VMEM)
    hbm = pl.BlockSpec(memory_space=pl.ANY)
    return pl.pallas_call(
        functools.partial(own_kernel, tile=256, routes=routes),
        in_specs=[[vmem] * 2, [vmem] * 2, hbm, hbm, hbm, [hbm] * len(arrays)],
        out_specs=[vmem] * 5 + [[hbm] * len(arrays)],
        out_shape=[out] * 3
        + [jax.ShapeDtypeStruct((rows // 2, d), BF), jax.ShapeDtypeStruct((rows // 2, d), F32)]
        + [[jax.ShapeDtypeStruct(a.shape, a.dtype) for a in arrays]],
        scratch_shapes=[pltpu.VMEM((d, width), BF)] * 2
        + [pltpu.VMEM((width, d), BF), pltpu.SemaphoreType.DMA((3, pl.cdiv(width, STEP)))]
        + [pltpu.SemaphoreType.DMA((len(arrays),))] * 2,
        compiler_params=pltpu.CompilerParams(
            vmem_limit_bytes=58 << 20, collective_id=1, has_side_effects=True
        ),
        cost_estimate=BRIEF,
        name="own_rows",
    )(ms, cots, wg, wu, wd, arrays)


def more_kernel(*refs, count, width, routes):
    m, cot, refs = refs[:count], refs[count : 2 * count], refs[2 * count :]
    wg_ref, wu_ref, wd_ref, hidden_ref, down_hbm = refs[:5]
    n = len(routes)
    sources, refs = refs[5 : 5 + n], refs[5 + n :]
    h_ref, gb_ref, ub_ref, send_ref, keep_ref = refs[:5]
    landings, (down_all, down_sem, sent, got) = refs[5 : 5 + n], refs[5 + n :]
    down_copy = pltpu.make_async_copy(down_hbm, down_all, down_sem)
    step = pl.program_id(0)
    full, tail = divmod(width, STEP)
    steps = full + (1 if tail else 0)
    half = hidden_ref.shape[0] // 2
    lanes = 512

    @pl.when(step == 0)
    def _():
        greet(routes)
        for copy in links(sources, landings, sent, got, routes):
            copy.start()
        down_copy.start()

    def body(w):
        wg, wu, wd = wg_ref[:, :w], wu_ref[:, :w], wd_ref[:w, :]
        at = 0
        for i in range(count):
            long = m[i].shape[0]
            dst = slice(at, at + long)
            h, gb, ub = gated(m[i][...], cot[i][...], wg, wu, wd)
            h_ref[dst, :w] = h
            gb_ref[dst, :w] = gb
            ub_ref[dst, :w] = ub
            at += long

    if tail:
        pl.when(step < full)(lambda: body(STEP))
        pl.when(step == full)(lambda: body(tail))
    else:
        body(STEP)

    @pl.when(step == steps - 1)
    def _():
        down_copy.wait()

        def product(c, carry):
            cols = pl.ds(pl.multiple_of(c * lanes, lanes), lanes)
            total = contract(hidden_ref[...], down_all[:, cols], 1, 0)
            keep_ref[:, cols] = total[:half]
            send_ref[:, cols] = total[half:].astype(BF)
            return carry

        lax.fori_loop(0, keep_ref.shape[1] // lanes, product, 0)
        for copy in links(sources, landings, sent, got, routes):
            copy.wait()


def more_rows(ms, cots, wg, wu, wd, hidden, carried):
    count = len(ms)
    d = ms[0].shape[1]
    width = wg.shape[1]
    rows = sum(m.shape[0] for m in ms)
    own = hidden.shape[0]
    fixed = lambda i: (0, 0)
    col = lambda i: (0, i)
    row = lambda i: (i, 0)
    whole = lambda a: pl.BlockSpec(a.shape, fixed, pipeline_mode=pl.Buffered(1))
    anywhere = pl.BlockSpec(memory_space=pl.ANY)
    shape = jax.ShapeDtypeStruct
    arrays = [value for value, _ in carried]
    return pl.pallas_call(
        functools.partial(
            more_kernel, count=count, width=width, routes=tuple(route for _, route in carried)
        ),
        grid=(pl.cdiv(width, STEP),),
        in_specs=[whole(a) for a in list(ms) + list(cots)]
        + [pl.BlockSpec((d, STEP), col)] * 2
        + [pl.BlockSpec((STEP, d), row), whole(hidden), anywhere]
        + [anywhere] * len(arrays),
        out_specs=[pl.BlockSpec((rows, STEP), col)] * 3
        + [pl.BlockSpec((own // 2, d), fixed)] * 2
        + [anywhere] * len(arrays),
        out_shape=[shape((rows, width), BF)] * 3
        + [shape((own // 2, d), BF), shape((own // 2, d), F32)]
        + [shape(a.shape, a.dtype) for a in arrays],
        scratch_shapes=[pltpu.VMEM(wd.shape, BF), pltpu.SemaphoreType.DMA]
        + [pltpu.SemaphoreType.DMA((len(arrays),))] * 2,
        compiler_params=pltpu.CompilerParams(
            vmem_limit_bytes=58 << 20, collective_id=3, has_side_effects=True
        ),
        cost_estimate=BRIEF,
        name="more_rows",
    )(*ms, *cots, wg, wu, wd, hidden, wd, *arrays)


def far_kernel(*refs, longs, ready, width, tile, block, offsets, sliced, routes, cross, part_route):
    count = len(longs)
    m, cot = refs[:count], refs[count : 2 * count]
    refs = refs[2 * count :]
    m_src, c_src = m, cot
    if sliced:
        m_src, c_src = refs[:count], refs[count : 2 * count]
        refs = refs[2 * count :]
    wg_ref, wu_ref, wd_ref = refs[:3]
    known = [refs[3:6], refs[6:9]]
    refs = refs[9:]
    n = len(routes)
    summed = part_route is not None
    if summed:
        (part_send, part_keep), refs = refs[:2], refs[2:]
    sources, refs = refs[:n], refs[n:]
    (gk, uk, dk), refs = refs[:3], refs[3:]
    if summed:
        part_out, refs = refs[0], refs[1:]
    landings, refs = refs[:n], refs[n:]
    m_far, c_far, m_cols, c_cols, m_turned, c_turned = refs[:6]
    h_all, gb_all, ub_all, sends, gets, sent, got, row_sems, col_sems = refs[6:15]
    part_got = refs[15] if summed else None
    step = pl.program_id(0)
    first = gk.shape[0]
    full, tail = divmod(width, STEP)
    steps = full + (1 if tail else 0)
    begins = [sum(longs[:i]) for i in range(count)]
    near = begins[ready]
    total = sum(longs)

    def carried():
        return links(sources, landings, sent, got, routes, steps)

    def part_copy():
        return link(part_send, part_got, sent, got, steps + n, part_route)

    def row_copies():
        return [
            pltpu.make_async_copy(
                src[i], dst.at[pl.ds(begins[i] - near, longs[i]), :], row_sems.at[k, i]
            )
            for i in range(ready, count)
            for k, (src, dst) in enumerate(((m, m_far), (cot, c_far)))
        ]

    def column_copies():
        spans = [(0, None)]
        if not sliced:
            dp, ctx = lax.axis_index("dp"), lax.axis_index("ctx")
            n_ctx = lax.axis_size("ctx")
            spans = [
                (j * block, pl.multiple_of(((dp ^ a) * n_ctx + (ctx ^ b)) * block, 128))
                for j, (a, b) in enumerate(offsets)
            ]
        made = []
        for i in range(count):
            for k, (src, dst) in enumerate(((m_src, m_cols), (c_src, c_cols))):
                for j, (at, start) in enumerate(spans):
                    rows_at = pl.ds(begins[i], longs[i])
                    if start is None:
                        pair = src[i], dst.at[rows_at, :]
                    else:
                        pair = src[i].at[:, pl.ds(start, block)], dst.at[rows_at, pl.ds(at, block)]
                    made.append(pltpu.make_async_copy(*pair, col_sems.at[k, i, j]))
        return made

    @pl.when(step == 0)
    def _():
        greet(list(routes) + [cross] + [part_route] * summed)
        for copy in ([part_copy()] if summed else []) + carried() + row_copies() + column_copies():
            copy.start()
        for copy in row_copies():
            copy.wait()

    def crossing(c, w):
        return link(sends.at[c, :, :, :w], gets.at[c, :, :, :w], sent, got, c, cross)

    def body(w):
        wg, wu, wd = wg_ref[:, :w], wu_ref[:, :w], wd_ref[:w, :]
        at = 0
        for some in known:
            long = some[0].shape[0]
            for src, dst in zip(some, (h_all, gb_all, ub_all)):
                dst[at : at + long, :w] = src[:, :w]
            at += long
        for t in range((total - near) // tile):
            src = slice(t * tile, (t + 1) * tile)
            dst = slice(near + t * tile, near + (t + 1) * tile)
            h, gb, ub = gated(m_far[src, :], c_far[src, :], wg, wu, wd)
            h_all[dst, :w] = h
            gb_all[dst, :w] = gb
            ub_all[dst, :w] = ub

        @pl.when(step == 0)
        def _():
            for copy in column_copies():
                copy.wait()
            for src, dst in ((m_cols, m_turned), (c_cols, c_turned)):
                for t in range(total // tile):
                    dst[:, t * tile : (t + 1) * tile] = src[t * tile : (t + 1) * tile, :].T

        lanes = pl.ds(pl.multiple_of(step * STEP, STEP), w)
        for i, (src, keep) in enumerate(((gb_all, gk), (ub_all, uk))):
            grad = contract(m_turned[...], src[:, :w], 1, 0)
            keep[:, lanes] = grad[:first]
            sends[step, i, :, :w] = grad[first:].astype(BF)
        grad = contract(c_turned[...], h_all[:, :w], 1, 0)
        dk[lanes, :] = grad[:first].T
        sends[step, 2, :, :w] = grad[first:].astype(BF)
        crossing(step, w).start()

    if tail:
        pl.when(step < full)(lambda: body(STEP))
        pl.when(step == full)(lambda: body(tail))
    else:
        body(STEP)

    @pl.when(step == steps - 1)
    def _():
        if summed:
            part_copy().wait()
            part_out[...] = part_keep[...] + part_got[...].astype(F32)
        for c in range(steps):
            w = STEP if c < full else tail
            crossing(c, w).wait()
            at = slice(c * STEP, c * STEP + w)
            gk[:, at] += gets[c, 0, :, :w].astype(F32)
            uk[:, at] += gets[c, 1, :, :w].astype(F32)
            dk[at, :] += gets[c, 2, :, :w].astype(F32).T
        for copy in carried():
            copy.wait()


def far_rows(
    ms,
    cots,
    m_cols,
    cot_cols,
    weights,
    known,
    span,
    ready,
    block,
    offsets,
    cross,
    part,
    carried,
    collective_id,
    name,
):
    base, steps, width = span
    longs = tuple(m.shape[0] for m in ms)
    total, later = sum(longs), sum(longs[ready:])
    d = weights[0].shape[0]
    wide = block * len(offsets)
    first = wide // 2
    fixed = lambda i: (0, 0)
    col = lambda i: (0, i + base)
    row = lambda i: (i + base, 0)
    anywhere = pl.BlockSpec(memory_space=pl.ANY)
    shape = jax.ShapeDtypeStruct
    extra = [] if m_cols is None else list(m_cols) + list(cot_cols)
    arrays = [value for value, _ in carried]
    parts = [] if part is None else list(part[:2])
    part_specs = [] if part is None else [
        anywhere,
        pl.BlockSpec(part[1].shape, fixed, pipeline_mode=pl.Buffered(1)),
    ]
    part_shapes = [] if part is None else [part[1].shape]
    sems = pltpu.SemaphoreType.DMA((steps + len(carried) + 1,))
    return pl.pallas_call(
        functools.partial(
            far_kernel,
            longs=longs,
            ready=ready,
            width=width,
            tile=512,
            block=block,
            offsets=offsets,
            sliced=m_cols is not None,
            routes=tuple(route for _, route in carried),
            cross=cross,
            part_route=None if part is None else part[2],
        ),
        grid=(steps,),
        in_specs=[anywhere] * (2 * len(ms) + len(extra))
        + [pl.BlockSpec((d, STEP), col)] * 2
        + [pl.BlockSpec((STEP, d), row)]
        + [pl.BlockSpec((a.shape[0], STEP), col) for a in known]
        + part_specs
        + [anywhere] * len(carried),
        out_specs=[pl.BlockSpec((first, width), fixed)] * 2
        + [pl.BlockSpec((width, first), fixed)]
        + [pl.BlockSpec(a, fixed) for a in part_shapes]
        + [anywhere] * len(carried),
        out_shape=[shape((first, width), F32)] * 2
        + [shape((width, first), F32)]
        + [shape(a, F32) for a in part_shapes]
        + [shape(a.shape, a.dtype) for a in arrays],
        scratch_shapes=[pltpu.VMEM((later, d), BF)] * 2
        + [pltpu.VMEM((total, wide), BF)] * 2
        + [pltpu.VMEM((wide, total), BF)] * 2
        + [pltpu.VMEM((total, STEP), BF)] * 3
        + [pltpu.VMEM((steps, 3, first, STEP), BF)] * 2
        + [sems] * 2
        + [
            pltpu.SemaphoreType.DMA((2, len(ms))),
            pltpu.SemaphoreType.DMA((2, len(ms), len(offsets))),
        ]
        + [pltpu.VMEM(a, BF) for a in part_shapes],
        compiler_params=pltpu.CompilerParams(
            vmem_limit_bytes=60 << 20, collective_id=collective_id, has_side_effects=True
        ),
        cost_estimate=BRIEF,
        name=name,
    )(*ms, *cots, *extra, *weights, *known, *parts, *arrays)


TILE = 32


def finish_kernel(
    low_two,
    far_two,
    middle,
    low_four,
    far_four,
    middle_back,
    x_ref,
    gain_ref,
    mlp_part,
    sources,
    layer_ref,
    tokens_ref,
    gains_ref,
    landings,
    parts,
    other_parts,
    blocks,
    landed,
    sent,
    got,
    peer_sent,
    peer_got,
    *,
    routes,
):
    dp, ctx = lax.axis_index("dp"), lax.axis_index("ctx")
    n_dp, n_ctx = lax.axis_size("dp"), lax.axis_size("ctx")
    core = lax.rem(lax.axis_index("tp"), 2)
    half, d = middle.shape
    owners, _, block = blocks.shape
    mesh = pl.DeviceIdType.MESH
    near = ("tp", 1)
    codes = [(a, b) for a in range(n_dp) for b in range(n_ctx)][1:]
    ids = [{"dp": dp ^ a, "ctx": ctx ^ b} for a, b in codes]
    barrier = pltpu.get_barrier_semaphore()
    for peer in ids + [mate(*near)]:
        pl.semaphore_signal(barrier, inc=1, device_id=peer, device_id_type=mesh)
    pl.semaphore_wait(barrier, len(ids) + 1)
    n = len(routes)
    carried = links(sources, landings, sent, got, routes)
    for copy in carried:
        copy.start()

    own = pl.ds(pl.multiple_of(core * half, half), half)
    parts[0:1, :] = jnp.zeros((1, d), F32)
    parts[1:2, :] = mlp_part[...]

    def tokens_step(t, carry):
        at = pl.ds(pl.multiple_of(t * TILE, TILE), TILE)
        out_at = pl.ds(pl.multiple_of(core * half + t * TILE, TILE), TILE)
        x = x_ref[at, :].astype(F32)
        inverse = lax.rsqrt(jnp.mean(x * x, axis=-1, keepdims=True) + EPSILON)
        normed = x * inverse
        back = low_four[at, :].astype(F32) + far_four[at, :].astype(F32)
        parts[0:1, :] += jnp.sum(back * normed, axis=0, keepdims=True)
        scaled = back * gain_ref[...]
        mean = jnp.mean(scaled * normed, axis=-1, keepdims=True)
        tokens_ref[out_at, :] = middle_back[at, :] + inverse * (scaled - normed * mean)
        return carry

    lax.fori_loop(0, half // TILE, tokens_step, 0)
    to_core = [
        link(parts, other_parts, sent, got, n, near),
        link(tokens_ref.at[own, :], tokens_ref.at[own, :], sent, got, n + 1, near),
        link(layer_ref.at[own, :], layer_ref.at[own, :], sent, got, n + 2, near),
    ]
    to_core[0].start()
    to_core[1].start()

    def layer_step(t, carry):
        at = pl.ds(pl.multiple_of(t * TILE, TILE), TILE)
        out_at = pl.ds(pl.multiple_of(core * half + t * TILE, TILE), TILE)
        layer_ref[out_at, :] = middle[at, :] + (
            low_two[at, :].astype(F32) + far_two[at, :].astype(F32)
        )
        return carry

    lax.fori_loop(0, half // TILE, layer_step, 0)
    to_core[2].start()
    to_core[0].wait()
    for k in range(owners):
        at = slice(k * block, (k + 1) * block)
        blocks[k] = parts[:, at] + other_parts[:, at]
    copies = [
        pltpu.make_async_remote_copy(
            src_ref=blocks.at[peer["dp"] * n_ctx + peer["ctx"]],
            dst_ref=landed.at[k],
            send_sem=peer_sent.at[k],
            recv_sem=peer_got.at[k],
            device_id=peer,
            device_id_type=mesh,
        )
        for k, peer in enumerate(ids)
    ]
    for copy in copies:
        copy.start()
    for copy in copies:
        copy.wait()
    total = blocks[dp * n_ctx + ctx]
    for k in range(len(ids)):
        total = total + landed[k]
    gains_ref[...] = total
    for copy in to_core[1:] + carried:
        copy.wait()


def finish(values, gain, mlp_part, rows, carried):
    d = values[2].shape[1]
    owners = lax.axis_size("dp") * lax.axis_size("ctx")
    block = d // owners
    arrays = [value for value, _ in carried]
    vmem = pl.BlockSpec(memory_space=pltpu.VMEM)
    anywhere = pl.BlockSpec(memory_space=pl.ANY)
    shape = jax.ShapeDtypeStruct
    layer_out, tokens_grad, gains, landed = pl.pallas_call(
        functools.partial(finish_kernel, routes=tuple(route for _, route in carried)),
        in_specs=[vmem] * 9 + [[anywhere] * len(arrays)],
        out_specs=[vmem] * 3 + [[anywhere] * len(arrays)],
        out_shape=[shape((rows, d), F32)] * 2
        + [shape((2, block), F32), [shape(a.shape, a.dtype) for a in arrays]],
        scratch_shapes=[pltpu.VMEM((2, d), F32)] * 2
        + [pltpu.VMEM((owners, 2, block), F32), pltpu.VMEM((owners - 1, 2, block), F32)]
        + [pltpu.SemaphoreType.DMA((len(arrays) + 3,))] * 2
        + [pltpu.SemaphoreType.DMA((owners - 1,))] * 2,
        compiler_params=pltpu.CompilerParams(
            vmem_limit_bytes=58 << 20, collective_id=5, has_side_effects=True
        ),
        cost_estimate=BRIEF,
        name="finish",
    )(*values, gain, mlp_part, arrays)
    return layer_out, tokens_grad, gains, *landed


def shards(
    tokens,
    segments,
    attn_gain,
    query_weight,
    key_weight,
    value_weight,
    output_weight,
    mlp_gain,
    gate_weight,
    up_weight,
    down_weight,
    cotangent,
):
    rows, d = tokens.shape
    half = rows // 2
    seq = segments.shape[1]
    window = min(seq, seq // 2 + QB)
    ctx, dp = lax.axis_index("ctx"), lax.axis_index("dp")
    n_ctx, n_dp = lax.axis_size("ctx"), lax.axis_size("dp")
    core = lax.rem(lax.axis_index("tp"), 2)
    tp_rest = bits_of("tp")[1:]
    block_width = d // (n_ctx * n_dp)
    every_bit = bits_of("ctx") + bits_of("dp")
    attn_share = [("ctx", 1)]
    mlp_reduce = bits_of("ctx")[1:] + bits_of("dp")[:-1]
    attn_reduce = [b for b in every_bit if b not in attn_share]

    def owner_offsets(reduce_bits):
        return [
            [bit for i, bit in enumerate(reduce_bits) if code >> (len(reduce_bits) - 1 - i) & 1]
            for code in range(1 << len(reduce_bits))
        ]

    def owner_start(chosen, flip=()):
        other_dp, other_ctx = dp, ctx
        for axis, mask in list(chosen) + list(flip):
            if axis == "dp":
                other_dp = other_dp ^ mask
            else:
                other_ctx = other_ctx ^ mask
        return (other_dp * n_ctx + other_ctx) * block_width

    def columns(value, chosen, flip=()):
        return lax.dynamic_slice_in_dim(value, owner_start(chosen, flip), block_width, 1)

    def all_columns(value, reduce_bits, flip=()):
        return jnp.concatenate(
            [columns(value, chosen, flip) for chosen in owner_offsets(reduce_bits)], 1
        )

    def own_half(value):
        return lax.dynamic_slice_in_dim(value, core * half, half, 0)

    def other_half(value):
        return lax.dynamic_slice_in_dim(value, (1 - core) * half, half, 0)

    def both_halves(value):
        return jnp.concatenate([own_half(value), other_half(value)], 0)

    def join_cores(value):
        return jnp.concatenate([value, swap(value, "tp", 1)], 0)

    def with_core(pieces):
        return [piece for value in pieces for piece in (value, swap(value, "tp", 1))]

    def mirror(value):
        return swap(value, "dp", n_dp - 1)

    def tp_low(send, keep):
        total = keep + swap(send.astype(BF), "tp", 1).astype(F32)
        for axis, mask in tp_rest[:-1]:
            low = total.astype(BF)
            total = low.astype(F32) + swap(low, axis, mask).astype(F32)
        return total.astype(BF)

    def tp_end(low, other):
        return low.astype(F32) + other.astype(F32)

    def after(value, *others):
        return lax.optimization_barrier((value,) + others)[0]

    def halves(value, dim):
        middle = value.shape[dim] // 2
        keep = lax.slice_in_dim(value, 0, middle, axis=dim)
        return keep, lax.slice_in_dim(value, middle, 2 * middle, axis=dim).astype(BF)

    def reduce_blocks(value, reduce_bits, dim):
        for axis, mask in reduce_bits:
            keep, send = halves(value, dim)
            value = keep + swap(send, axis, mask).astype(F32)
        return value

    seg_row = segments
    seg_col = jnp.swapaxes(segments, 0, 1)
    query_pos = ctx * rows + jnp.arange(rows, dtype=jnp.int32)
    cos_table, sin_table = rope_tables(query_pos, HEAD)
    kv_weight = jnp.concatenate([key_weight, value_weight], 1)
    cot_half = own_half(cotangent)
    cot_own = [cot_half, other_half(cotangent)]
    x_half = own_half(tokens).astype(F32)

    attn_in, q_rot, kv_own = enter(
        tokens, attn_gain[None], query_weight, kv_weight, cos_table, sin_table
    )
    kv_parts = [kv_own]
    for axis, mask in bits_of("ctx"):
        kv_parts = kv_parts + [swap(piece, axis, mask) for piece in kv_parts]
    kv_all = jnp.stack(kv_parts, 0)
    quarter = half // 2
    last, side, across = tp_rest[-1], ("ctx", 1), ("dp", n_dp - 1)

    def own_quarter(value):
        which = lax.rem(lax.div(lax.axis_index("tp"), last[1]), 2)
        return lax.dynamic_slice_in_dim(value, which * quarter, quarter, 0)

    cot_dp_q = mirror(own_quarter(cot_half))
    cot_ctx_a = swap(cot_half[:quarter], *side)
    attn_cols_half = own_half(all_columns(attn_in, attn_reduce, attn_share))
    kv_all, attn_cols_half, *_ = lax.optimization_barrier(
        (kv_all, attn_cols_half, cot_dp_q, cot_ctx_a)
    )
    attn_cols_far = swap(attn_cols_half, *side)
    cot_dp_r = swap(cot_dp_q, *last)
    heads_out, lse = attend(q_rot, kv_all, seg_col, seg_row, window)
    heads_out = after(heads_out, attn_cols_far, cot_dp_r)
    heads_mine, heads_other = own_half(heads_out), other_half(heads_out)
    low_one = tp_low(
        contract(heads_other, output_weight, 1, 0), contract(heads_mine, output_weight, 1, 0)
    )
    far_one, cot_ctx_b, cot_both_q = exchange(
        [(low_one, last), (cot_half[quarter:], side), (cot_dp_q, side)], 2, "exchange_one"
    )
    cot_ctx = jnp.concatenate([cot_ctx_a, cot_ctx_b], 0)
    middle = x_half + tp_end(low_one, far_one)
    inverse_two = lax.rsqrt(jnp.mean(middle * middle, axis=-1, keepdims=True) + EPSILON)
    normed_two = middle * inverse_two
    mlp_half = (normed_two * mlp_gain).astype(BF)
    mlp_own = [mlp_half, swap(mlp_half, "tp", 1)]
    hidden_own, gate_own, up_own, back_send, back_keep, arrived = own_rows(
        mlp_own,
        cot_own,
        gate_weight,
        up_weight,
        down_weight,
        [
            (mlp_half, side),
            (own_quarter(mlp_half), across),
            (cot_both_q, last),
        ],
    )
    mlp_ctx, mlp_dp_q, cot_both_r = arrived
    low_three = tp_low(back_send, back_keep)
    heads_rel = jnp.concatenate([heads_mine, heads_other], 0)
    mlp_near, cot_near = with_core([mlp_ctx]), with_core([cot_ctx])
    more = more_rows(
        mlp_near,
        cot_near,
        gate_weight,
        up_weight,
        down_weight,
        hidden_own,
        [
            (low_three, last),
            (mlp_dp_q, side),
            (heads_rel, side),
        ],
    )
    down_send, down_keep, far_three, mlp_both_q, heads_far = more[3:]
    low_two = tp_low(down_send, down_keep)
    mlp_in_back = tp_end(low_three, far_three)
    scaled = mlp_in_back * mlp_gain
    middle_back = cot_half.astype(F32) + inverse_two * (
        scaled - normed_two * jnp.mean(scaled * normed_two, axis=-1, keepdims=True)
    )
    mlp_gain_part = jnp.sum(mlp_in_back * normed_two, axis=0)
    branch_half = middle_back.astype(BF)
    branch_own = join_cores(branch_half)
    heads_back = contract(branch_own, output_weight, 1, 1).astype(BF)

    flip = attn_share
    branch_cols = all_columns(branch_own, attn_reduce)
    branch_cols_half = all_columns(branch_half, attn_reduce, flip)
    query_back, kv_part, kv_far, (branch_cols_far, mlp_dp_r) = attend_back(
        q_rot,
        heads_back,
        kv_all,
        lse,
        seg_col,
        seg_row,
        cos_table,
        sin_table,
        window,
        [(branch_cols_half, side), (mlp_dp_q, last)],
    )
    mlp_both_r = swap(after(mlp_both_q, far_three), *last)
    kv_far, query_back, *_ = lax.optimization_barrier((kv_far, query_back, mlp_both_r))
    output_part = contract(heads_rel, branch_cols, 0, 0) + contract(
        heads_far, join_cores(branch_cols_far), 0, 0
    )
    output_keep, output_send = halves(reduce_blocks(output_part, attn_reduce[:-2], 1), 1)
    query_rel = jnp.concatenate([own_half(query_back), other_half(query_back)], 0)

    mlp_group = mlp_own + mlp_near + with_core([mlp_dp_q, mlp_dp_r, mlp_both_q, mlp_both_r])
    cot_group = cot_own + cot_near + with_core([cot_dp_q, cot_dp_r, cot_both_q, cot_both_r])
    offsets = tuple(
        (
            sum(mask for axis, mask in chosen if axis == "dp"),
            sum(mask for axis, mask in chosen if axis == "ctx"),
        )
        for chosen in owner_offsets(mlp_reduce)
    )
    aligned = block_width % 128 == 0
    m_cols = None if aligned else [all_columns(m, mlp_reduce) for m in mlp_group]
    c_cols = None if aligned else [all_columns(c, mlp_reduce) for c in cot_group]
    hidden_width = gate_weight.shape[1]
    early_steps = pl.cdiv(hidden_width, STEP) // 2
    early_width = early_steps * STEP

    def far_span(base, steps, width, part, carried, collective_id, name):
        return far_rows(
            mlp_group,
            cot_group,
            m_cols,
            c_cols,
            [gate_weight, up_weight, down_weight],
            [hidden_own, gate_own, up_own, *more[:3]],
            (base, steps, width),
            4,
            block_width,
            offsets,
            mlp_reduce[0],
            part,
            carried,
            collective_id,
            name,
        )

    early = far_span(
        0,
        early_steps,
        early_width,
        None,
        [(kv_far[j - 1], ("ctx", j)) for j in range(1, n_ctx)]
        + [(query_rel, side), (output_send, attn_reduce[-2]), (low_two, last)],
        0,
        "far_early",
    )
    output_near, far_two = early[-2:]
    query_far = early[-3]
    output_keep, output_send = halves(output_keep + output_near.astype(F32), 1)
    kv_back = join_keys(kv_part, early[3 : 2 + n_ctx], cos_table, sin_table)
    qkv_back = jnp.concatenate([query_back, kv_back], 1)
    back_mine, back_other = own_half(qkv_back), other_half(qkv_back)
    q_width = query_back.shape[1]

    def attn_back(part):
        return contract(part[:, :q_width], query_weight, 1, 1) + contract(
            part[:, q_width:], kv_weight, 1, 1
        )

    low_four = tp_low(attn_back(back_other), attn_back(back_mine))

    attn_cols = both_halves(all_columns(attn_in, attn_reduce))
    back_rel = jnp.concatenate([back_mine, back_other], 0)
    back_far_rel = jnp.concatenate([query_far, swap(back_rel[:, q_width:], *side)], 1)
    qkv_keep, qkv_send = halves(
        reduce_blocks(
            contract(attn_cols, back_rel, 0, 0)
            + contract(join_cores(attn_cols_far), back_far_rel, 0, 0),
            attn_reduce[:-2],
            0,
        ),
        0,
    )
    late = far_span(
        early_steps,
        pl.cdiv(hidden_width, STEP) - early_steps,
        hidden_width - early_width,
        (qkv_send, qkv_keep, attn_reduce[-2]),
        [(low_four, last), (output_send, attn_reduce[-1])],
        6,
        "far_late",
    )
    qkv_part, far_four, output_far = late[3:]
    gate_part = jnp.concatenate([early[0], late[0]], 1)
    up_part = jnp.concatenate([early[1], late[1]], 1)
    down_part = jnp.concatenate([early[2], late[2]], 0)
    output_grad = output_keep + output_far.astype(F32)
    qkv_keep, qkv_send = halves(qkv_part, 0)
    layer_out, tokens_grad, gains, qkv_far = finish(
        (low_two, far_two, middle, low_four, far_four, middle_back, own_half(tokens)),
        attn_gain[None],
        mlp_gain_part[None],
        rows,
        [(qkv_send, attn_reduce[-1])],
    )
    qkv_grad = qkv_keep + qkv_far.astype(F32)
    gate_grad = reduce_blocks(gate_part, mlp_reduce[1:], 0)
    up_grad = reduce_blocks(up_part, mlp_reduce[1:], 0)
    down_grad = reduce_blocks(down_part, mlp_reduce[1:], 1)
    return (
        layer_out,
        tokens_grad,
        gains[0],
        qkv_grad[:, :q_width],
        qkv_grad[:, q_width : q_width + HEAD],
        qkv_grad[:, q_width + HEAD :],
        output_grad,
        gains[1],
        gate_grad,
        up_grad,
        down_grad,
    )


def solution(mesh):
    return jax.shard_map(
        shards,
        mesh=mesh,
        in_specs=(
            P(("dp", "ctx"), None),
            P("dp", None),
            P(),
            P(None, "tp"),
            P(None, "tp"),
            P(None, "tp"),
            P("tp", None),
            P(),
            P(None, "tp"),
            P(None, "tp"),
            P("tp", None),
            P(("dp", "ctx"), None),
        ),
        out_specs=(
            P(("dp", "ctx"), None),
            P(("dp", "ctx"), None),
            P(("dp", "ctx")),
            P(("dp", "ctx"), "tp"),
            P(("dp", "ctx"), "tp"),
            P(("dp", "ctx"), "tp"),
            P("tp", ("dp", "ctx")),
            P(("dp", "ctx")),
            P(("dp", "ctx"), "tp"),
            P(("dp", "ctx"), "tp"),
            P("tp", ("dp", "ctx")),
        ),
        check_vma=False,
    )
```

```python
import functools

import jax
import jax.numpy as jnp
from jax import lax
from jax.experimental import pallas as pl
from jax.experimental.pallas import tpu as pltpu
from jax.sharding import PartitionSpec as P

HEAD = 64
EPSILON = 1e-05
MASKED = -1000000000.0
BF = jnp.bfloat16
F32 = jnp.float32
QB = 128
BRIEF = pl.CostEstimate(flops=1, bytes_accessed=1, transcendentals=0)


def contract(left_side, right_side, left_dim, right_dim):
    return lax.dot_general(
        left_side,
        right_side,
        (((left_dim,), (right_dim,)), ((), ())),
        preferred_element_type=F32,
    )


def swap(value, axis, mask):
    size = lax.axis_size(axis)
    return lax.ppermute(value, axis, [(i, i ^ mask) for i in range(size)])


def bits_of(axis):
    return [(axis, 1 << k) for k in range((lax.axis_size(axis) - 1).bit_length())]


def rope_tables(positions, head_width):
    frequency = 10000.0 ** (-jnp.arange(0, head_width, 2, dtype=F32) / head_width)
    angles = positions.astype(F32)[:, None] * frequency[None, :]
    cos_half, sin_half = jnp.cos(angles), jnp.sin(angles)
    return (
        jnp.concatenate([cos_half] * 4, -1),
        jnp.concatenate([sin_half] * 4, -1),
    )


def lane_index(shape):
    return lax.broadcasted_iota(jnp.int32, shape, len(shape) - 1)


def turn(values):
    low = lane_index(values.shape) % HEAD < HEAD // 2
    width = values.shape[-1]
    return jnp.where(
        low, -pltpu.roll(values, width - HEAD // 2, 1), pltpu.roll(values, HEAD // 2, 1)
    )


def mate(axis, mask):
    return {axis: lax.axis_index(axis) ^ mask}


def greet(routes):
    barrier = pltpu.get_barrier_semaphore()
    distinct = sorted(set(routes))
    for axis, mask in distinct:
        pl.semaphore_signal(
            barrier, inc=1, device_id=mate(axis, mask), device_id_type=pl.DeviceIdType.MESH
        )
    pl.semaphore_wait(barrier, len(distinct))


def link(src, dst, sent, got, slot, route):
    return pltpu.make_async_remote_copy(
        src_ref=src,
        dst_ref=dst,
        send_sem=sent.at[slot],
        recv_sem=got.at[slot],
        device_id=mate(*route),
        device_id_type=pl.DeviceIdType.MESH,
    )


def links(sources, landings, sent, got, routes, base=0):
    return [
        link(src, dst, sent, got, base + k, route)
        for k, (src, dst, route) in enumerate(zip(sources, landings, routes))
    ]


def exchange_kernel(*refs, routes):
    n = len(routes)
    greet(routes)
    copies = links(refs[:n], refs[n : 2 * n], *refs[2 * n :], routes)
    for copy in copies:
        copy.start()
    for copy in copies:
        copy.wait()


def exchange(carried, collective_id, name):
    arrays = [value for value, _ in carried]
    anywhere = pl.BlockSpec(memory_space=pl.ANY)
    return pl.pallas_call(
        functools.partial(exchange_kernel, routes=tuple(route for _, route in carried)),
        in_specs=[anywhere] * len(arrays),
        out_specs=[anywhere] * len(arrays),
        out_shape=[jax.ShapeDtypeStruct(a.shape, a.dtype) for a in arrays],
        scratch_shapes=[pltpu.SemaphoreType.DMA((len(arrays),))] * 2,
        compiler_params=pltpu.CompilerParams(collective_id=collective_id, has_side_effects=True),
        cost_estimate=BRIEF,
        name=name,
    )(*arrays)


def enter_kernel(x_ref, gain_ref, wq_ref, wkv_ref, cos_ref, sin_ref, a_ref, q_ref, kv_ref):
    x = x_ref[...].astype(F32)
    inverse = lax.rsqrt(jnp.mean(x * x, axis=-1, keepdims=True) + EPSILON)
    a = (x * inverse * gain_ref[...]).astype(BF)
    a_ref[...] = a
    cos, sin = cos_ref[...], sin_ref[...]
    pairs = q_ref.shape[1] // 128
    q = jnp.dot(a, wq_ref[...], preferred_element_type=F32)
    cos_all = jnp.concatenate([cos] * pairs, -1)
    sin_all = jnp.concatenate([sin] * pairs, -1)
    q_rot = (q * cos_all + turn(q) * sin_all).astype(BF)
    q_ref[...] = q_rot * (HEAD**-0.5)
    kv = jnp.dot(a, wkv_ref[...], preferred_element_type=F32)
    is_key = lane_index(kv.shape) < HEAD
    kv_ref[...] = jnp.where(is_key, kv * cos + turn(kv) * sin, kv).astype(BF)


def enter(tokens, gain, wq, wkv, cos, sin):
    rows, d = tokens.shape
    tile = 128
    row = lambda i: (i, 0)
    fixed = lambda i: (0, 0)
    return pl.pallas_call(
        enter_kernel,
        grid=(rows // tile,),
        in_specs=[
            pl.BlockSpec((tile, d), row),
            pl.BlockSpec((1, d), fixed),
            pl.BlockSpec(wq.shape, fixed),
            pl.BlockSpec(wkv.shape, fixed),
            pl.BlockSpec((tile, 128), row),
            pl.BlockSpec((tile, 128), row),
        ],
        out_specs=[
            pl.BlockSpec((tile, d), row),
            pl.BlockSpec((tile, wq.shape[1]), row),
            pl.BlockSpec((tile, 128), row),
        ],
        out_shape=[
            jax.ShapeDtypeStruct((rows, d), BF),
            jax.ShapeDtypeStruct((rows, wq.shape[1]), BF),
            jax.ShapeDtypeStruct((rows, 128), BF),
        ],
        cost_estimate=BRIEF,
        name="enter",
    )(tokens, gain, wq, wkv, cos, sin)


def lay_keys(ctx, kv_ref, k_refs, v_refs):
    count, rows, _ = kv_ref.shape
    for j in range(count):
        kv = kv_ref[j].astype(F32)
        other = pltpu.roll(kv, HEAD, 1)
        low = lane_index(kv.shape) < HEAD
        at = pl.ds(pl.multiple_of((ctx ^ j) * rows, rows), rows)
        k_refs[0][at, :] = jnp.where(low, kv, 0.0).astype(BF)
        k_refs[1][at, :] = jnp.where(low, 0.0, other).astype(BF)
        v_refs[0][at, :] = jnp.where(low, other, 0.0).astype(BF)
        v_refs[1][at, :] = jnp.where(low, 0.0, kv).astype(BF)


def mask_of(ctx, block, rows, window, segc_ref, segr_ref, pairs):
    first_q = ctx * rows + block * QB
    start = pl.multiple_of(jnp.maximum(first_q + QB - window, 0), QB)
    key_seg = segc_ref[pl.ds(start, window), :]
    query_seg = segr_ref[:, pl.ds(pl.multiple_of(first_q, QB), QB)]
    key_pos = start + lax.broadcasted_iota(jnp.int32, (window, QB), 0)
    query_pos = first_q + lax.broadcasted_iota(jnp.int32, (window, QB), 1)
    bias = jnp.where((key_seg == query_seg) & (key_pos <= query_pos), 0.0, MASKED)
    return start, jnp.concatenate([bias] * pairs, -1)


def stack_pairs(ref, at, pairs):
    return jnp.concatenate([ref[at, 128 * g : 128 * (g + 1)] for g in range(pairs)], 0)


def forward_kernel(q_ref, kv_ref, segc_ref, segr_ref, o_ref, lse_ref, k0, k1, v0, v1, *, window):
    rows = q_ref.shape[0]
    pairs = q_ref.shape[1] // 128
    ctx = lax.axis_index("ctx")
    k_refs, v_refs = (k0, k1), (v0, v1)
    lay_keys(ctx, kv_ref, k_refs, v_refs)

    def body(block, carry):
        start, bias = mask_of(ctx, block, rows, window, segc_ref, segr_ref, pairs)
        at = pl.ds(pl.multiple_of(block * QB, QB), QB)
        keys_at = pl.ds(start, window)
        queries = stack_pairs(q_ref, at, pairs)
        mixed = None
        for parity in range(2):
            scores = contract(k_refs[parity][keys_at, :], queries, 1, 1) + bias
            top = jnp.max(scores, axis=0, keepdims=True)
            weights = jnp.exp(scores - top)
            total = jnp.sum(weights, axis=0, keepdims=True)
            lse_ref[pl.ds(block * 2 + parity, 1), :] = top + jnp.log(total)
            part = contract(v_refs[parity][keys_at, :], weights.astype(BF), 0, 0) / total
            mixed = part if mixed is None else mixed + part
        mixed = mixed.T.astype(BF)
        for g in range(pairs):
            o_ref[at, 128 * g : 128 * (g + 1)] = mixed[QB * g : QB * (g + 1), :]
        return carry

    lax.fori_loop(0, rows // QB, body, 0)


def attend(q, kv, seg_col, seg_row, window):
    rows, width = q.shape
    count = kv.shape[0]
    pairs = width // 128
    return pl.pallas_call(
        functools.partial(forward_kernel, window=window),
        out_shape=[
            jax.ShapeDtypeStruct((rows, width), BF),
            jax.ShapeDtypeStruct((rows // QB * 2, QB * pairs), F32),
        ],
        in_specs=[pl.BlockSpec(memory_space=pltpu.VMEM)] * 4,
        out_specs=[pl.BlockSpec(memory_space=pltpu.VMEM)] * 2,
        scratch_shapes=[pltpu.VMEM((count * rows, 128), BF)] * 4,
        cost_estimate=BRIEF,
        name="attend",
    )(q, kv, seg_col, seg_row)


def backward_kernel(
    q_ref,
    hb_ref,
    kv_ref,
    lse_ref,
    segc_ref,
    segr_ref,
    cos_ref,
    sin_ref,
    sources,
    qb_ref,
    own_ref,
    far_ref,
    landings,
    k0,
    k1,
    v0,
    v1,
    dk,
    dv,
    sent,
    got,
    *,
    window,
    routes,
):
    rows = q_ref.shape[0]
    pairs = q_ref.shape[1] // 128
    count = kv_ref.shape[0]
    ctx = lax.axis_index("ctx")
    core = lax.rem(lax.axis_index("tp"), 2)
    k_refs, v_refs = (k0, k1), (v0, v1)
    greet(routes)
    carried = links(sources, landings, sent, got, routes)
    for copy in carried:
        copy.start()
    lay_keys(ctx, kv_ref, k_refs, v_refs)
    dk[...] = jnp.zeros_like(dk)
    dv[...] = jnp.zeros_like(dv)
    half_blocks = rows // QB // 2

    def body(block, carry):
        start, bias = mask_of(ctx, block, rows, window, segc_ref, segr_ref, pairs)
        at = pl.ds(pl.multiple_of(block * QB, QB), QB)
        keys_at = pl.ds(start, window)
        queries = stack_pairs(q_ref, at, pairs)
        swapped = lax.rem(block + core * half_blocks, 2 * half_blocks)
        backs = stack_pairs(hb_ref, pl.ds(pl.multiple_of(swapped * QB, QB), QB), pairs)
        low = lane_index(queries.shape) < HEAD
        zero = jnp.zeros_like(queries)
        dq = None
        for parity in range(2):
            keep = low if parity == 0 else jnp.logical_not(low)
            keys = k_refs[parity][keys_at, :]
            scores = contract(keys, queries, 1, 1) + bias
            weights = jnp.exp(scores - lse_ref[pl.ds(block * 2 + parity, 1), :])
            back = contract(v_refs[parity][keys_at, :], backs, 1, 1)
            delta = jnp.sum(weights * back, axis=0, keepdims=True)
            score_back = (weights * (back - delta)).astype(BF)
            part = contract(keys, score_back, 0, 0)
            dq = part if dq is None else dq + part
            dk[keys_at, :] += contract(score_back, jnp.where(keep, queries, zero), 1, 0)
            dv[keys_at, :] += contract(weights.astype(BF), jnp.where(keep, backs, zero), 1, 0)
        dq = dq.T * (HEAD**-0.5)
        cos, sin = cos_ref[at, :], sin_ref[at, :]
        for g in range(pairs):
            piece = dq[QB * g : QB * (g + 1), :]
            qb_ref[at, 128 * g : 128 * (g + 1)] = (piece * cos - turn(piece * sin)).astype(BF)
        return carry

    lax.fori_loop(0, rows // QB, body, 0)
    for j in range(count):
        at = pl.ds(pl.multiple_of((ctx ^ j) * rows, rows), rows)
        a, b = dk[at, :], dv[at, :]
        low = lane_index(a.shape) < HEAD
        both = jnp.where(low, a + pltpu.roll(a, HEAD, 1), b + pltpu.roll(b, HEAD, 1))
        if j == 0:
            own_ref[...] = both
        else:
            far_ref[j - 1] = both.astype(BF)
    for copy in carried:
        copy.wait()


def attend_back(q, hb, kv, lse, seg_col, seg_row, cos, sin, window, carried):
    rows, width = q.shape
    count = kv.shape[0]
    arrays = [value for value, _ in carried]
    anywhere = pl.BlockSpec(memory_space=pl.ANY)
    return pl.pallas_call(
        functools.partial(
            backward_kernel, window=window, routes=tuple(route for _, route in carried)
        ),
        out_shape=[
            jax.ShapeDtypeStruct((rows, width), BF),
            jax.ShapeDtypeStruct((rows, 128), F32),
            jax.ShapeDtypeStruct((count - 1, rows, 128), BF),
            [jax.ShapeDtypeStruct(a.shape, a.dtype) for a in arrays],
        ],
        in_specs=[pl.BlockSpec(memory_space=pltpu.VMEM)] * 8 + [[anywhere] * len(arrays)],
        out_specs=[pl.BlockSpec(memory_space=pltpu.VMEM)] * 3 + [[anywhere] * len(arrays)],
        scratch_shapes=[pltpu.VMEM((count * rows, 128), BF)] * 4
        + [pltpu.VMEM((count * rows, 128), F32)] * 2
        + [pltpu.SemaphoreType.DMA((len(arrays),))] * 2,
        compiler_params=pltpu.CompilerParams(collective_id=4, has_side_effects=True),
        cost_estimate=BRIEF,
        name="attend_back",
    )(q, hb, kv, lse, seg_col, seg_row, cos, sin, arrays)


def join_kernel(*refs):
    own_ref, cos_ref, sin_ref = refs[0], refs[-3], refs[-2]
    out_ref = refs[-1]
    total = own_ref[...]
    for ref in refs[1:-3]:
        total = total + ref[...].astype(F32)
    is_key = lane_index(total.shape) < HEAD
    turned = total * cos_ref[...] - turn(total * sin_ref[...])
    out_ref[...] = jnp.where(is_key, turned, total).astype(BF)


def join_keys(own, far, cos, sin):
    return pl.pallas_call(
        join_kernel,
        out_shape=jax.ShapeDtypeStruct(own.shape, BF),
        name="join_keys",
    )(own, *far, cos, sin)


STEP = 256


def gated(m, cot, wg, wu, wd):
    gate = contract(m, wg, 1, 0)
    up = contract(m, wu, 1, 0)
    back = contract(cot, wd, 1, 1)
    sig = 0.5 * jnp.tanh(0.5 * gate) + 0.5
    silu = gate * sig
    return (
        (silu * up).astype(BF),
        (back * up * (sig + silu * (1.0 - sig))).astype(BF),
        (back * silu).astype(BF),
    )


def own_kernel(
    m_refs,
    c_refs,
    wg_hbm,
    wu_hbm,
    wd_hbm,
    sources,
    h_ref,
    gb_ref,
    ub_ref,
    send_ref,
    keep_ref,
    landings,
    wg_ref,
    wu_ref,
    wd_ref,
    sems,
    sent,
    got,
    *,
    tile,
    routes,
):
    half, d = m_refs[0].shape
    rows = 2 * half
    width = wg_ref.shape[1]
    full, tail = divmod(width, STEP)

    def span(c, w):
        return pl.ds(c * STEP if isinstance(c, int) else pl.multiple_of(c * STEP, STEP), w)

    def copies(c, w):
        at = span(c, w)
        return [
            pltpu.make_async_copy(wg_hbm.at[:, at], wg_ref.at[:, at], sems.at[0, c]),
            pltpu.make_async_copy(wu_hbm.at[:, at], wu_ref.at[:, at], sems.at[1, c]),
            pltpu.make_async_copy(wd_hbm.at[at, :], wd_ref.at[at, :], sems.at[2, c]),
        ]

    carried = links(sources, landings, sent, got, routes)
    greet(routes)
    for copy in carried:
        copy.start()
    ahead = min(3, full)
    for c in range(ahead):
        for copy in copies(c, STEP):
            copy.start()

    def chunk(c, w):
        for copy in copies(c, w):
            copy.wait()
        at = span(c, w)
        wg, wu, wd = wg_ref[:, at], wu_ref[:, at], wd_ref[at, :]
        for t in range(rows // tile):
            r = slice(t * tile, (t + 1) * tile)
            piece, at_row = divmod(t * tile, half)
            local = slice(at_row, at_row + tile)
            h, gb, ub = gated(m_refs[piece][local, :], c_refs[piece][local, :], wg, wu, wd)
            h_ref[r, at] = h
            gb_ref[r, at] = gb
            ub_ref[r, at] = ub

    def chunk_step(c, carry):
        @pl.when(c + ahead < full)
        def _():
            for copy in copies(c + ahead, STEP):
                copy.start()

        if tail:

            @pl.when(c + ahead == full)
            def _():
                for copy in copies(full, tail):
                    copy.start()

        chunk(c, STEP)
        return carry

    lax.fori_loop(0, full, chunk_step, 0)
    if tail:
        chunk(full, tail)

    def back_step(i, carry):
        at = span(i, STEP)
        wg, wu = wg_ref[at, :], wu_ref[at, :]
        for t in range(rows // tile):
            r = slice(t * tile, (t + 1) * tile)
            part = contract(gb_ref[r, :], wg, 1, 1) + contract(ub_ref[r, :], wu, 1, 1)
            if t * tile < half:
                keep_ref[r, at] = part
            else:
                send_ref[t * tile - half : (t + 1) * tile - half, at] = part.astype(BF)
        return carry

    lax.fori_loop(0, d // STEP, back_step, 0)
    for copy in carried:
        copy.wait()


def own_rows(ms, cots, wg, wu, wd, carried):
    arrays = [value for value, _ in carried]
    routes = tuple(route for _, route in carried)
    rows, d = 2 * ms[0].shape[0], ms[0].shape[1]
    width = wg.shape[1]
    out = jax.ShapeDtypeStruct((rows, width), BF)
    vmem = pl.BlockSpec(memory_space=pltpu.VMEM)
    hbm = pl.BlockSpec(memory_space=pl.ANY)
    return pl.pallas_call(
        functools.partial(own_kernel, tile=256, routes=routes),
        in_specs=[[vmem] * 2, [vmem] * 2, hbm, hbm, hbm, [hbm] * len(arrays)],
        out_specs=[vmem] * 5 + [[hbm] * len(arrays)],
        out_shape=[out] * 3
        + [jax.ShapeDtypeStruct((rows // 2, d), BF), jax.ShapeDtypeStruct((rows // 2, d), F32)]
        + [[jax.ShapeDtypeStruct(a.shape, a.dtype) for a in arrays]],
        scratch_shapes=[pltpu.VMEM((d, width), BF)] * 2
        + [pltpu.VMEM((width, d), BF), pltpu.SemaphoreType.DMA((3, pl.cdiv(width, STEP)))]
        + [pltpu.SemaphoreType.DMA((len(arrays),))] * 2,
        compiler_params=pltpu.CompilerParams(
            vmem_limit_bytes=58 << 20, collective_id=1, has_side_effects=True
        ),
        cost_estimate=BRIEF,
        name="own_rows",
    )(ms, cots, wg, wu, wd, arrays)


def more_kernel(*refs, count, width, routes):
    m, cot, refs = refs[:count], refs[count : 2 * count], refs[2 * count :]
    wg_ref, wu_ref, wd_ref, hidden_ref, down_hbm = refs[:5]
    n = len(routes)
    sources, refs = refs[5 : 5 + n], refs[5 + n :]
    h_ref, gb_ref, ub_ref, send_ref, keep_ref = refs[:5]
    landings, (down_all, down_sem, sent, got) = refs[5 : 5 + n], refs[5 + n :]
    down_copy = pltpu.make_async_copy(down_hbm, down_all, down_sem)
    step = pl.program_id(0)
    full, tail = divmod(width, STEP)
    steps = full + (1 if tail else 0)
    half = hidden_ref.shape[0] // 2
    lanes = 512

    @pl.when(step == 0)
    def _():
        greet(routes)
        for copy in links(sources, landings, sent, got, routes):
            copy.start()

    def body(w):
        wg, wu, wd = wg_ref[:, :w], wu_ref[:, :w], wd_ref[:w, :]
        at = 0
        for i in range(count):
            long = m[i].shape[0]
            dst = slice(at, at + long)
            h, gb, ub = gated(m[i][...], cot[i][...], wg, wu, wd)
            h_ref[dst, :w] = h
            gb_ref[dst, :w] = gb
            ub_ref[dst, :w] = ub
            at += long

    @pl.when(step == steps // 2)
    def _():
        down_copy.start()

    if tail:
        pl.when(step < full)(lambda: body(STEP))
        pl.when(step == full)(lambda: body(tail))
    else:
        body(STEP)

    @pl.when(step == steps - 1)
    def _():
        down_copy.wait()

        def product(c, carry):
            cols = pl.ds(pl.multiple_of(c * lanes, lanes), lanes)
            total = contract(hidden_ref[...], down_all[:, cols], 1, 0)
            keep_ref[:, cols] = total[:half]
            send_ref[:, cols] = total[half:].astype(BF)
            return carry

        lax.fori_loop(0, keep_ref.shape[1] // lanes, product, 0)
        for copy in links(sources, landings, sent, got, routes):
            copy.wait()


def more_rows(ms, cots, wg, wu, wd, hidden, carried):
    count = len(ms)
    d = ms[0].shape[1]
    width = wg.shape[1]
    rows = sum(m.shape[0] for m in ms)
    own = hidden.shape[0]
    fixed = lambda i: (0, 0)
    col = lambda i: (0, i)
    row = lambda i: (i, 0)
    whole = lambda a: pl.BlockSpec(a.shape, fixed, pipeline_mode=pl.Buffered(1))
    anywhere = pl.BlockSpec(memory_space=pl.ANY)
    shape = jax.ShapeDtypeStruct
    arrays = [value for value, _ in carried]
    return pl.pallas_call(
        functools.partial(
            more_kernel, count=count, width=width, routes=tuple(route for _, route in carried)
        ),
        grid=(pl.cdiv(width, STEP),),
        in_specs=[whole(a) for a in list(ms) + list(cots)]
        + [pl.BlockSpec((d, STEP), col)] * 2
        + [pl.BlockSpec((STEP, d), row), whole(hidden), anywhere]
        + [anywhere] * len(arrays),
        out_specs=[pl.BlockSpec((rows, STEP), col)] * 3
        + [pl.BlockSpec((own // 2, d), fixed)] * 2
        + [anywhere] * len(arrays),
        out_shape=[shape((rows, width), BF)] * 3
        + [shape((own // 2, d), BF), shape((own // 2, d), F32)]
        + [shape(a.shape, a.dtype) for a in arrays],
        scratch_shapes=[pltpu.VMEM(wd.shape, BF), pltpu.SemaphoreType.DMA]
        + [pltpu.SemaphoreType.DMA((len(arrays),))] * 2,
        compiler_params=pltpu.CompilerParams(
            vmem_limit_bytes=58 << 20, collective_id=3, has_side_effects=True
        ),
        cost_estimate=BRIEF,
        name="more_rows",
    )(*ms, *cots, wg, wu, wd, hidden, wd, *arrays)


def far_kernel(*refs, longs, ready, width, tile, block, offsets, sliced, routes, cross, part_route):
    count = len(longs)
    m, cot = refs[:count], refs[count : 2 * count]
    refs = refs[2 * count :]
    m_src, c_src = m, cot
    if sliced:
        m_src, c_src = refs[:count], refs[count : 2 * count]
        refs = refs[2 * count :]
    wg_ref, wu_ref, wd_ref = refs[:3]
    known = [refs[3:6], refs[6:9]]
    refs = refs[9:]
    n = len(routes)
    summed = part_route is not None
    if summed:
        (part_send, part_keep), refs = refs[:2], refs[2:]
    sources, refs = refs[:n], refs[n:]
    (gk, uk, dk), refs = refs[:3], refs[3:]
    if summed:
        part_out, refs = refs[0], refs[1:]
    landings, refs = refs[:n], refs[n:]
    m_far, c_far, m_cols, c_cols, m_turned, c_turned = refs[:6]
    h_all, gb_all, ub_all, sends, gets, sent, got, row_sems, col_sems = refs[6:15]
    part_got = refs[15] if summed else None
    step = pl.program_id(0)
    first = gk.shape[0]
    full, tail = divmod(width, STEP)
    steps = full + (1 if tail else 0)
    begins = [sum(longs[:i]) for i in range(count)]
    near = begins[ready]
    total = sum(longs)

    def carried():
        return links(sources, landings, sent, got, routes, steps)

    def part_copy():
        return link(part_send, part_got, sent, got, steps + n, part_route)

    def row_copies():
        return [
            pltpu.make_async_copy(
                src[i], dst.at[pl.ds(begins[i] - near, longs[i]), :], row_sems.at[k, i]
            )
            for i in range(ready, count)
            for k, (src, dst) in enumerate(((m, m_far), (cot, c_far)))
        ]

    def column_copies():
        spans = [(0, None)]
        if not sliced:
            dp, ctx = lax.axis_index("dp"), lax.axis_index("ctx")
            n_ctx = lax.axis_size("ctx")
            spans = [
                (j * block, pl.multiple_of(((dp ^ a) * n_ctx + (ctx ^ b)) * block, 128))
                for j, (a, b) in enumerate(offsets)
            ]
        made = []
        for i in range(count):
            for k, (src, dst) in enumerate(((m_src, m_cols), (c_src, c_cols))):
                for j, (at, start) in enumerate(spans):
                    rows_at = pl.ds(begins[i], longs[i])
                    if start is None:
                        pair = src[i], dst.at[rows_at, :]
                    else:
                        pair = src[i].at[:, pl.ds(start, block)], dst.at[rows_at, pl.ds(at, block)]
                    made.append(pltpu.make_async_copy(*pair, col_sems.at[k, i, j]))
        return made

    @pl.when(step == 0)
    def _():
        greet(list(routes) + [cross] + [part_route] * summed)
        for copy in ([part_copy()] if summed else []) + carried() + row_copies() + column_copies():
            copy.start()
        for copy in row_copies():
            copy.wait()

    def crossing(c, w):
        return link(sends.at[c, :, :, :w], gets.at[c, :, :, :w], sent, got, c, cross)

    def body(w):
        wg, wu, wd = wg_ref[:, :w], wu_ref[:, :w], wd_ref[:w, :]
        at = 0
        for some in known:
            long = some[0].shape[0]
            for src, dst in zip(some, (h_all, gb_all, ub_all)):
                dst[at : at + long, :w] = src[:, :w]
            at += long
        for t in range((total - near) // tile):
            src = slice(t * tile, (t + 1) * tile)
            dst = slice(near + t * tile, near + (t + 1) * tile)
            h, gb, ub = gated(m_far[src, :], c_far[src, :], wg, wu, wd)
            h_all[dst, :w] = h
            gb_all[dst, :w] = gb
            ub_all[dst, :w] = ub

        @pl.when(step == 0)
        def _():
            for copy in column_copies():
                copy.wait()
            for src, dst in ((m_cols, m_turned), (c_cols, c_turned)):
                for t in range(total // tile):
                    dst[:, t * tile : (t + 1) * tile] = src[t * tile : (t + 1) * tile, :].T

        lanes = pl.ds(pl.multiple_of(step * STEP, STEP), w)
        for i, (src, keep) in enumerate(((gb_all, gk), (ub_all, uk))):
            grad = contract(m_turned[...], src[:, :w], 1, 0)
            keep[:, lanes] = grad[:first]
            sends[step, i, :, :w] = grad[first:].astype(BF)
        grad = contract(c_turned[...], h_all[:, :w], 1, 0)
        dk[lanes, :] = grad[:first].T
        sends[step, 2, :, :w] = grad[first:].astype(BF)
        crossing(step, w).start()

    if tail:
        pl.when(step < full)(lambda: body(STEP))
        pl.when(step == full)(lambda: body(tail))
    else:
        body(STEP)

    @pl.when(step == steps - 1)
    def _():
        if summed:
            part_copy().wait()
            part_out[...] = part_keep[...] + part_got[...].astype(F32)
        for c in range(steps):
            w = STEP if c < full else tail
            crossing(c, w).wait()
            at = slice(c * STEP, c * STEP + w)
            gk[:, at] += gets[c, 0, :, :w].astype(F32)
            uk[:, at] += gets[c, 1, :, :w].astype(F32)
            dk[at, :] += gets[c, 2, :, :w].astype(F32).T
        for copy in carried():
            copy.wait()


def far_rows(
    ms,
    cots,
    m_cols,
    cot_cols,
    weights,
    known,
    span,
    ready,
    block,
    offsets,
    cross,
    part,
    carried,
    collective_id,
    name,
):
    base, steps, width = span
    longs = tuple(m.shape[0] for m in ms)
    total, later = sum(longs), sum(longs[ready:])
    d = weights[0].shape[0]
    wide = block * len(offsets)
    first = wide // 2
    fixed = lambda i: (0, 0)
    col = lambda i: (0, i + base)
    row = lambda i: (i + base, 0)
    anywhere = pl.BlockSpec(memory_space=pl.ANY)
    shape = jax.ShapeDtypeStruct
    extra = [] if m_cols is None else list(m_cols) + list(cot_cols)
    arrays = [value for value, _ in carried]
    parts = [] if part is None else list(part[:2])
    part_specs = [] if part is None else [
        anywhere,
        pl.BlockSpec(part[1].shape, fixed, pipeline_mode=pl.Buffered(1)),
    ]
    part_shapes = [] if part is None else [part[1].shape]
    sems = pltpu.SemaphoreType.DMA((steps + len(carried) + 1,))
    return pl.pallas_call(
        functools.partial(
            far_kernel,
            longs=longs,
            ready=ready,
            width=width,
            tile=512,
            block=block,
            offsets=offsets,
            sliced=m_cols is not None,
            routes=tuple(route for _, route in carried),
            cross=cross,
            part_route=None if part is None else part[2],
        ),
        grid=(steps,),
        in_specs=[anywhere] * (2 * len(ms) + len(extra))
        + [pl.BlockSpec((d, STEP), col)] * 2
        + [pl.BlockSpec((STEP, d), row)]
        + [pl.BlockSpec((a.shape[0], STEP), col) for a in known]
        + part_specs
        + [anywhere] * len(carried),
        out_specs=[pl.BlockSpec((first, width), fixed)] * 2
        + [pl.BlockSpec((width, first), fixed)]
        + [pl.BlockSpec(a, fixed) for a in part_shapes]
        + [anywhere] * len(carried),
        out_shape=[shape((first, width), F32)] * 2
        + [shape((width, first), F32)]
        + [shape(a, F32) for a in part_shapes]
        + [shape(a.shape, a.dtype) for a in arrays],
        scratch_shapes=[pltpu.VMEM((later, d), BF)] * 2
        + [pltpu.VMEM((total, wide), BF)] * 2
        + [pltpu.VMEM((wide, total), BF)] * 2
        + [pltpu.VMEM((total, STEP), BF)] * 3
        + [pltpu.VMEM((steps, 3, first, STEP), BF)] * 2
        + [sems] * 2
        + [
            pltpu.SemaphoreType.DMA((2, len(ms))),
            pltpu.SemaphoreType.DMA((2, len(ms), len(offsets))),
        ]
        + [pltpu.VMEM(a, BF) for a in part_shapes],
        compiler_params=pltpu.CompilerParams(
            vmem_limit_bytes=60 << 20, collective_id=collective_id, has_side_effects=True
        ),
        cost_estimate=BRIEF,
        name=name,
    )(*ms, *cots, *extra, *weights, *known, *parts, *arrays)


TILE = 32


def finish_kernel(
    low_two,
    far_two,
    middle,
    low_four,
    far_four,
    middle_back,
    x_ref,
    gain_ref,
    mlp_part,
    sources,
    layer_ref,
    tokens_ref,
    gains_ref,
    landings,
    parts,
    other_parts,
    blocks,
    landed,
    sent,
    got,
    peer_sent,
    peer_got,
    *,
    routes,
):
    dp, ctx = lax.axis_index("dp"), lax.axis_index("ctx")
    n_dp, n_ctx = lax.axis_size("dp"), lax.axis_size("ctx")
    core = lax.rem(lax.axis_index("tp"), 2)
    half, d = middle.shape
    owners, _, block = blocks.shape
    mesh = pl.DeviceIdType.MESH
    near = ("tp", 1)
    codes = [(a, b) for a in range(n_dp) for b in range(n_ctx)][1:]
    ids = [{"dp": dp ^ a, "ctx": ctx ^ b} for a, b in codes]
    barrier = pltpu.get_barrier_semaphore()
    for peer in ids + [mate(*near)]:
        pl.semaphore_signal(barrier, inc=1, device_id=peer, device_id_type=mesh)
    pl.semaphore_wait(barrier, len(ids) + 1)
    n = len(routes)
    carried = links(sources, landings, sent, got, routes)
    for copy in carried:
        copy.start()

    own = pl.ds(pl.multiple_of(core * half, half), half)
    parts[0:1, :] = jnp.zeros((1, d), F32)
    parts[1:2, :] = mlp_part[...]

    def tokens_step(t, carry):
        at = pl.ds(pl.multiple_of(t * TILE, TILE), TILE)
        out_at = pl.ds(pl.multiple_of(core * half + t * TILE, TILE), TILE)
        x = x_ref[at, :].astype(F32)
        inverse = lax.rsqrt(jnp.mean(x * x, axis=-1, keepdims=True) + EPSILON)
        normed = x * inverse
        back = low_four[at, :].astype(F32) + far_four[at, :].astype(F32)
        parts[0:1, :] += jnp.sum(back * normed, axis=0, keepdims=True)
        scaled = back * gain_ref[...]
        mean = jnp.mean(scaled * normed, axis=-1, keepdims=True)
        tokens_ref[out_at, :] = middle_back[at, :] + inverse * (scaled - normed * mean)
        return carry

    lax.fori_loop(0, half // TILE, tokens_step, 0)
    to_core = [
        link(parts, other_parts, sent, got, n, near),
        link(tokens_ref.at[own, :], tokens_ref.at[own, :], sent, got, n + 1, near),
        link(layer_ref.at[own, :], layer_ref.at[own, :], sent, got, n + 2, near),
    ]
    to_core[0].start()
    to_core[1].start()

    def layer_step(t, carry):
        at = pl.ds(pl.multiple_of(t * TILE, TILE), TILE)
        out_at = pl.ds(pl.multiple_of(core * half + t * TILE, TILE), TILE)
        layer_ref[out_at, :] = middle[at, :] + (
            low_two[at, :].astype(F32) + far_two[at, :].astype(F32)
        )
        return carry

    lax.fori_loop(0, half // TILE, layer_step, 0)
    to_core[2].start()
    to_core[0].wait()
    for k in range(owners):
        at = slice(k * block, (k + 1) * block)
        blocks[k] = parts[:, at] + other_parts[:, at]
    copies = [
        pltpu.make_async_remote_copy(
            src_ref=blocks.at[peer["dp"] * n_ctx + peer["ctx"]],
            dst_ref=landed.at[k],
            send_sem=peer_sent.at[k],
            recv_sem=peer_got.at[k],
            device_id=peer,
            device_id_type=mesh,
        )
        for k, peer in enumerate(ids)
    ]
    for copy in copies:
        copy.start()
    for copy in copies:
        copy.wait()
    total = blocks[dp * n_ctx + ctx]
    for k in range(len(ids)):
        total = total + landed[k]
    gains_ref[...] = total
    for copy in to_core[1:] + carried:
        copy.wait()


def finish(values, gain, mlp_part, rows, carried):
    d = values[2].shape[1]
    owners = lax.axis_size("dp") * lax.axis_size("ctx")
    block = d // owners
    arrays = [value for value, _ in carried]
    vmem = pl.BlockSpec(memory_space=pltpu.VMEM)
    anywhere = pl.BlockSpec(memory_space=pl.ANY)
    shape = jax.ShapeDtypeStruct
    layer_out, tokens_grad, gains, landed = pl.pallas_call(
        functools.partial(finish_kernel, routes=tuple(route for _, route in carried)),
        in_specs=[vmem] * 9 + [[anywhere] * len(arrays)],
        out_specs=[vmem] * 3 + [[anywhere] * len(arrays)],
        out_shape=[shape((rows, d), F32)] * 2
        + [shape((2, block), F32), [shape(a.shape, a.dtype) for a in arrays]],
        scratch_shapes=[pltpu.VMEM((2, d), F32)] * 2
        + [pltpu.VMEM((owners, 2, block), F32), pltpu.VMEM((owners - 1, 2, block), F32)]
        + [pltpu.SemaphoreType.DMA((len(arrays) + 3,))] * 2
        + [pltpu.SemaphoreType.DMA((owners - 1,))] * 2,
        compiler_params=pltpu.CompilerParams(
            vmem_limit_bytes=58 << 20, collective_id=5, has_side_effects=True
        ),
        cost_estimate=BRIEF,
        name="finish",
    )(*values, gain, mlp_part, arrays)
    return layer_out, tokens_grad, gains, *landed


def shards(
    tokens,
    segments,
    attn_gain,
    query_weight,
    key_weight,
    value_weight,
    output_weight,
    mlp_gain,
    gate_weight,
    up_weight,
    down_weight,
    cotangent,
):
    rows, d = tokens.shape
    half = rows // 2
    seq = segments.shape[1]
    window = min(seq, seq // 2 + QB)
    ctx, dp = lax.axis_index("ctx"), lax.axis_index("dp")
    n_ctx, n_dp = lax.axis_size("ctx"), lax.axis_size("dp")
    core = lax.rem(lax.axis_index("tp"), 2)
    tp_rest = bits_of("tp")[1:]
    block_width = d // (n_ctx * n_dp)
    every_bit = bits_of("ctx") + bits_of("dp")
    attn_share = [("ctx", 1)]
    mlp_reduce = bits_of("ctx")[1:] + bits_of("dp")[:-1]
    attn_reduce = [b for b in every_bit if b not in attn_share]

    def owner_offsets(reduce_bits):
        return [
            [bit for i, bit in enumerate(reduce_bits) if code >> (len(reduce_bits) - 1 - i) & 1]
            for code in range(1 << len(reduce_bits))
        ]

    def owner_start(chosen, flip=()):
        other_dp, other_ctx = dp, ctx
        for axis, mask in list(chosen) + list(flip):
            if axis == "dp":
                other_dp = other_dp ^ mask
            else:
                other_ctx = other_ctx ^ mask
        return (other_dp * n_ctx + other_ctx) * block_width

    def columns(value, chosen, flip=()):
        return lax.dynamic_slice_in_dim(value, owner_start(chosen, flip), block_width, 1)

    def all_columns(value, reduce_bits, flip=()):
        return jnp.concatenate(
            [columns(value, chosen, flip) for chosen in owner_offsets(reduce_bits)], 1
        )

    def own_half(value):
        return lax.dynamic_slice_in_dim(value, core * half, half, 0)

    def other_half(value):
        return lax.dynamic_slice_in_dim(value, (1 - core) * half, half, 0)

    def both_halves(value):
        return jnp.concatenate([own_half(value), other_half(value)], 0)

    def join_cores(value):
        return jnp.concatenate([value, swap(value, "tp", 1)], 0)

    def with_core(pieces):
        return [piece for value in pieces for piece in (value, swap(value, "tp", 1))]

    def mirror(value):
        return swap(value, "dp", n_dp - 1)

    def tp_low(send, keep):
        total = keep + swap(send.astype(BF), "tp", 1).astype(F32)
        for axis, mask in tp_rest[:-1]:
            low = total.astype(BF)
            total = low.astype(F32) + swap(low, axis, mask).astype(F32)
        return total.astype(BF)

    def tp_end(low, other):
        return low.astype(F32) + other.astype(F32)

    def after(value, *others):
        return lax.optimization_barrier((value,) + others)[0]

    def halves(value, dim):
        middle = value.shape[dim] // 2
        keep = lax.slice_in_dim(value, 0, middle, axis=dim)
        return keep, lax.slice_in_dim(value, middle, 2 * middle, axis=dim).astype(BF)

    def reduce_blocks(value, reduce_bits, dim):
        for axis, mask in reduce_bits:
            keep, send = halves(value, dim)
            value = keep + swap(send, axis, mask).astype(F32)
        return value

    seg_row = segments
    seg_col = jnp.swapaxes(segments, 0, 1)
    query_pos = ctx * rows + jnp.arange(rows, dtype=jnp.int32)
    cos_table, sin_table = rope_tables(query_pos, HEAD)
    kv_weight = jnp.concatenate([key_weight, value_weight], 1)
    cot_half = own_half(cotangent)
    cot_own = [cot_half, other_half(cotangent)]
    x_half = own_half(tokens).astype(F32)

    attn_in, q_rot, kv_own = enter(
        tokens, attn_gain[None], query_weight, kv_weight, cos_table, sin_table
    )
    kv_parts = [kv_own]
    for axis, mask in bits_of("ctx"):
        kv_parts = kv_parts + [swap(piece, axis, mask) for piece in kv_parts]
    kv_all = jnp.stack(kv_parts, 0)
    quarter = half // 2
    last, side, across = tp_rest[-1], ("ctx", 1), ("dp", n_dp - 1)

    def own_quarter(value):
        which = lax.rem(lax.div(lax.axis_index("tp"), last[1]), 2)
        return lax.dynamic_slice_in_dim(value, which * quarter, quarter, 0)

    cot_dp_q = mirror(own_quarter(cot_half))
    cot_ctx_a = swap(cot_half[:quarter], *side)
    attn_cols_half = own_half(all_columns(attn_in, attn_reduce, attn_share))
    kv_all, attn_cols_half, *_ = lax.optimization_barrier(
        (kv_all, attn_cols_half, cot_dp_q, cot_ctx_a)
    )
    attn_cols_far = swap(attn_cols_half, *side)
    cot_dp_r = swap(cot_dp_q, *last)
    heads_out, lse = attend(q_rot, kv_all, seg_col, seg_row, window)
    heads_out = after(heads_out, attn_cols_far, cot_dp_r)
    heads_mine, heads_other = own_half(heads_out), other_half(heads_out)
    low_one = tp_low(
        contract(heads_other, output_weight, 1, 0), contract(heads_mine, output_weight, 1, 0)
    )
    far_one, cot_ctx_b, cot_both_q = exchange(
        [(low_one, last), (cot_half[quarter:], side), (cot_dp_q, side)], 2, "exchange_one"
    )
    cot_ctx = jnp.concatenate([cot_ctx_a, cot_ctx_b], 0)
    middle = x_half + tp_end(low_one, far_one)
    inverse_two = lax.rsqrt(jnp.mean(middle * middle, axis=-1, keepdims=True) + EPSILON)
    normed_two = middle * inverse_two
    mlp_half = (normed_two * mlp_gain).astype(BF)
    mlp_own = [mlp_half, swap(mlp_half, "tp", 1)]
    hidden_own, gate_own, up_own, back_send, back_keep, arrived = own_rows(
        mlp_own,
        cot_own,
        gate_weight,
        up_weight,
        down_weight,
        [
            (mlp_half, side),
            (own_quarter(mlp_half), across),
            (cot_both_q, last),
        ],
    )
    mlp_ctx, mlp_dp_q, cot_both_r = arrived
    low_three = tp_low(back_send, back_keep)
    heads_rel = jnp.concatenate([heads_mine, heads_other], 0)
    mlp_near, cot_near = with_core([mlp_ctx]), with_core([cot_ctx])
    more = more_rows(
        mlp_near,
        cot_near,
        gate_weight,
        up_weight,
        down_weight,
        hidden_own,
        [
            (low_three, last),
            (mlp_dp_q, side),
            (heads_rel, side),
        ],
    )
    down_send, down_keep, far_three, mlp_both_q, heads_far = more[3:]
    low_two = tp_low(down_send, down_keep)
    mlp_in_back = tp_end(low_three, far_three)
    scaled = mlp_in_back * mlp_gain
    middle_back = cot_half.astype(F32) + inverse_two * (
        scaled - normed_two * jnp.mean(scaled * normed_two, axis=-1, keepdims=True)
    )
    mlp_gain_part = jnp.sum(mlp_in_back * normed_two, axis=0)
    branch_half = middle_back.astype(BF)
    branch_own = join_cores(branch_half)
    heads_back = contract(branch_own, output_weight, 1, 1).astype(BF)

    flip = attn_share
    branch_cols = all_columns(branch_own, attn_reduce)
    branch_cols_half = all_columns(branch_half, attn_reduce, flip)
    query_back, kv_part, kv_far, (branch_cols_far, mlp_dp_r) = attend_back(
        q_rot,
        heads_back,
        kv_all,
        lse,
        seg_col,
        seg_row,
        cos_table,
        sin_table,
        window,
        [(branch_cols_half, side), (mlp_dp_q, last)],
    )
    mlp_both_r = swap(after(mlp_both_q, far_three), *last)
    kv_far, query_back, *_ = lax.optimization_barrier((kv_far, query_back, mlp_both_r))
    output_part = contract(heads_rel, branch_cols, 0, 0) + contract(
        heads_far, join_cores(branch_cols_far), 0, 0
    )
    output_keep, output_send = halves(reduce_blocks(output_part, attn_reduce[:-2], 1), 1)
    query_rel = jnp.concatenate([own_half(query_back), other_half(query_back)], 0)

    mlp_group = mlp_own + mlp_near + with_core([mlp_dp_q, mlp_dp_r, mlp_both_q, mlp_both_r])
    cot_group = cot_own + cot_near + with_core([cot_dp_q, cot_dp_r, cot_both_q, cot_both_r])
    offsets = tuple(
        (
            sum(mask for axis, mask in chosen if axis == "dp"),
            sum(mask for axis, mask in chosen if axis == "ctx"),
        )
        for chosen in owner_offsets(mlp_reduce)
    )
    aligned = block_width % 128 == 0
    m_cols = None if aligned else [all_columns(m, mlp_reduce) for m in mlp_group]
    c_cols = None if aligned else [all_columns(c, mlp_reduce) for c in cot_group]
    hidden_width = gate_weight.shape[1]
    early_steps = pl.cdiv(hidden_width, STEP) // 2
    early_width = early_steps * STEP

    def far_span(base, steps, width, part, carried, collective_id, name):
        return far_rows(
            mlp_group,
            cot_group,
            m_cols,
            c_cols,
            [gate_weight, up_weight, down_weight],
            [hidden_own, gate_own, up_own, *more[:3]],
            (base, steps, width),
            4,
            block_width,
            offsets,
            mlp_reduce[0],
            part,
            carried,
            collective_id,
            name,
        )

    early = far_span(
        0,
        early_steps,
        early_width,
        None,
        [(kv_far[j - 1], ("ctx", j)) for j in range(1, n_ctx)]
        + [(query_rel, side), (output_send, attn_reduce[-2]), (low_two, last)],
        0,
        "far_early",
    )
    output_near, far_two = early[-2:]
    query_far = early[-3]
    output_keep, output_send = halves(output_keep + output_near.astype(F32), 1)
    kv_back = join_keys(kv_part, early[3 : 2 + n_ctx], cos_table, sin_table)
    qkv_back = jnp.concatenate([query_back, kv_back], 1)
    back_mine, back_other = own_half(qkv_back), other_half(qkv_back)
    q_width = query_back.shape[1]

    def attn_back(part):
        return contract(part[:, :q_width], query_weight, 1, 1) + contract(
            part[:, q_width:], kv_weight, 1, 1
        )

    low_four = tp_low(attn_back(back_other), attn_back(back_mine))

    attn_cols = both_halves(all_columns(attn_in, attn_reduce))
    back_rel = jnp.concatenate([back_mine, back_other], 0)
    back_far_rel = jnp.concatenate([query_far, swap(back_rel[:, q_width:], *side)], 1)
    qkv_keep, qkv_send = halves(
        reduce_blocks(
            contract(attn_cols, back_rel, 0, 0)
            + contract(join_cores(attn_cols_far), back_far_rel, 0, 0),
            attn_reduce[:-2],
            0,
        ),
        0,
    )
    late = far_span(
        early_steps,
        pl.cdiv(hidden_width, STEP) - early_steps,
        hidden_width - early_width,
        (qkv_send, qkv_keep, attn_reduce[-2]),
        [(low_four, last), (output_send, attn_reduce[-1])],
        6,
        "far_late",
    )
    qkv_part, far_four, output_far = late[3:]
    gate_part = jnp.concatenate([early[0], late[0]], 1)
    up_part = jnp.concatenate([early[1], late[1]], 1)
    down_part = jnp.concatenate([early[2], late[2]], 0)
    output_grad = output_keep + output_far.astype(F32)
    qkv_keep, qkv_send = halves(qkv_part, 0)
    layer_out, tokens_grad, gains, qkv_far = finish(
        (low_two, far_two, middle, low_four, far_four, middle_back, own_half(tokens)),
        attn_gain[None],
        mlp_gain_part[None],
        rows,
        [(qkv_send, attn_reduce[-1])],
    )
    qkv_grad = qkv_keep + qkv_far.astype(F32)
    gate_grad = reduce_blocks(gate_part, mlp_reduce[1:], 0)
    up_grad = reduce_blocks(up_part, mlp_reduce[1:], 0)
    down_grad = reduce_blocks(down_part, mlp_reduce[1:], 1)
    return (
        layer_out,
        tokens_grad,
        gains[0],
        qkv_grad[:, :q_width],
        qkv_grad[:, q_width : q_width + HEAD],
        qkv_grad[:, q_width + HEAD :],
        output_grad,
        gains[1],
        gate_grad,
        up_grad,
        down_grad,
    )


def solution(mesh):
    return jax.shard_map(
        shards,
        mesh=mesh,
        in_specs=(
            P(("dp", "ctx"), None),
            P("dp", None),
            P(),
            P(None, "tp"),
            P(None, "tp"),
            P(None, "tp"),
            P("tp", None),
            P(),
            P(None, "tp"),
            P(None, "tp"),
            P("tp", None),
            P(("dp", "ctx"), None),
        ),
        out_specs=(
            P(("dp", "ctx"), None),
            P(("dp", "ctx"), None),
            P(("dp", "ctx")),
            P(("dp", "ctx"), "tp"),
            P(("dp", "ctx"), "tp"),
            P(("dp", "ctx"), "tp"),
            P("tp", ("dp", "ctx")),
            P(("dp", "ctx")),
            P(("dp", "ctx"), "tp"),
            P(("dp", "ctx"), "tp"),
            P("tp", ("dp", "ctx")),
        ),
        check_vma=False,
    )
```
